128 devices in a mesh: vp: 4 (over x), dp: 32 (over z, y, core).
Axes of the slice: x: 4, y: 4, z: 4, core: 2. Of those that a mesh axis runs over, the one named last changes fastest.
Arguments:
- hidden: bfloat16 [192, 512, 1024], P('dp')
- mask_pos: int32 [192, 77], P('dp')
- labels: int32 [192, 77], P('dp')
- w_trans: bfloat16 [1024, 1024], replicated
- b_trans: float32 [1024], replicated
- ln_gain: float32 [1024], replicated
- ln_bias: float32 [1024], replicated
- emb_table: bfloat16 [30592, 1024], P('vp')
- b_vocab: float32 [30592], P('vp')
Outputs:
- output 1: float32 [], replicated
- output 2: bfloat16 [192, 512, 1024], P('dp')
- output 3: float32 [1024, 1024], replicated
- output 4: float32 [1024], replicated
- output 5: float32 [1024], replicated
- output 6: float32 [1024], replicated
- output 7: float32 [30592, 1024], P('vp')
- output 8: float32 [30592], P('vp')
All inputs are finite; a program needn't handle non-finite values.
Results may differ from the reference program's by a relative error of at most 0.0107114.
Values sent between devices are 32-bit elements.
A program may use at most 1 GiB of HBM per device.

```python
import jax
import jax.numpy as jnp
from jax import lax

HIDDEN = 1024
VOCAB_PAD = 30592
VOCAB_REAL = 30522
SEQ_LEN = 512
N_MASKS = 77
BATCH_ALL = 192
SHARDS = 4
LOG_VOCAB = (VOCAB_REAL - 1).bit_length()
LN_EPS = 1e-5
PAD_BIAS = -1.0e9


def head_norm(pre_act, ln_gain, ln_bias):
    gelu_out = jax.nn.gelu(pre_act, approximate=False)
    row_mean = jnp.mean(gelu_out, axis=-1, keepdims=True)
    centered = gelu_out - row_mean
    row_var = jnp.mean(centered * centered, axis=-1, keepdims=True)
    return centered * lax.rsqrt(row_var + LN_EPS) * ln_gain + ln_bias


def setup_inputs(seed: int = 0) -> dict:
    sub_keys = jax.random.split(jax.random.key(seed), 12)
    hidden = jax.random.normal(sub_keys[0], (BATCH_ALL, SEQ_LEN, HIDDEN), jnp.float32).astype(jnp.bfloat16)

    def draw_row(row_key):
        return jax.random.permutation(row_key, SEQ_LEN)[:N_MASKS]

    mask_pos = jax.vmap(draw_row)(jax.random.split(sub_keys[1], BATCH_ALL)).astype(jnp.int32)
    label_exp = jax.random.randint(sub_keys[2], (BATCH_ALL, N_MASKS), 0, LOG_VOCAB + 1)
    label_top = jnp.minimum(jnp.left_shift(jnp.ones_like(label_exp), label_exp), VOCAB_REAL)
    labels = jax.random.randint(sub_keys[3], (BATCH_ALL, N_MASKS), 0, label_top)
    labels = labels.at[0, 0].set(VOCAB_REAL - 1).astype(jnp.int32)
    w_trans = (jax.random.normal(sub_keys[4], (HIDDEN, HIDDEN), jnp.float32) * HIDDEN ** -0.5).astype(jnp.bfloat16)
    b_trans = 0.5 * jax.random.normal(sub_keys[5], (HIDDEN,), jnp.float32)
    ln_gain = 1.0 + 0.3 * jax.random.normal(sub_keys[6], (HIDDEN,), jnp.float32)
    ln_bias = 0.3 * jax.random.normal(sub_keys[7], (HIDDEN,), jnp.float32)
    emb_table = (jax.random.normal(sub_keys[8], (VOCAB_PAD, HIDDEN), jnp.float32) * HIDDEN ** -0.5).astype(jnp.bfloat16)
    bias_slope = jax.random.uniform(sub_keys[9], (), jnp.float32, 0.3, 0.6)
    bias_noise = jax.random.normal(sub_keys[10], (VOCAB_PAD,), jnp.float32)
    vocab_ids = jnp.arange(VOCAB_PAD)
    b_vocab = 0.5 * bias_noise - bias_slope * jnp.log1p(vocab_ids.astype(jnp.float32))
    b_vocab = jnp.where(vocab_ids < VOCAB_REAL, b_vocab, PAD_BIAS).astype(jnp.float32)
    return {"hidden": hidden, "mask_pos": mask_pos, "labels": labels, "w_trans": w_trans, "b_trans": b_trans, "ln_gain": ln_gain, "ln_bias": ln_bias, "emb_table": emb_table, "b_vocab": b_vocab}


def reference(hidden, mask_pos, labels, w_trans, b_trans, ln_gain, ln_bias, emb_table, b_vocab):
    n_rows = hidden.shape[0]
    n_tokens = n_rows * N_MASKS
    shard_rows = VOCAB_PAD // SHARDS
    masked_h = jnp.take_along_axis(hidden, mask_pos[:, :, None], axis=1).reshape(n_tokens, HIDDEN)
    pre_act = jnp.dot(masked_h, w_trans, preferred_element_type=jnp.float32) + b_trans
    u_norm, head_vjp = jax.vjp(head_norm, pre_act, ln_gain, ln_bias)
    u_bf16 = u_norm.astype(jnp.bfloat16)
    flat_labels = labels.reshape(n_tokens)
    emb_blocks = emb_table.reshape(SHARDS, shard_rows, HIDDEN)
    bias_blocks = b_vocab.reshape(SHARDS, shard_rows)
    row_starts = jnp.arange(SHARDS) * shard_rows
    row_ids = jnp.arange(shard_rows)

    def block_logits(emb_block, bias_block):
        return jnp.dot(u_bf16, emb_block.T, preferred_element_type=jnp.float32) + bias_block

    def block_stats(block):
        emb_block, bias_block, row_start = block
        logits = block_logits(emb_block, bias_block)
        local_max = jnp.max(logits, axis=1)
        local_sum = jnp.sum(jnp.exp(logits - local_max[:, None]), axis=1)
        is_label = (flat_labels - row_start)[:, None] == row_ids[None, :]
        label_logit = jnp.sum(jnp.where(is_label, logits, 0.0), axis=1)
        return local_max, local_sum, label_logit

    block_max, block_sum, block_label = lax.map(block_stats, (emb_blocks, bias_blocks, row_starts))
    global_max = jnp.max(block_max, axis=0)
    log_norm = global_max + jnp.log(jnp.sum(block_sum * jnp.exp(block_max - global_max), axis=0))
    mlm_loss = jnp.mean(log_norm - jnp.sum(block_label, axis=0))

    def block_grads(block):
        emb_block, bias_block, row_start = block
        logits = block_logits(emb_block, bias_block)
        is_label = (flat_labels - row_start)[:, None] == row_ids[None, :]
        d_logits = (jnp.exp(logits - log_norm[:, None]) - is_label.astype(jnp.float32)) / n_tokens
        d_logits_bf = d_logits.astype(jnp.bfloat16)
        d_emb_block = jnp.dot(d_logits_bf.T, u_bf16, preferred_element_type=jnp.float32)
        du_part = jnp.dot(d_logits_bf, emb_block, preferred_element_type=jnp.float32).astype(jnp.bfloat16)
        return d_emb_block, jnp.sum(d_logits, axis=0), du_part

    d_emb_blocks, d_bias_blocks, du_parts = lax.map(block_grads, (emb_blocks, bias_blocks, row_starts))
    d_unorm = jnp.sum(du_parts.astype(jnp.float32), axis=0)
    d_pre, d_ln_gain, d_ln_bias = head_vjp(d_unorm)
    d_pre_bf = d_pre.astype(jnp.bfloat16)
    d_w_trans = jnp.dot(masked_h.T, d_pre_bf, preferred_element_type=jnp.float32)
    d_b_trans = jnp.sum(d_pre, axis=0)
    d_masked = jnp.dot(d_pre_bf, w_trans.T, preferred_element_type=jnp.float32).astype(jnp.bfloat16)
    row_index = jnp.arange(n_rows)[:, None]
    d_hidden = jnp.zeros_like(hidden).at[row_index, mask_pos].set(d_masked.reshape(n_rows, N_MASKS, HIDDEN))
    return (mlm_loss, d_hidden, d_w_trans, d_b_trans, d_ln_gain, d_ln_bias, d_emb_blocks.reshape(VOCAB_PAD, HIDDEN), d_bias_blocks.reshape(VOCAB_PAD))
```

```python
import functools

import jax
import jax.numpy as jnp
from jax import lax
from jax.experimental import pallas as pl
from jax.experimental.pallas import tpu as pltpu
from jax.sharding import PartitionSpec as P

MESH = pl.DeviceIdType.MESH
LN_EPS = 1e-5
TOK = 512
VROWS = 3824
NCH = 8
ROWS = 3840
HALF = 1920
SH = 480
SUB = 120
BLK = 384

def add_rows(dst, k, d0, srcs, n, blk):
    def body(i, c):
        o = pl.multiple_of(i * blk, 8)
        v = dst[k, pl.ds(pl.multiple_of(d0 + o, 8), blk), :]
        for s in srcs:
            v = v + s[pl.ds(o, blk), :]
        dst[k, pl.ds(pl.multiple_of(d0 + o, 8), blk), :] = v
        return c
    lax.fori_loop(0, n // blk, body, 0)


def reduce_kernel(gt, u, both, r1, r2, r3, r4, a1, a2, ssem, rsem, psend, precv):
    m, oth = both.at[0], both.at[1]
    dp = lax.axis_index("dp")
    z, y, c = dp // 8, (dp // 2) % 4, dp % 2
    ynb = [z * 8 + ((y + d) % 4) * 2 + c for d in (1, 3)]
    znb = [((z + d) % 4) * 8 + y * 2 + c for d in (1, 3)]
    mate = dp + 1 - 2 * c
    barrier = pltpu.get_barrier_semaphore()
    for d in ynb + znb + [mate]:
        pl.semaphore_signal(barrier, inc=1, device_id={"dp": d}, device_id_type=MESH)
    pl.semaphore_wait(barrier, 5)
    halves = ((0, y, ynb, z, znb), (HALF, z, znb, y, ynb))

    def copy(src, dst, st, h, d, k, dev):
        return pltpu.make_async_remote_copy(
            src_ref=src, dst_ref=dst, send_sem=ssem.at[st, h, d, k], recv_sem=rsem.at[st, h, d, k],
            device_id={"dp": dev}, device_id_type=MESH)

    def rows(k, start, n):
        return m.at[k, pl.ds(pl.multiple_of(start, 8), n)]

    def stage_copies(st, k):
        out = []
        for h, (b, p, pn, q, qn) in enumerate(halves):
            b2 = b + p * SH
            op, oq = (p + 2) % 4, (q + 2) % 4
            pp, pm, qp, qm = (p + 1) % 4, (p + 3) % 4, (q + 1) % 4, (q + 3) % 4
            if st == 0:
                a = rows(k, b + op * SH, 240), r1.at[k % 2, h, 0], rows(k, b + op * SH + 240, 240), r1.at[k % 2, h, 1], pn
            elif st == 1:
                a = rows(k, b + pp * SH, SH), r2.at[k % 2, h, 0], rows(k, b + pm * SH, SH), r2.at[k % 2, h, 1], pn
            elif st == 2:
                a = (rows(k, b2 + oq * SUB, 64), r3.at[k % 2, h, 0], rows(k, b2 + oq * SUB + 64, 56),
                     r3.at[k % 2, h, 1, pl.ds(0, 56)], qn)
            elif st == 3:
                a = rows(k, b2 + qp * SUB, SUB), r4.at[k % 2, h, 0], rows(k, b2 + qm * SUB, SUB), r4.at[k % 2, h, 1], qn
            elif st == 4:
                s = rows(k, b2 + q * SUB, SUB)
                a = s, a1.at[k % 3, h, 0], s, a1.at[k % 3, h, 1], qn
            elif st == 5:
                a = (a1.at[k % 3, h, 0, pl.ds(0, 64)], a2.at[k % 3, h, 0], a1.at[k % 3, h, 1, pl.ds(64, 56)],
                     a2.at[k % 3, h, 1, pl.ds(0, 56)], qn)
            elif st == 6:
                s = rows(k, b2, SH)
                a = s, s, s, s, pn
            else:
                s0, s1 = rows(k, b + pm * SH, 240), rows(k, b + pp * SH + 240, 240)
                a = s0, s0, s1, s1, pn
            out.append(copy(a[0], a[1], st, h, 0, k, a[4][0]))
            out.append(copy(a[2], a[3], st, h, 1, k, a[4][1]))
        return out

    def mate_copy(k):
        return pltpu.make_async_remote_copy(
            src_ref=m.at[k], dst_ref=oth.at[k], send_sem=psend.at[k], recv_sem=precv.at[k],
            device_id={"dp": mate}, device_id_type=MESH)

    def stage(st, k):
        if st == 0:
            def mm(i, cc):
                o = pl.multiple_of(i * SH, 8)
                m[k, pl.ds(o, SH), :] = jnp.dot(gt[pl.ds(o, SH), :], u[:, pl.ds(pl.multiple_of(k * 128, 128), 128)], preferred_element_type=jnp.float32)
                return cc
            lax.fori_loop(0, ROWS // SH, mm, 0)
        else:
            for cp in stage_copies(st - 1, k):
                cp.wait()
            for h, (b, p, pn, q, qn) in enumerate(halves):
                b2 = b + p * SH
                pp, pm, qp, qm = (p + 1) % 4, (p + 3) % 4, (q + 1) % 4, (q + 3) % 4
                if st == 1:
                    add_rows(m, k, b + pp * SH, [r1.at[k % 2, h, 0]], 240, 80)
                    add_rows(m, k, b + pm * SH + 240, [r1.at[k % 2, h, 1]], 240, 80)
                elif st == 2:
                    add_rows(m, k, b2, [r2.at[k % 2, h, 0], r2.at[k % 2, h, 1]], SH, 80)
                elif st == 3:
                    add_rows(m, k, b2 + qp * SUB, [r3.at[k % 2, h, 0]], 64, 64)
                    add_rows(m, k, b2 + qm * SUB + 64, [r3.at[k % 2, h, 1]], 56, 56)
                elif st == 4:
                    add_rows(m, k, b2 + q * SUB, [r4.at[k % 2, h, 0], r4.at[k % 2, h, 1]], SUB, 40)
                elif st == 5:
                    rows(k, b2 + qm * SUB, SUB)[...] = a1[k % 3, h, 0]
                    rows(k, b2 + qp * SUB, SUB)[...] = a1[k % 3, h, 1]
                elif st == 6:
                    oq = (q + 2) % 4
                    rows(k, b2 + oq * SUB, 64)[...] = a2[k % 3, h, 0]
                    rows(k, b2 + oq * SUB + 64, 56)[...] = a2[k % 3, h, 1, pl.ds(0, 56)]
        if st < 8:
            for cp in stage_copies(st, k):
                cp.start()
        else:
            mate_copy(k).start()

    def step(t, carry):
        for st in range(8, -1, -1):
            k = t - st

            @pl.when((k >= 0) & (k < NCH))
            def _():
                stage(st, k)
        return carry

    lax.fori_loop(0, NCH + 8, step, 0)

    def drain(k, carry):
        mate_copy(k).wait()
        return carry

    lax.fori_loop(0, NCH, drain, 0)


def reduce_call(gt, u):
    f32 = jnp.float32
    vm = pl.BlockSpec(memory_space=pltpu.VMEM)
    return pl.pallas_call(
        reduce_kernel,
        out_shape=pltpu.VMEM((2, NCH, ROWS, 128), f32),
        in_specs=[vm, vm],
        out_specs=vm,
        scratch_shapes=[
            pltpu.VMEM((2, 2, 2, 240, 128), f32), pltpu.VMEM((2, 2, 2, SH, 128), f32),
            pltpu.VMEM((2, 2, 2, 64, 128), f32), pltpu.VMEM((2, 2, 2, SUB, 128), f32),
            pltpu.VMEM((3, 2, 2, SUB, 128), f32), pltpu.VMEM((3, 2, 2, 64, 128), f32),
            pltpu.SemaphoreType.DMA((8, 2, 2, NCH)), pltpu.SemaphoreType.DMA((8, 2, 2, NCH)),
            pltpu.SemaphoreType.DMA((NCH,)), pltpu.SemaphoreType.DMA((NCH,)),
        ],
        compiler_params=pltpu.CompilerParams(collective_id=1, has_side_effects=True, vmem_limit_bytes=20 << 20),
        name="reduce_rows",
    )(gt, u)


def write_kernel(both, out, sem):
    c = lax.axis_index("dp") % 2
    cps = []
    for k in range(NCH):
        for j, src in enumerate((both.at[0], both.at[1])):
            r0 = (c if j == 0 else 1 - c) * 3824
            cp = pltpu.make_async_copy(src.at[k, pl.ds(0, 3824)],
                                       out.at[pl.ds(pl.multiple_of(r0, 8), 3824), pl.ds(k * 128, 128)], sem.at[k, j])
            cp.start()
            cps.append(cp)
    for cp in cps:
        cp.wait()


def write_call(both):
    vm = pl.BlockSpec(memory_space=pltpu.VMEM)
    return pl.pallas_call(
        write_kernel,
        out_shape=jax.ShapeDtypeStruct((7648, 1024), jnp.float32),
        in_specs=[vm],
        out_specs=pl.BlockSpec(memory_space=pl.ANY),
        scratch_shapes=[pltpu.SemaphoreType.DMA((NCH, 2))],
        compiler_params=pltpu.CompilerParams(vmem_limit_bytes=1 << 20),
        name="write_rows",
    )(both)


def head_norm(pre_act, ln_gain, ln_bias):
    gelu_out = jax.nn.gelu(pre_act, approximate=False)
    row_mean = jnp.mean(gelu_out, axis=-1, keepdims=True)
    centered = gelu_out - row_mean
    row_var = jnp.mean(centered * centered, axis=-1, keepdims=True)
    return centered * lax.rsqrt(row_var + LN_EPS) * ln_gain + ln_bias


def column(row):
    return jnp.transpose(jnp.broadcast_to(row, (128, 128)))


def softmax_kernel(n_valid, scale, u_own, lab_own, bias, emb, gt, u_all, small,
                   emb_v, logit, u_rx, lab_rx, stat, stats, sem_e, sem_s, sem_r, st_s, st_r):
    f32 = jnp.float32
    dp, vp = lax.axis_index("dp"), lax.axis_index("vp")
    c = dp % 2
    mate = dp + 1 - 2 * c
    peers = [(dx, dc) for dx in range(4) for dc in range(2) if (dx, dc) != (0, 0)]

    def peer(dx, dc):
        return {"vp": (vp + dx) % 4, "dp": (dp // 2) * 2 + (c + dc) % 2}

    barrier = pltpu.get_barrier_semaphore()
    for dx, dc in peers:
        pl.semaphore_signal(barrier, inc=1, device_id=peer(dx, dc), device_id_type=MESH)

    def load(i, n):
        r0 = pl.multiple_of(c * VROWS, 16) + i * BLK
        return pltpu.make_async_copy(emb.at[pl.ds(r0, n)], emb_v.at[pl.ds(i * BLK, n)], sem_e.at[i])

    n_blk = ROWS // BLK
    last = VROWS - (n_blk - 1) * BLK
    for i in range(n_blk):
        load(i, BLK if i < n_blk - 1 else last).start()
    emb_v[pl.ds(VROWS, ROWS - VROWS), :] = jnp.zeros((ROWS - VROWS, 1024), jnp.bfloat16)
    own0 = pl.multiple_of(c * TOK, TOK)
    oth0 = pl.multiple_of((1 - c) * TOK, TOK)
    u_all[pl.ds(own0, TOK), :] = u_own[...].astype(jnp.bfloat16)
    pl.semaphore_wait(barrier, len(peers))
    cp_u = pltpu.make_async_remote_copy(src_ref=u_own, dst_ref=u_rx, send_sem=sem_s.at[0], recv_sem=sem_r.at[0],
                                        device_id={"dp": mate}, device_id_type=MESH)
    cp_l = pltpu.make_async_remote_copy(src_ref=lab_own, dst_ref=lab_rx, send_sem=sem_s.at[1], recv_sem=sem_r.at[1],
                                        device_id={"dp": mate}, device_id_type=MESH)
    cp_u.start()
    cp_l.start()
    row0 = (vp * 2 * VROWS + c * VROWS).astype(f32)

    def local_labels(ref):
        v = ref[0:1, :] - row0
        return jnp.where((v >= 0) & (v < VROWS), v, -1.0)

    def half_logits(tok0, lab):
        u = u_all[pl.ds(tok0, TOK), :]
        labs = jnp.broadcast_to(lab, (8, TOK))
        sub = lax.broadcasted_iota(jnp.int32, (8, TOK), 0).astype(f32)

        def block(i, carry):
            mx, sm, lb = carry
            e = emb_v[pl.ds(pl.multiple_of(i * BLK, BLK), BLK), :]
            x = lax.dot_general(e, u, (((1,), (1,)), ((), ())), preferred_element_type=f32)
            b = jnp.concatenate([column(bias[pl.ds(i * 3 + j, 1), :]) for j in range(BLK // 128)], axis=0)
            x = x + jnp.concatenate([b] * (TOK // 128), axis=1)
            logit[pl.ds(pl.multiple_of(i * BLK, BLK), BLK), pl.ds(tok0, TOK)] = x
            x = x.reshape(BLK // 8, 8, TOK)
            top = jnp.maximum(mx, jnp.max(x, axis=0))
            sm = sm * jnp.exp(mx - top) + jnp.sum(jnp.exp(x - top[None]), axis=0)
            rel = labs - sub - (i * BLK).astype(f32)
            ids = (lax.broadcasted_iota(jnp.int32, (BLK // 8, 8, TOK), 0) * 8).astype(f32)
            lb = lb + jnp.sum(jnp.where(ids == rel[None], x, 0.0), axis=0)
            return top, sm, lb

        init = (jnp.full((8, TOK), -3e38, f32), jnp.zeros((8, TOK), f32), jnp.zeros((8, TOK), f32))
        mx, sm, lb = lax.fori_loop(0, n_blk, block, init)
        top = jnp.max(mx, axis=0, keepdims=True)
        sm = jnp.sum(sm * jnp.exp(mx - top), axis=0, keepdims=True)
        lb = jnp.sum(lb, axis=0, keepdims=True)
        stat[:, pl.ds(tok0, TOK)] = jnp.concatenate([top, sm, lb, jnp.zeros((5, TOK), f32)], axis=0)

    for i in range(n_blk):
        load(i, BLK if i < n_blk - 1 else last).wait()
    lab1 = local_labels(lab_own)
    half_logits(own0, lab1)
    cp_u.wait()
    cp_l.wait()
    u_all[pl.ds(oth0, TOK), :] = u_rx[...].astype(jnp.bfloat16)
    lab2 = local_labels(lab_rx)
    half_logits(oth0, lab2)
    cps = [pltpu.make_async_remote_copy(src_ref=stat, dst_ref=stats.at[j], send_sem=st_s.at[j], recv_sem=st_r.at[j],
                                        device_id=peer(dx, dc), device_id_type=MESH)
           for j, (dx, dc) in enumerate(peers)]
    for cp in cps:
        cp.start()
    for cp in cps:
        cp.wait()
    mine = stat[...]
    top = mine[0:1]
    for j in range(len(peers)):
        top = jnp.maximum(top, stats[j, 0:1, :])
    tot = mine[1:2] * jnp.exp(mine[0:1] - top)
    tgt = mine[2:3]
    for j in range(len(peers)):
        tot = tot + stats[j, 1:2, :] * jnp.exp(stats[j, 0:1, :] - top)
        tgt = tgt + stats[j, 2:3, :]
    norm = top + jnp.log(tot)
    lane = lax.broadcasted_iota(jnp.int32, (1, 2 * TOK), 1)
    valid = (lane % TOK) < n_valid
    diff = jnp.where(valid, norm - tgt, 0.0)
    own_lane = (lane // TOK) == c
    diff = jnp.where(own_lane, diff, 0.0)
    small[30:31, :] = sum(diff[:, j * 128:(j + 1) * 128] for j in range(8))
    norm = jnp.where(valid, norm, 3e38)
    stat[0:1, :] = norm
    stat[1:2, pl.ds(own0, TOK)] = lab1
    stat[1:2, pl.ds(oth0, TOK)] = lab2

    def grad(i, carry):
        r = pl.multiple_of(i * 128, 128)
        x = logit[pl.ds(r, 128), :]
        ids = (lax.broadcasted_iota(jnp.int32, (128, 2 * TOK), 0) + i * 128).astype(f32)
        g = (jnp.exp(x - stat[0:1, :]) - jnp.where(ids == stat[1:2, :], 1.0, 0.0)) * scale
        gt[pl.ds(r, 128), :] = g.astype(jnp.bfloat16)
        s = sum(g[:, j * 128:(j + 1) * 128] for j in range(8))
        small[pl.ds(i, 1), :] = jnp.sum(jnp.transpose(s), axis=0, keepdims=True)
        return carry

    lax.fori_loop(0, ROWS // 128, grad, 0)


def softmax_call(n_valid, scale, u_own, lab_own, bias, emb):

    f32, bf = jnp.float32, jnp.bfloat16
    vm = pl.BlockSpec(memory_space=pltpu.VMEM)
    dma = pltpu.SemaphoreType.DMA
    return pl.pallas_call(
        functools.partial(softmax_kernel, n_valid, scale),
        out_shape=(pltpu.VMEM((ROWS, 2 * TOK), bf), pltpu.VMEM((2 * TOK, 1024), bf), pltpu.VMEM((32, 128), f32)),
        in_specs=[vm, vm, vm, pl.BlockSpec(memory_space=pl.ANY)],
        out_specs=(vm, vm, vm),
        scratch_shapes=[
            pltpu.VMEM((ROWS, 1024), bf), pltpu.VMEM((ROWS, 2 * TOK), f32), pltpu.VMEM((TOK, 1024), f32),
            pltpu.VMEM((8, TOK), f32), pltpu.VMEM((8, 2 * TOK), f32), pltpu.VMEM((7, 8, 2 * TOK), f32),
            dma((ROWS // BLK,)), dma((2,)), dma((2,)), dma((7,)), dma((7,)),
        ],
        compiler_params=pltpu.CompilerParams(collective_id=0, has_side_effects=True, vmem_limit_bytes=44 << 20),
        name="softmax_rows",
    )(u_own, lab_own, bias, emb)


def solution(mesh):
    n_groups = mesh.shape["dp"]
    f32, bf = jnp.float32, jnp.bfloat16

    def local_step(hidden, mask_pos, labels, w_trans, b_trans, ln_gain, ln_bias, emb_table, b_vocab):
        n_rows, seq_len = hidden.shape[0], hidden.shape[1]
        n_masks = mask_pos.shape[1]
        n_own = n_rows * n_masks
        n_tokens = n_own * n_groups
        dp, vp = lax.axis_index("dp"), lax.axis_index("vp")
        c = dp % 2
        pos_onehot = (mask_pos[:, :, None] == jnp.arange(seq_len)[None, None, :]).astype(bf)
        masked_h = jnp.einsum("clt,cte->cle", pos_onehot, hidden, preferred_element_type=f32).astype(bf)
        masked_h = jnp.pad(masked_h.reshape(n_own, 1024), ((0, TOK - n_own), (0, 0)))
        pre_act = jnp.dot(masked_h, w_trans, preferred_element_type=f32) + b_trans
        u_norm, head_vjp = jax.vjp(head_norm, pre_act, ln_gain, ln_bias)
        u_own = u_norm.astype(bf).astype(f32)
        lab = jnp.pad(labels.reshape(n_own).astype(f32), (0, TOK - n_own), constant_values=-1e6)
        lab = jnp.broadcast_to(lab[None], (8, TOK))
        b_half = lax.dynamic_slice(b_vocab, (c * VROWS,), (VROWS,))
        bias = jnp.pad(b_half, (0, ROWS - VROWS), constant_values=-3e38).reshape(ROWS // 128, 128)
        gt, u_all, small = softmax_call(n_own, 1.0 / n_tokens, u_own, lab, bias, emb_table)
        emb_half = lax.dynamic_slice(emb_table, (c * VROWS, 0), (VROWS, 1024))
        du = lax.dot_general(gt[:VROWS], emb_half, (((0,), (0,)), ((), ())), preferred_element_type=f32)
        perm = [(i, i ^ 1) for i in range(n_groups)]
        du_mine = lax.dynamic_slice(du, (c * TOK, 0), (TOK, 1024))
        du_theirs = lax.dynamic_slice(du, ((1 - c) * TOK, 0), (TOK, 1024))
        du_block = (du_mine + lax.ppermute(du_theirs, "dp", perm)).astype(bf)
        d_unorm = lax.psum(du_block.astype(f32), "vp")
        d_pre, d_ln_gain, d_ln_bias = head_vjp(d_unorm)
        d_pre_bf = d_pre.astype(bf)
        h_part = lax.dynamic_slice(masked_h, (0, vp * 256), (TOK, 256))
        dw_part = lax.dot_general(h_part, d_pre_bf, (((0,), (0,)), ((), ())), preferred_element_type=f32)
        d_b = lax.dynamic_update_slice(jnp.zeros((8192,), f32), small[:30].reshape(ROWS)[:VROWS], (c * VROWS,)).reshape(8, 1024)
        loss = jnp.broadcast_to(jnp.sum(small[30]) / n_tokens, (1, 1024))
        packed = jnp.concatenate([dw_part, d_b, jnp.stack([jnp.sum(d_pre, axis=0), d_ln_gain, d_ln_bias]), loss], axis=0)
        packed = lax.psum(packed, "dp")
        d_w_trans = lax.all_gather(packed[:256], "vp", tiled=True)
        d_masked = jnp.dot(d_pre_bf, w_trans.T, preferred_element_type=f32).astype(bf)[:n_own].reshape(n_rows, n_masks, 1024)
        d_hidden = jnp.einsum("clt,cle->cte", pos_onehot, d_masked, preferred_element_type=f32).astype(bf)
        d_emb = write_call(reduce_call(gt, u_all))
        d_b_vocab = packed[256:264].reshape(8192)[:2 * VROWS]
        return packed[267, 0], d_hidden, d_w_trans, packed[264], packed[265], packed[266], d_emb, d_b_vocab

    in_specs = (P("dp", None, None), P("dp", None), P("dp", None), P(None, None), P(None), P(None), P(None), P("vp", None), P("vp"))
    out_specs = (P(), P("dp", None, None), P(None, None), P(None), P(None), P(None), P("vp", None), P("vp"))
    return jax.shard_map(local_step, mesh=mesh, in_specs=in_specs, out_specs=out_specs, check_vma=False)
```

```python
import functools

import jax
import jax.numpy as jnp
from jax import lax
from jax.experimental import pallas as pl
from jax.experimental.pallas import tpu as pltpu
from jax.sharding import PartitionSpec as P

MESH = pl.DeviceIdType.MESH
F32, BF = jnp.float32, jnp.bfloat16
VMEM, DMA, ds = pltpu.VMEM, pltpu.SemaphoreType.DMA, pl.ds
LN_EPS = 1e-5
HALF_SQRT, INV_SQRT_2PI = 0.7071067811865476, 0.3989422804014327
LOW, HIGH, NO_LABEL = -3e38, 3e38, -1e6
W, L, TILE = 1024, 128, 8
SEQS, SEQ, MASKS, SLOT = 6, 512, 77, 80
USED, TOK = SEQS * SLOT, 512
VROWS, ROWS, BLK = 3824, 3840, 384
N_BLK = ROWS // BLK
LAST = VROWS - (N_BLK - 1) * BLK
NCH = W // L
HALF, SH, SUB = ROWS // 2, ROWS // 8, ROWS // 32
CUT, SCUT = SH // 2, 64
SCUTS = (SCUT, SUB - SCUT)
QROWS, XROWS, XCUT = 128, 136, 72
VEC0, SMALL0, MINI = W, W + 24, 1280
MSH, MSUB = MINI // 8, MINI // 32
LOSS_ROW, N_SMALL = ROWS // L, 32
OTH0 = NCH * ROWS
DW0 = 2 * OTH0
MG0 = DW0 + 8 * W
TAIL0 = MG0 + MINI
OUT_ROWS = TAIL0 + MINI - W
NSTAGE = 8
NEAR, FAR = (1, 3), 2
AROUND = NEAR + (FAR,)
TWO, THREE = (0, 1), (0, 1, 2)


def sl(start, n):
    return ds(pl.multiple_of(start, TILE), n)


def wait_all(cps):
    for cp in cps:
        cp.wait()


def start_all(cps):
    for cp in cps:
        cp.start()


def gelu_norm(a):
    cdf = 0.5 * (1.0 + lax.erf(a * HALF_SQRT))
    g = a * cdf
    cen = g - jnp.mean(g, axis=-1, keepdims=True)
    rstd = lax.rsqrt(jnp.mean(cen * cen, axis=-1, keepdims=True) + LN_EPS)
    return cdf, rstd, cen * rstd


def dot(a, b, ca, cb):
    return lax.dot_general(a, b, (((ca,), (cb,)), ((), ())), preferred_element_type=F32)


def lanes(j):
    return ds(j * L, L)


def add_rows(dst, srcs, n, blk):
    def body(i, carry):
        r = sl(i * blk, blk)
        v = dst[r, :]
        for s in srcs:
            v = v + s[r, :]
        dst[r, :] = v
        return carry
    lax.fori_loop(0, n // blk, body, 0)


def head_kernel(scale, pos, lab_own, bias, vecs, hidden, emb, w_in, dz, aux, out,
                gt, u_all, r1, r2, r3, r4, a1, a2, part, drx, xr1, dabx, dwrx, m8, mr1, mr2,
                wbuf, zbuf, abuf, ztmp, lab_rx, stat, stats, small,
                ssem, rsem, psend, precv, sem_h, sem_w, es, er, st_s, st_r, xs, xr, ms, mr):
    dp, vp = lax.axis_index("dp"), lax.axis_index("vp")
    z, y, c = dp // 8, (dp // 2) % 4, dp % 2
    ynb = [z * 8 + ((y + d) % 4) * 2 + c for d in AROUND]
    znb = [((z + d) % 4) * 8 + y * 2 + c for d in AROUND]
    xnb = [(vp + d) % 4 for d in AROUND]
    mate = dp + 1 - 2 * c
    peers = [{"vp": v, "dp": d} for v in xnb for d in (dp, mate)] + [{"vp": vp, "dp": mate}]

    def load_hidden(b):
        r = sl(b * SEQ, SEQ)
        return pltpu.make_async_copy(hidden.at[r], gt.at[r], sem_h.at[b])

    def load_emb(i, slot, n):
        return pltpu.make_async_copy(emb.at[ds(pl.multiple_of(c * VROWS, 16) + i * BLK, n)],
                                     wbuf.at[ds(pl.multiple_of(slot * BLK, 16), n)], sem_w.at[slot])

    load_w = pltpu.make_async_copy(w_in, u_all, sem_h.at[SEQS])
    store_dz = pltpu.make_async_copy(u_all.at[ds(0, TOK)], dz, sem_h.at[0])
    load_w_again = pltpu.make_async_copy(w_in, gt.at[ds(0, W)], sem_h.at[SEQS])
    for b in range(SEQS):
        load_hidden(b).start()
    load_w.start()
    load_emb(0, 0, BLK).start()

    barrier = pltpu.get_barrier_semaphore()
    greet = peers + [{"dp": d} for d in ynb + znb]
    for d in greet:
        pl.semaphore_signal(barrier, inc=1, device_id=d, device_id_type=MESH)

    def remote(src, dst, send, recv, dev):
        return pltpu.make_async_remote_copy(src_ref=src, dst_ref=dst, send_sem=send, recv_sem=recv,
                                            device_id=dev, device_id_type=MESH)

    def to_mate(src, dst, i):
        return remote(src, dst, es.at[i], er.at[i], {"dp": mate})

    def to_x(src, dst, i, d):
        return remote(src, dst, xs.at[i, d], xr.at[i, d], {"vp": xnb[d]})

    c_u = [to_mate(part, drx, 0), to_mate(lab_own, lab_rx, 1)]
    own0 = pl.multiple_of(c * TOK, TOK)
    oth0 = pl.multiple_of((1 - c) * TOK, TOK)

    load_w.wait()

    def transform(b, carry):
        load_hidden(b).wait()
        where = jnp.broadcast_to(pos[ds(b, 1), :], (SEQ, L))
        hot = jnp.where(where == lax.broadcasted_iota(jnp.int32, (SEQ, L), 0), 1.0, 0.0).astype(BF)
        zrow = dot(hot, gt[sl(b * SEQ, SEQ), :], 0, 0)[:SLOT].astype(BF)
        ztmp[...] = zrow
        r = sl(b * SLOT, SLOT)
        zbuf[r, :] = ztmp[:, ds(pl.multiple_of(vp * 2 * L, L), 2 * L)]
        a = dot(zrow, u_all[...], 1, 0) + vecs[0:1, :]
        dabx[r, :] = a
        _, _, xhat = gelu_norm(a)
        part[r, :] = (xhat * vecs[1:2, :] + vecs[2:3, :]).astype(BF).astype(F32)
        return carry

    lax.fori_loop(0, SEQS, transform, 0)
    zbuf[ds(USED, TOK - USED), :] = jnp.zeros((TOK - USED, 2 * L), BF)
    part[ds(USED, TOK - USED), :] = jnp.zeros((TOK - USED, W), F32)
    dabx[ds(USED, TOK - USED), :] = jnp.zeros((TOK - USED, W), F32)
    abuf[...] = dabx[sl(vp * QROWS, QROWS), :]
    u_all[ds(own0, TOK), :] = part[...].astype(BF)
    pl.semaphore_wait(barrier, len(greet))
    start_all(c_u)

    def stream(body, init, again):
        def blk(i, carry):
            slot = i % 2
            for at, n in ((i + 2 < N_BLK, BLK), (i + 2 == N_BLK, LAST)):
                pl.when(at)(lambda: load_emb(i + 1, 1 - slot, n).start())
            if again:
                pl.when(i + 1 == N_BLK)(lambda: load_emb(0, 1 - slot, BLK).start())
            for at, n in ((i + 1 < N_BLK, BLK), (i + 1 == N_BLK, LAST)):
                pl.when(at)(lambda: load_emb(i, slot, n).wait())
            return body(i, wbuf[ds(pl.multiple_of(slot * BLK, 16), BLK), :], carry)
        return lax.fori_loop(0, N_BLK, blk, init)

    row0 = (vp * 2 * VROWS + c * VROWS).astype(F32)

    def local_labels(ref):
        v = ref[0:1, :] - row0
        return jnp.where((v >= 0) & (v < VROWS), v, -1.0)

    def logits(tok0, lab, again):
        u = u_all[ds(tok0, TOK), :]
        labs = jnp.broadcast_to(lab, (TILE, TOK)) - lax.broadcasted_iota(jnp.int32, (TILE, TOK), 0).astype(F32)

        def block(i, e, carry):
            mx, sm, lb = carry
            x = dot(e, u, 1, 1)
            col = [jnp.transpose(jnp.broadcast_to(bias[ds(c * LOSS_ROW + i * (BLK // L) + j, 1), :], (L, L)))
                   for j in range(BLK // L)]
            x = x + jnp.concatenate([jnp.concatenate(col, axis=0)] * (TOK // L), axis=1)
            for j in range(TOK // L):
                out[sl((tok0 // L + j) * ROWS + i * BLK, BLK), :] = x[:, j * L:(j + 1) * L]
            x = x.reshape(BLK // TILE, TILE, TOK)
            top = jnp.maximum(mx, jnp.max(x, axis=0))
            sm = sm * jnp.exp(mx - top) + jnp.sum(jnp.exp(x - top[None]), axis=0)
            ids = (lax.broadcasted_iota(jnp.int32, (BLK // TILE, TILE, TOK), 0) * TILE).astype(F32)
            lb = lb + jnp.sum(jnp.where(ids == (labs - (i * BLK).astype(F32))[None], x, 0.0), axis=0)
            return top, sm, lb

        zero = jnp.zeros((TILE, TOK), F32)
        mx, sm, lb = stream(block, (jnp.full((TILE, TOK), LOW, F32), zero, zero), again)
        top = jnp.max(mx, axis=0, keepdims=True)
        sm = jnp.sum(sm * jnp.exp(mx - top), axis=0, keepdims=True)
        lb = jnp.sum(lb, axis=0, keepdims=True)
        stat[:, ds(tok0, TOK)] = jnp.concatenate([top, sm, lb, jnp.zeros((TILE - 3, TOK), F32)], axis=0)

    lab1 = local_labels(lab_own)
    logits(own0, lab1, True)
    wait_all(c_u)
    u_all[ds(oth0, TOK), :] = drx[...].astype(BF)
    lab2 = local_labels(lab_rx)
    logits(oth0, lab2, True)
    c_st = [remote(stat, stats.at[j], st_s.at[j], st_r.at[j], d) for j, d in enumerate(peers)]
    start_all(c_st)
    wait_all(c_st)
    mx, sm, lb = (jnp.concatenate([stat[i:i + 1, :]] + [stats[j, i:i + 1, :] for j in range(len(peers))], axis=0)
                  for i in THREE)
    top = jnp.max(mx, axis=0, keepdims=True)
    norm = top + jnp.log(jnp.sum(sm * jnp.exp(mx - top), axis=0, keepdims=True))
    diff = norm - jnp.sum(lb, axis=0, keepdims=True)
    stat[0:1, :] = norm
    stat[1:2, :] = diff
    own_real = lab_own[0:1, :] >= 0
    diff = jnp.where(own_real, stat[1:2, ds(own0, TOK)], 0.0)
    small[ds(LOSS_ROW, 1), :] = sum(diff[:, j * L:(j + 1) * L] for j in range(TOK // L))
    small[ds(LOSS_ROW + 1, 1), :] = jnp.zeros((1, L), F32)
    for t0, ref, lab in ((own0, lab_own, lab1), (oth0, lab_rx, lab2)):
        stat[0:1, ds(t0, TOK)] = jnp.where(ref[0:1, :] >= 0, stat[0:1, ds(t0, TOK)], HIGH)
        stat[1:2, ds(t0, TOK)] = lab

    def grad(i, carry):
        ids = (lax.broadcasted_iota(jnp.int32, (L, L), 0) + i * L).astype(F32)
        s = jnp.zeros((L, L), F32)
        for j in range(2 * TOK // L):
            x = out[sl(j * ROWS + i * L, L), :]
            g = (jnp.exp(x - stat[0:1, lanes(j)]) - jnp.where(ids == stat[1:2, lanes(j)], 1.0, 0.0)) * scale
            gt[ds(pl.multiple_of(i * L, L), L), lanes(j)] = g.astype(BF)
            s = s + g
        small[ds(i, 1), :] = jnp.sum(jnp.transpose(s), axis=0, keepdims=True)
        return carry

    lax.fori_loop(0, ROWS // L, grad, 0)

    def rows(k, start, n):
        return out.at[sl(k * ROWS + start, n)]

    halves = []
    for b, p, pn, q, qn in ((0, y, ynb, z, znb), (HALF, z, znb, y, ynb)):
        pc, qc = ([(t + d) % 4 * n for d in NEAR] for t, n in ((p, SH), (q, SUB)))
        halves.append((b, pn, qn, pc, qc, b + (p + FAR) % 4 * SH, b + p * SH, (q + FAR) % 4 * SUB, q * SUB))

    def stage_copies(st, k):
        cps = []
        for h, (b, pn, qn, pc, qc, po, b2, qo, q0) in enumerate(halves):
            for d in TWO:
                n = SCUTS[d]
                if st == 0:
                    a = rows(k, po + d * CUT, CUT), r1.at[k % 2, h, d], pn
                elif st == 1:
                    a = rows(k, b + pc[d], SH), r2.at[k % 2, h, d], pn
                elif st == 2:
                    a = rows(k, b2 + qo + d * SCUT, n), r3.at[k % 2, h, d, ds(0, n)], qn
                elif st == 3:
                    a = rows(k, b2 + qc[d], SUB), r4.at[k % 2, h, d], qn
                elif st == 4:
                    a = rows(k, b2 + q0, SUB), a1.at[k % 3, h, d], qn
                elif st == 5:
                    a = a1.at[k % 3, h, d, ds(d * SCUT, n)], a2.at[k % 3, h, d, ds(0, n)], qn
                elif st == 6:
                    a = rows(k, b2, SH), rows(k, b2, SH), pn
                else:
                    s = rows(k, b + pc[1 - d] + d * CUT, CUT)
                    a = s, s, pn
                src, dst, nb = a
                cps.append(remote(src, dst, ssem.at[st, h, d, k], rsem.at[st, h, d, k], {"dp": nb[d]}))
        return cps

    def mate_copy(k):
        return remote(rows(k, 0, ROWS), rows(k, OTH0, ROWS), psend.at[k], precv.at[k], {"dp": mate})

    def stage(st, k):
        if st == 0:
            def mm(i, carry):
                rows(k, i * SH, SH)[...] = dot(gt[ds(pl.multiple_of(i * SH, 16), SH), :],
                                               u_all[:, ds(pl.multiple_of(k * L, L), L)], 1, 0)
                return carry
            lax.fori_loop(0, ROWS // SH, mm, 0)
        else:
            wait_all(stage_copies(st - 1, k))
            for h, (b, pn, qn, pc, qc, po, b2, qo, q0) in enumerate(halves):
                both = lambda r: [r.at[k % 2, h, d] for d in TWO]
                if st == 2:
                    add_rows(rows(k, b2, SH), both(r2), SH, SLOT)
                elif st == 4:
                    add_rows(rows(k, b2 + q0, SUB), both(r4), SUB, SUB)
                for d in TWO:
                    n = SCUTS[d]
                    if st == 1:
                        add_rows(rows(k, b + pc[d] + d * CUT, CUT), [r1.at[k % 2, h, d]], CUT, SLOT)
                    elif st == 3:
                        add_rows(rows(k, b2 + qc[d] + d * SCUT, n), [r3.at[k % 2, h, d]], n, n)
                    elif st == 5:
                        rows(k, b2 + qc[1 - d], SUB)[...] = a1[k % 3, h, d]
                    elif st == 6:
                        rows(k, b2 + qo + d * SCUT, n)[...] = a2[k % 3, h, d, ds(0, n)]
        if st < NSTAGE:
            start_all(stage_copies(st, k))
        else:
            mate_copy(k).start()

    xp, xm, xo = xnb

    def qrow(q, o, n):
        return sl(q * QROWS + o, n)

    def arow(q, o, n):
        return sl(q * XROWS + o, n)

    def same(ref, r):
        return ref.at[r], ref.at[r]

    def dwrow(j, o, n):
        return sl(DW0 + j * W + o, n)

    XTWO = ((xo, 0), (xo, QROWS // 2))
    c_du = [to_mate(part, drx, 2)]
    c_x1 = [to_x(drx.at[qrow(q, o, QROWS // 2)], xr1.at[d], 0, d) for d, (q, o) in enumerate(XTWO)]
    c_x2 = [to_x(drx.at[qrow(xnb[d], 0, QROWS)], part.at[ds(d * QROWS, QROWS)], 1, d) for d in TWO]
    c_x3 = [to_x(*same(dabx, arow(vp, 0, XROWS)), 2, d) for d in TWO]
    c_x4 = [to_x(*same(dabx, arow(q, o, n)), 3, d)
            for d, (q, o, n) in enumerate(((xm, 0, XCUT), (xp, XCUT, XROWS - XCUT)))]
    c_dw = [to_mate(part.at[qrow(1 - c, 0, QROWS)], dwrx.at[ds(0, QROWS)], 3),
            to_mate(part.at[ds(2 * QROWS, TILE)], dwrx.at[ds(QROWS, TILE)], 4)]
    c_w1 = [to_x(*same(out, dwrow(vp, 0, W)), 4, d) for d in TWO]
    c_w2 = [to_x(*same(out, dwrow(q, d * (W // 2), W // 2)), 5, d) for d, q in enumerate((xm, xp))]
    c_w3 = [to_mate(out.at[ds(DW0, 4 * W)], out.at[ds(DW0 + 4 * W, 4 * W)], 5),
            to_mate(out.at[ds(MG0 + W, MINI - W)], out.at[ds(TAIL0, MINI - W)], 6)]

    def du_part(col0, dst, again):
        def block(i, e, carry):
            dst[...] += dot(gt[ds(pl.multiple_of(i * BLK, L), BLK), ds(col0, TOK)], e, 0, 0)
            return carry
        stream(block, 0, again)

    def du_theirs():
        part[...] = jnp.zeros((TOK, W), F32)
        du_part(oth0, part, True)
        start_all(c_du)

    def du_mine():
        wait_all(c_du)
        du_part(own0, drx, False)

        def rnd(i, carry):
            r = sl(i * SCUT, SCUT)
            drx[r, :] = drx[r, :].astype(BF).astype(F32)
            return carry

        lax.fori_loop(0, TOK // SCUT, rnd, 0)
        start_all(c_x1)

    def du_near():
        wait_all(c_x1)
        for d, o in ((0, 0), (1, QROWS // 2)):
            drx[qrow(xnb[d], o, QROWS // 2), :] += xr1[d]
        start_all(c_x2)

    def norm_back():
        wait_all(c_x2)

        def block(i, sums):
            r = sl(i * 2 * TILE, 2 * TILE)
            a = abuf[r, :]
            dun = drx[qrow(vp, i * 2 * TILE, 2 * TILE), :] + part[r, :] + part[sl(QROWS + i * 2 * TILE, 2 * TILE), :]
            cdf, rstd, xhat = gelu_norm(a)
            dx = dun * vecs[1:2, :]
            dg = rstd * (dx - jnp.mean(dx, axis=-1, keepdims=True) - xhat * jnp.mean(dx * xhat, axis=-1, keepdims=True))
            da = dg * (cdf + a * jnp.exp(-0.5 * a * a) * INV_SQRT_2PI)
            dabx[arow(vp, i * 2 * TILE, 2 * TILE), :] = da.astype(BF).astype(F32)
            return tuple(s + t[:TILE] + t[TILE:] for s, t in zip(sums, (da, dun * xhat, dun)))

        sums = lax.fori_loop(0, QROWS // (2 * TILE), block, (jnp.zeros((TILE, W), F32),) * 3)
        sums = [jnp.sum(t, axis=0, keepdims=True) for t in sums]
        dabx[arow(vp, QROWS, TILE), :] = jnp.concatenate(sums + [jnp.zeros((TILE - 3, W), F32)], axis=0)
        start_all(c_x3)

    def pass_on():
        wait_all(c_x3)
        start_all(c_x4)

    def dab(q):
        return dabx[arow(q, 0, QROWS), :].astype(BF)

    def weight_grad():
        wait_all(c_x4)
        part[ds(0, 2 * QROWS), :] = sum(dot(zbuf[qrow(q, 0, QROWS), :], dab(q), 0, 0) for q in range(4))
        part[ds(2 * QROWS, TILE), :] = sum(dabx[arow(q, QROWS, TILE), :] for q in range(4))
        start_all(c_dw)

    def input_grad():
        load_w_again.start()
        wait_all(c_dw)
        for j in range(W // L):
            m8[lanes(j), :] = part[qrow(c, 0, QROWS), lanes(j)] + dwrx[ds(0, QROWS), lanes(j)]
            v = part[ds(2 * QROWS, TILE), lanes(j)] + dwrx[ds(QROWS, TILE), lanes(j)]
            for i in THREE:
                m8[ds(VEC0 + i * TILE + j, 1), :] = v[i:i + 1]
        m8[ds(SMALL0, N_SMALL), :] = small[...]
        m8[ds(SMALL0 + N_SMALL, MINI - SMALL0 - N_SMALL), :] = jnp.zeros((MINI - SMALL0 - N_SMALL, L), F32)
        start_all(mini_copies(0))

    mini = ((0, y, ynb, z, znb), (MINI // 2, z, znb, y, ynb))

    def mini_copies(st):
        cps = []
        for h, (b, p, pn, q, qn) in enumerate(mini):
            b2 = b + p * MSH
            for d, off in enumerate(AROUND):
                if st == 0:
                    a = m8.at[sl(b + (p + off) % 4 * MSH, MSH)], mr1.at[h, d], pn
                elif st == 1:
                    a = m8.at[sl(b2 + (q + off) % 4 * MSUB, MSUB)], mr2.at[h, d], qn
                elif st == 2:
                    a = *same(out, sl(MG0 + b2 + q * MSUB, MSUB)), qn
                else:
                    a = *same(out, sl(MG0 + b2, MSH)), pn
                src, dst, nb = a
                cps.append(remote(src, dst, ms.at[st, h, d], mr.at[st, h, d], {"dp": nb[d]}))
        return cps

    def mini_first():
        load_w_again.wait()
        for q in range(4):
            u_all[qrow(q, 0, QROWS), :] = dot(dab(q), gt[ds(0, W), :], 1, 1).astype(BF)
        store_dz.start()
        wait_all(mini_copies(0))
        for h, (b, p, pn, q, qn) in enumerate(mini):
            r = sl(b + p * MSH, MSH)
            m8[r, :] = m8[r, :] + sum(mr1[h, d] for d in THREE)
        start_all(mini_copies(1))

    def mini_second():
        store_dz.wait()
        wait_all(mini_copies(1))
        for h, (b, p, pn, q, qn) in enumerate(mini):
            r = b + p * MSH + q * MSUB
            out[sl(MG0 + r, MSUB), :] = m8[sl(r, MSUB), :] + sum(mr2[h, d] for d in THREE)
        start_all(mini_copies(2))

    def mini_third():
        wait_all(mini_copies(2))
        start_all(mini_copies(3))

    def weight_x():
        wait_all(mini_copies(3))
        out[dwrow(vp, 0, W), :] = out[ds(MG0, W), :]
        start_all(c_w1)

    def weight_on():
        wait_all(c_w1)
        start_all(c_w2)

    def weight_mate():
        wait_all(c_w2)
        start_all(c_w3)

    pieces = (du_theirs, du_mine, du_near, norm_back, pass_on, weight_grad, input_grad,
              mini_first, mini_second, mini_third, weight_x, weight_on, weight_mate)

    def step(t, carry):
        for st in reversed(range(NSTAGE + 1)):
            k = t - st
            pl.when((k >= 0) & (k < NCH))(functools.partial(stage, st, k))
        for at, piece in enumerate(pieces):
            pl.when(t == at + 1)(piece)
        return carry

    lax.fori_loop(0, NCH + NSTAGE, step, 0)

    def drain(k, carry):
        mate_copy(k).wait()
        return carry

    lax.fori_loop(0, NCH, drain, 0)
    wait_all(c_w3)
    save = [pltpu.make_async_copy(out.at[ds(r, MINI - W)], aux.at[j], sem_w.at[j]) for j, r in enumerate((MG0 + W, TAIL0))]
    start_all(save)
    wait_all(save)


def head_call(scale, pos, lab, bias, vecs, hidden, emb, w_in):
    vm, hbm = (pl.BlockSpec(memory_space=s) for s in (VMEM, pltpu.HBM))
    pair = (2, 2)
    sems = [(NSTAGE,) + pair + (NCH,)] * 2 + [(NCH,)] * 2 + [(SEQS + 1,), pair[:1]] + [(7,)] * 4 + [(6, 2)] * 2 + [(4, 2, 3)] * 2
    return pl.pallas_call(
        functools.partial(head_kernel, scale),
        out_shape=(jax.ShapeDtypeStruct((TOK, W), BF), jax.ShapeDtypeStruct((2, MINI - W, L), F32), VMEM((OUT_ROWS, L), F32)),
        in_specs=[vm] * 4 + [hbm] * 3,
        out_specs=(hbm, hbm, vm),
        scratch_shapes=[
            VMEM((ROWS, 2 * TOK), BF), VMEM((2 * TOK, W), BF),
            VMEM((2,) + pair + (CUT, L), F32), VMEM((2,) + pair + (SH, L), F32), VMEM((2,) + pair + (SCUT, L), F32),
            VMEM((2,) + pair + (SUB, L), F32), VMEM((3,) + pair + (SUB, L), F32), VMEM((3,) + pair + (SCUT, L), F32),
            VMEM((TOK, W), F32), VMEM((TOK, W), F32), VMEM((2, QROWS // 2, W), F32),
            VMEM((4 * XROWS, W), F32), VMEM((XROWS, W), F32), VMEM((MINI, L), F32), VMEM((2, 3, MSH, L), F32),
            VMEM((2, 3, MSUB, L), F32), VMEM((2 * BLK, W), BF), VMEM((TOK, 2 * L), BF), VMEM((QROWS, W), F32),
            VMEM((SLOT, W), BF), VMEM((TILE, TOK), F32), VMEM((TILE, 2 * TOK), F32), VMEM((7, TILE, 2 * TOK), F32),
            VMEM((N_SMALL, L), F32),
        ] + [DMA(s) for s in sems],
        compiler_params=pltpu.CompilerParams(collective_id=0, has_side_effects=True, vmem_limit_bytes=30560000),
        name="mlm_head",
    )(pos, lab, bias, vecs, hidden, emb, w_in)


def write_kernel(res, pos_in, dz_in, d_emb, d_w, d_hid, hid, pos, dz, sem, sem_w, sem_h, sem_i):
    c = lax.axis_index("dp") % 2
    cps = []
    for j, core in enumerate((c, 1 - c)):
        for k in range(NCH):
            cps.append(pltpu.make_async_copy(
                res.at[ds(j * OTH0 + k * ROWS, VROWS)], d_emb.at[sl(core * VROWS, VROWS), lanes(k)], sem.at[k, j]))
            for x in range(4):
                cps.append(pltpu.make_async_copy(
                    res.at[ds(DW0 + (j * 4 + x) * W + k * L, L)],
                    d_w.at[sl(x * 2 * L + core * L, L), lanes(k)], sem_w.at[k, j, x]))
    loads = [pltpu.make_async_copy(src, dst, sem_i.at[j]) for j, (src, dst) in enumerate(((pos_in, pos), (dz_in, dz)))]
    start_all(loads)
    start_all(cps)
    wait_all(loads)
    for b in range(SEQS):
        where = jnp.broadcast_to(pos[b:b + 1, :], (SEQ, L))
        hot = jnp.where(where == lax.broadcasted_iota(jnp.int32, (SEQ, L), 0), 1.0, 0.0).astype(BF)
        rows = jnp.concatenate([dz[b * SLOT:(b + 1) * SLOT, :], jnp.zeros((L - SLOT, W), BF)], axis=0)
        r = ds(b * SEQ, SEQ)
        hid[r, :] = dot(hot, rows, 1, 0).astype(BF)
        cp = pltpu.make_async_copy(hid.at[r], d_hid.at[r], sem_h.at[b])
        cp.start()
        cps.append(cp)
    wait_all(cps)


def write_call(res, pos, dz):
    vm, hbm = (pl.BlockSpec(memory_space=s) for s in (VMEM, pltpu.HBM))
    return pl.pallas_call(
        write_kernel,
        out_shape=tuple(jax.ShapeDtypeStruct(s, t) for s, t in (
            ((2 * VROWS, W), F32), ((W, W), F32), ((SEQS * SEQ, W), BF))),
        in_specs=[vm, hbm, hbm],
        out_specs=(hbm,) * 3,
        scratch_shapes=[VMEM((SEQS * SEQ, W), BF), VMEM((TILE, L), jnp.int32), VMEM((TOK, W), BF), DMA((NCH, 2)), DMA((NCH, 2, 4)),
                        DMA((SEQS,)), DMA((2,))],
        compiler_params=pltpu.CompilerParams(vmem_limit_bytes=16 << 20),
        name="write_rows",
    )(res, *(pltpu.with_memory_space_constraint(t, pltpu.HBM) for t in (pos, dz)))


def solution(mesh):
    n_groups = mesh.shape["dp"]

    def local_step(hidden, mask_pos, labels, w_trans, b_trans, ln_gain, ln_bias, emb_table, b_vocab):
        n_rows, seq_len, width = hidden.shape
        n_masks = mask_pos.shape[1]
        n_tokens = n_rows * n_masks * n_groups
        pos = jnp.pad(mask_pos, ((0, TILE - n_rows), (0, L - n_masks)), constant_values=-1)
        lab = jnp.pad(labels.astype(F32), ((0, 0), (0, SLOT - n_masks)), constant_values=NO_LABEL).reshape(1, USED)
        lab = jnp.broadcast_to(jnp.pad(lab, ((0, 0), (0, TOK - USED)), constant_values=NO_LABEL), (TILE, TOK))
        bias = jnp.pad(b_vocab.reshape(2, VROWS), ((0, 0), (0, ROWS - VROWS)), constant_values=LOW).reshape(2 * LOSS_ROW, L)
        vecs = jnp.stack([b_trans, ln_gain, ln_bias])
        dz, aux, res = head_call(1.0 / n_tokens, pos, lab, bias, vecs, hidden.reshape(n_rows * seq_len, width), emb_table, w_trans)
        d_emb, d_w_trans, d_hidden = write_call(res, pos, dz)
        aux, d_w_trans = lax.optimization_barrier((aux, d_w_trans))
        first = SMALL0 - VEC0
        vec = aux[0, :first].reshape(3, width)
        small = aux[:, first:first + N_SMALL]
        mlm_loss = jnp.sum(small[:, LOSS_ROW]) / n_tokens
        db = small.reshape(2, N_SMALL * L)[:, :VROWS]
        d_b_vocab = jnp.where(lax.axis_index("dp") % 2 == 0, db, db[::-1]).reshape(2 * VROWS)
        return (mlm_loss, d_hidden.reshape(hidden.shape), d_w_trans, vec[0], vec[1], vec[2], d_emb, d_b_vocab)

    in_specs = (P("dp", None, None), P("dp", None), P("dp", None), P(None, None), P(None), P(None), P(None), P("vp", None), P("vp"))
    out_specs = (P(), P("dp", None, None), P(None, None), P(None), P(None), P(None), P("vp", None), P("vp"))
    return jax.shard_map(local_step, mesh=mesh, in_specs=in_specs, out_specs=out_specs, check_vma=False)
```

```python
import functools

import jax
import jax.numpy as jnp
from jax import lax
from jax.experimental import pallas as pl
from jax.experimental.pallas import tpu as pltpu
from jax.sharding import PartitionSpec as P

MESH = pl.DeviceIdType.MESH
F32, BF = jnp.float32, jnp.bfloat16
VMEM, DMA, ds = pltpu.VMEM, pltpu.SemaphoreType.DMA, pl.ds
LN_EPS = 1e-5
HALF_SQRT, INV_SQRT_2PI = 0.7071067811865476, 0.3989422804014327
LOW, HIGH, NO_LABEL = -3e38, 3e38, -1e6
W, L, TILE = 1024, 128, 8
SEQS, SEQ, MASKS, SLOT = 6, 512, 77, 80
USED, TOK = SEQS * SLOT, 512
VROWS, ROWS, BLK = 3824, 3840, 384
N_BLK = ROWS // BLK
LAST = VROWS - (N_BLK - 1) * BLK
NCH = W // L
HALF, SH, SUB = ROWS // 2, ROWS // 8, ROWS // 32
CUT, SCUT = SH // 2, 64
SCUTS = (SCUT, SUB - SCUT)
QROWS, XROWS, XCUT = 128, 136, 72
VEC0, SMALL0, MINI = W, W + 24, 1280
MSH, MSUB = MINI // 8, MINI // 32
LOSS_ROW, N_SMALL = ROWS // L, 32
OTH0 = NCH * ROWS
DW0 = 2 * OTH0
MG0 = DW0 + 8 * W
TAIL0 = MG0 + MINI
OUT_ROWS = TAIL0 + MINI - W
NSTAGE = 8
NEAR, FAR = (1, 3), 2
AROUND = NEAR + (FAR,)
TWO, THREE = (0, 1), (0, 1, 2)


def sl(start, n):
    return ds(pl.multiple_of(start, TILE), n)


def wait_all(cps):
    for cp in cps:
        cp.wait()


def start_all(cps):
    for cp in cps:
        cp.start()


def gelu_norm(a):
    cdf = 0.5 * (1.0 + lax.erf(a * HALF_SQRT))
    g = a * cdf
    cen = g - jnp.mean(g, axis=-1, keepdims=True)
    rstd = lax.rsqrt(jnp.mean(cen * cen, axis=-1, keepdims=True) + LN_EPS)
    return cdf, rstd, cen * rstd


def dot(a, b, ca, cb):
    return lax.dot_general(a, b, (((ca,), (cb,)), ((), ())), preferred_element_type=F32)


def lanes(j):
    return ds(j * L, L)


def add_rows(dst, srcs, n, blk):
    def body(i, carry):
        r = sl(i * blk, blk)
        v = dst[r, :]
        for s in srcs:
            v = v + s[r, :]
        dst[r, :] = v
        return carry
    lax.fori_loop(0, n // blk, body, 0)


def head_kernel(scale, pos_in, lab_in, b_in, b_trans, ln_gain, ln_bias, hidden, emb, w_in, dz, aux, out,
                gt, u_all, r1, r2, r3, r4, a1, a2, part, drx, xr1, dabx, dwrx, m8, mr1, mr2,
                wbuf, zbuf, abuf, pos, lab_own, bias, lab_rx, stat, stats, small,
                ssem, rsem, psend, precv, sem_h, sem_w, es, er, st_s, st_r, xs, xr, ms, mr):
    dp, vp = lax.axis_index("dp"), lax.axis_index("vp")
    z, y, c = dp // 8, (dp // 2) % 4, dp % 2
    ynb = [z * 8 + ((y + d) % 4) * 2 + c for d in AROUND]
    znb = [((z + d) % 4) * 8 + y * 2 + c for d in AROUND]
    xnb = [(vp + d) % 4 for d in AROUND]
    mate = dp + 1 - 2 * c
    peers = [{"vp": v, "dp": d} for v in xnb for d in (dp, mate)] + [{"vp": vp, "dp": mate}]

    def load_hidden(b):
        r = sl(b * SEQ, SEQ)
        return pltpu.make_async_copy(hidden.at[r], gt.at[r], sem_h.at[b])

    def load_emb(i, slot, n):
        return pltpu.make_async_copy(emb.at[ds(pl.multiple_of(c * VROWS, 16) + i * BLK, n)],
                                     wbuf.at[ds(pl.multiple_of(slot * BLK, 16), n)], sem_w.at[slot])

    load_w = pltpu.make_async_copy(w_in, u_all, sem_h.at[SEQS])
    store_dz = pltpu.make_async_copy(u_all.at[ds(0, TOK)], dz, sem_h.at[0])
    load_w_again = pltpu.make_async_copy(w_in, gt.at[ds(0, W)], sem_h.at[SEQS])
    for b in range(SEQS):
        load_hidden(b).start()
    load_w.start()
    load_emb(0, 0, BLK).start()

    barrier = pltpu.get_barrier_semaphore()
    greet = peers + [{"dp": d} for d in ynb + znb]
    for d in greet:
        pl.semaphore_signal(barrier, inc=1, device_id=d, device_id_type=MESH)

    def remote(src, dst, send, recv, dev):
        return pltpu.make_async_remote_copy(src_ref=src, dst_ref=dst, send_sem=send, recv_sem=recv,
                                            device_id=dev, device_id_type=MESH)

    def to_mate(src, dst, i):
        return remote(src, dst, es.at[i], er.at[i], {"dp": mate})

    def to_x(src, dst, i, d):
        return remote(src, dst, xs.at[i, d], xr.at[i, d], {"vp": xnb[d]})

    c_u = [to_mate(part, drx, 0), to_mate(lab_own, lab_rx, 1)]
    own0 = pl.multiple_of(c * TOK, TOK)
    oth0 = pl.multiple_of((1 - c) * TOK, TOK)

    pos[...] = jnp.full((TILE, L), -1, jnp.int32)
    pos[ds(0, SEQS), ds(0, MASKS)] = pos_in[...]
    lane = lax.broadcasted_iota(jnp.int32, (L, TOK), 1)
    seq = sum((lane >= b * SLOT).astype(jnp.int32) for b in range(1, SEQS))
    slot = lane - seq * SLOT
    place = jnp.where(slot == lax.broadcasted_iota(jnp.int32, (L, TOK), 0), 1.0, 0.0).astype(BF)[:MASKS]
    high, low = lab_in[...] >> 8, lab_in[...] & 255
    spread = dot(high.astype(F32).astype(BF), place, 1, 0) * 256.0 + dot(low.astype(F32).astype(BF), place, 1, 0)
    row = lax.broadcasted_iota(jnp.int32, (SEQS, TOK), 0)
    lab = jnp.sum(jnp.where(row == seq[:SEQS], spread, 0.0), axis=0, keepdims=True)
    lab = jnp.where(slot[:1] < MASKS, lab, NO_LABEL)
    lab_own[...] = jnp.broadcast_to(lab, (TILE, TOK))
    rest = VROWS % L
    for core in TWO:
        @pl.when(c == core)
        def _():
            for i in range(VROWS // L):
                bias[ds(i, 1), :] = b_in[:, core * VROWS + i * L:core * VROWS + (i + 1) * L]
            bias[ds(LOSS_ROW - 1, 1), :] = jnp.full((1, L), LOW, F32)
            bias[ds(LOSS_ROW - 1, 1), ds(0, rest)] = b_in[:, (core + 1) * VROWS - rest:(core + 1) * VROWS]

    z0 = SEQS * SEQ

    def gather(b, carry):
        load_hidden(b).wait()
        where = jnp.broadcast_to(pos[ds(b, 1), :], (SEQ, L))
        hot = jnp.where(where == lax.broadcasted_iota(jnp.int32, (SEQ, L), 0), 1.0, 0.0).astype(BF)
        gt[ds(pl.multiple_of(z0 + b * SLOT, 16), SLOT), :] = dot(hot, gt[sl(b * SEQ, SEQ), :], 0, 0)[:SLOT].astype(BF)
        return carry

    gt[ds(z0 + USED, TOK - USED), :] = jnp.zeros((TOK - USED, W), BF)
    lax.fori_loop(0, SEQS, gather, 0)
    load_w.wait()
    zbuf[...] = gt[ds(z0, TOK), ds(pl.multiple_of(vp * 2 * L, L), 2 * L)]

    def transform(i, carry):
        r = sl(i * 2 * L, 2 * L)
        dabx[r, :] = dot(gt[ds(pl.multiple_of(z0 + i * 2 * L, L), 2 * L), :], u_all[...], 1, 0) + b_trans[...]
        return carry

    lax.fori_loop(0, TOK // (2 * L), transform, 0)

    def norm(i, carry):
        r = sl(i * 4 * TILE, 4 * TILE)
        _, _, xhat = gelu_norm(dabx[r, :])
        part[r, :] = (xhat * ln_gain[...] + ln_bias[...]).astype(BF).astype(F32)
        return carry

    lax.fori_loop(0, TOK // (4 * TILE), norm, 0)
    abuf[...] = dabx[sl(vp * QROWS, QROWS), :]
    u_all[ds(own0, TOK), :] = part[...].astype(BF)
    pl.semaphore_wait(barrier, len(greet))
    start_all(c_u)

    def stream(body, init, again):
        def blk(i, carry):
            slot = i % 2
            for at, n in ((i + 2 < N_BLK, BLK), (i + 2 == N_BLK, LAST)):
                pl.when(at)(lambda: load_emb(i + 1, 1 - slot, n).start())
            if again:
                pl.when(i + 1 == N_BLK)(lambda: load_emb(0, 1 - slot, BLK).start())
            for at, n in ((i + 1 < N_BLK, BLK), (i + 1 == N_BLK, LAST)):
                pl.when(at)(lambda: load_emb(i, slot, n).wait())
            return body(i, wbuf[ds(pl.multiple_of(slot * BLK, 16), BLK), :], carry)
        return lax.fori_loop(0, N_BLK, blk, init)

    row0 = (vp * 2 * VROWS + c * VROWS).astype(F32)

    def local_labels(ref):
        v = ref[0:1, :] - row0
        return jnp.where((v >= 0) & (v < VROWS), v, -1.0)

    def logits(tok0, again):
        u = u_all[ds(tok0, TOK), :]

        def block(i, e, carry):
            mx, sm = carry
            x = dot(e, u, 1, 1)
            col = [jnp.transpose(jnp.broadcast_to(bias[ds(i * (BLK // L) + j, 1), :], (L, L)))
                   for j in range(BLK // L)]
            x = x + jnp.concatenate([jnp.concatenate(col, axis=0)] * (TOK // L), axis=1)
            for j in range(TOK // L):
                out[sl((tok0 // L + j) * ROWS + i * BLK, BLK), :] = x[:, j * L:(j + 1) * L]
            x = x.reshape(BLK // TILE, TILE, TOK)
            top = jnp.maximum(mx, jnp.max(x, axis=0))
            sm = sm * jnp.exp(mx - top) + jnp.sum(jnp.exp(x - top[None]), axis=0)
            return top, sm

        mx, sm = stream(block, (jnp.full((TILE, TOK), LOW, F32), jnp.zeros((TILE, TOK), F32)), again)
        top = jnp.max(mx, axis=0, keepdims=True)
        sm = jnp.sum(sm * jnp.exp(mx - top), axis=0, keepdims=True)
        stat[:, ds(tok0, TOK)] = jnp.concatenate([top, sm, jnp.zeros((TILE - 2, TOK), F32)], axis=0)

    lab1 = local_labels(lab_own)
    logits(own0, True)
    wait_all(c_u)
    u_all[ds(oth0, TOK), :] = drx[...].astype(BF)
    lab2 = local_labels(lab_rx)
    logits(oth0, True)
    c_st = [remote(stat, stats.at[j], st_s.at[j], st_r.at[j], d) for j, d in enumerate(peers)]
    start_all(c_st)
    wait_all(c_st)
    mx, sm = (jnp.concatenate([stat[i:i + 1, :]] + [stats[j, i:i + 1, :] for j in range(len(peers))], axis=0)
              for i in TWO)
    top = jnp.max(mx, axis=0, keepdims=True)
    norm = top + jnp.log(jnp.sum(sm * jnp.exp(mx - top), axis=0, keepdims=True))
    stat[0:1, :] = norm
    own_norm = jnp.where(lab_own[0:1, :] >= 0, stat[0:1, ds(own0, TOK)], 0.0)
    small[ds(LOSS_ROW, 1), :] = sum(own_norm[:, j * L:(j + 1) * L] for j in range(TOK // L))
    for t0, ref, lab in ((own0, lab_own, lab1), (oth0, lab_rx, lab2)):
        stat[0:1, ds(t0, TOK)] = jnp.where(ref[0:1, :] >= 0, stat[0:1, ds(t0, TOK)], HIGH)
        stat[1:2, ds(t0, TOK)] = lab

    def grad(i, target):
        ids = (lax.broadcasted_iota(jnp.int32, (L, L), 0) + i * L).astype(F32)
        s = jnp.zeros((L, L), F32)
        for j in range(2 * TOK // L):
            x = out[sl(j * ROWS + i * L, L), :]
            hit = ids == stat[1:2, lanes(j)]
            g = (jnp.exp(x - stat[0:1, lanes(j)]) - jnp.where(hit, 1.0, 0.0)) * scale
            gt[ds(pl.multiple_of(i * L, L), L), lanes(j)] = g.astype(BF)
            s = s + g
            target = target + jnp.where(hit, x, 0.0)
        small[ds(i, 1), :] = jnp.sum(jnp.transpose(s), axis=0, keepdims=True)
        return target

    target = lax.fori_loop(0, ROWS // L, grad, jnp.zeros((L, L), F32))
    small[ds(LOSS_ROW + 1, 1), :] = jnp.sum(target, axis=0, keepdims=True)

    def rows(k, start, n):
        return out.at[sl(k * ROWS + start, n)]

    halves = []
    for b, p, pn, q, qn in ((0, y, ynb, z, znb), (HALF, z, znb, y, ynb)):
        pc, qc = ([(t + d) % 4 * n for d in NEAR] for t, n in ((p, SH), (q, SUB)))
        halves.append((b, pn, qn, pc, qc, b + (p + FAR) % 4 * SH, b + p * SH, (q + FAR) % 4 * SUB, q * SUB))

    def stage_copies(st, k):
        cps = []
        for h, (b, pn, qn, pc, qc, po, b2, qo, q0) in enumerate(halves):
            for d in TWO:
                n = SCUTS[d]
                if st == 0:
                    a = rows(k, po + d * CUT, CUT), r1.at[k % 2, h, d], pn
                elif st == 1:
                    a = rows(k, b + pc[d], SH), r2.at[k % 2, h, d], pn
                elif st == 2:
                    a = rows(k, b2 + qo + d * SCUT, n), r3.at[k % 3, h, d, ds(0, n)], qn
                elif st == 3:
                    a = rows(k, b2 + qc[d], SUB), r4.at[k % 3, h, d], qn
                elif st == 4:
                    a = rows(k, b2 + q0, SUB), a1.at[k % 4, h, d], qn
                elif st == 5:
                    a = a1.at[k % 4, h, d, ds(d * SCUT, n)], a2.at[k % 3, h, d, ds(0, n)], qn
                elif st == 6:
                    a = rows(k, b2, SH), rows(k, b2, SH), pn
                else:
                    s = rows(k, b + pc[1 - d] + d * CUT, CUT)
                    a = s, s, pn
                src, dst, nb = a
                cps.append(remote(src, dst, ssem.at[st, h, d, k], rsem.at[st, h, d, k], {"dp": nb[d]}))
        return cps

    def mate_copy(k):
        return remote(rows(k, 0, ROWS), rows(k, OTH0, ROWS), psend.at[k], precv.at[k], {"dp": mate})

    def stage(st, k):
        if st == 0:
            def mm(i, carry):
                rows(k, i * SH, SH)[...] = dot(gt[ds(pl.multiple_of(i * SH, 16), SH), :],
                                               u_all[:, ds(pl.multiple_of(k * L, L), L)], 1, 0)
                return carry
            lax.fori_loop(0, ROWS // SH, mm, 0)
        else:
            wait_all(stage_copies(st - 1, k))
            for h, (b, pn, qn, pc, qc, po, b2, qo, q0) in enumerate(halves):
                both = lambda r, m: [r.at[k % m, h, d] for d in TWO]
                if st == 2:
                    add_rows(rows(k, b2, SH), both(r2, 2), SH, SLOT)
                elif st == 4:
                    add_rows(rows(k, b2 + q0, SUB), both(r4, 3), SUB, SUB)
                for d in TWO:
                    n = SCUTS[d]
                    if st == 1:
                        add_rows(rows(k, b + pc[d] + d * CUT, CUT), [r1.at[k % 2, h, d]], CUT, SLOT)
                    elif st == 3:
                        add_rows(rows(k, b2 + qc[d] + d * SCUT, n), [r3.at[k % 3, h, d]], n, n)
                    elif st == 5:
                        rows(k, b2 + qc[1 - d], SUB)[...] = a1[k % 4, h, d]
                    elif st == 6:
                        rows(k, b2 + qo + d * SCUT, n)[...] = a2[k % 3, h, d, ds(0, n)]
        if st < NSTAGE:
            start_all(stage_copies(st, k))
        else:
            mate_copy(k).start()

    xp, xm, xo = xnb

    def qrow(q, o, n):
        return sl(q * QROWS + o, n)

    def arow(q, o, n):
        return sl(q * XROWS + o, n)

    def same(ref, r):
        return ref.at[r], ref.at[r]

    def dwrow(j, o, n):
        return sl(DW0 + j * W + o, n)

    XTWO = ((xo, 0), (xo, QROWS // 2))
    c_du = [to_mate(part, drx, 2)]
    c_x1 = [to_x(drx.at[qrow(q, o, QROWS // 2)], xr1.at[d], 0, d) for d, (q, o) in enumerate(XTWO)]
    c_x2 = [to_x(drx.at[qrow(xnb[d], 0, QROWS)], part.at[ds(d * QROWS, QROWS)], 1, d) for d in TWO]
    c_x3 = [to_x(*same(dabx, arow(vp, 0, XROWS)), 2, d) for d in TWO]
    c_x4 = [to_x(*same(dabx, arow(q, o, n)), 3, d)
            for d, (q, o, n) in enumerate(((xm, 0, XCUT), (xp, XCUT, XROWS - XCUT)))]
    c_dw = [to_mate(part.at[qrow(1 - c, 0, QROWS)], dwrx.at[ds(0, QROWS)], 3),
            to_mate(part.at[ds(2 * QROWS, TILE)], dwrx.at[ds(QROWS, TILE)], 4)]
    c_w1 = [to_x(*same(out, dwrow(vp, 0, W)), 4, d) for d in TWO]
    c_w2 = [to_x(*same(out, dwrow(q, d * (W // 2), W // 2)), 5, d) for d, q in enumerate((xm, xp))]
    c_w3 = [to_mate(out.at[ds(DW0, 4 * W)], out.at[ds(DW0 + 4 * W, 4 * W)], 5),
            to_mate(out.at[ds(MG0 + W, MINI - W)], out.at[ds(TAIL0, MINI - W)], 6)]

    def du_part(col0, dst, again):
        def block(i, e, carry):
            dst[...] += dot(gt[ds(pl.multiple_of(i * BLK, L), BLK), ds(col0, TOK)], e, 0, 0)
            return carry
        stream(block, 0, again)

    def du_theirs():
        part[...] = jnp.zeros((TOK, W), F32)
        du_part(oth0, part, True)
        start_all(c_du)

    def du_mine():
        wait_all(c_du)
        du_part(own0, drx, False)

        def rnd(i, carry):
            r = sl(i * SCUT, SCUT)
            drx[r, :] = drx[r, :].astype(BF).astype(F32)
            return carry

        lax.fori_loop(0, TOK // SCUT, rnd, 0)
        start_all(c_x1)

    def du_near():
        wait_all(c_x1)
        for d, o in ((0, 0), (1, QROWS // 2)):
            drx[qrow(xnb[d], o, QROWS // 2), :] += xr1[d]
        start_all(c_x2)

    def norm_back():
        wait_all(c_x2)

        def block(i, sums):
            r = sl(i * 2 * TILE, 2 * TILE)
            a = abuf[r, :]
            dun = drx[qrow(vp, i * 2 * TILE, 2 * TILE), :] + part[r, :] + part[sl(QROWS + i * 2 * TILE, 2 * TILE), :]
            cdf, rstd, xhat = gelu_norm(a)
            dx = dun * ln_gain[...]
            dg = rstd * (dx - jnp.mean(dx, axis=-1, keepdims=True) - xhat * jnp.mean(dx * xhat, axis=-1, keepdims=True))
            da = dg * (cdf + a * jnp.exp(-0.5 * a * a) * INV_SQRT_2PI)
            dabx[arow(vp, i * 2 * TILE, 2 * TILE), :] = da.astype(BF).astype(F32)
            return tuple(s + t[:TILE] + t[TILE:] for s, t in zip(sums, (da, dun * xhat, dun)))

        sums = lax.fori_loop(0, QROWS // (2 * TILE), block, (jnp.zeros((TILE, W), F32),) * 3)
        sums = [jnp.sum(t, axis=0, keepdims=True) for t in sums]
        sums.append(jnp.concatenate([small[ds(LOSS_ROW + 1, 1), :], jnp.zeros((1, W - L), F32)], axis=1))
        dabx[arow(vp, QROWS, TILE), :] = jnp.concatenate(sums + [jnp.zeros((TILE - len(sums), W), F32)], axis=0)
        start_all(c_x3)

    def pass_on():
        wait_all(c_x3)
        start_all(c_x4)

    def dab(q):
        return dabx[arow(q, 0, QROWS), :].astype(BF)

    def weight_grad():
        wait_all(c_x4)
        part[ds(0, 2 * QROWS), :] = sum(dot(zbuf[qrow(q, 0, QROWS), :], dab(q), 0, 0) for q in range(4))
        part[ds(2 * QROWS, TILE), :] = sum(dabx[arow(q, QROWS, TILE), :] for q in range(4))
        start_all(c_dw)

    def input_grad():
        load_w_again.start()
        wait_all(c_dw)
        for j in range(W // L):
            m8[lanes(j), :] = part[qrow(c, 0, QROWS), lanes(j)] + dwrx[ds(0, QROWS), lanes(j)]
            v = part[ds(2 * QROWS, TILE), lanes(j)] + dwrx[ds(QROWS, TILE), lanes(j)]
            for i in THREE:
                m8[ds(VEC0 + i * TILE + j, 1), :] = v[i:i + 1]
            if j == 0:
                small[ds(LOSS_ROW + 1, 1), :] = v[3:4]
        m8[ds(SMALL0, N_SMALL), :] = small[...]
        m8[ds(SMALL0 + N_SMALL, MINI - SMALL0 - N_SMALL), :] = jnp.zeros((MINI - SMALL0 - N_SMALL, L), F32)
        start_all(mini_copies(0))

    mini = ((0, y, ynb, z, znb), (MINI // 2, z, znb, y, ynb))

    def mini_copies(st):
        cps = []
        for h, (b, p, pn, q, qn) in enumerate(mini):
            b2 = b + p * MSH
            for d, off in enumerate(AROUND):
                if st == 0:
                    a = m8.at[sl(b + (p + off) % 4 * MSH, MSH)], mr1.at[h, d], pn
                elif st == 1:
                    a = m8.at[sl(b2 + (q + off) % 4 * MSUB, MSUB)], mr2.at[h, d], qn
                elif st == 2:
                    a = *same(out, sl(MG0 + b2 + q * MSUB, MSUB)), qn
                else:
                    a = *same(out, sl(MG0 + b2, MSH)), pn
                src, dst, nb = a
                cps.append(remote(src, dst, ms.at[st, h, d], mr.at[st, h, d], {"dp": nb[d]}))
        return cps

    def mini_first():
        load_w_again.wait()
        for q in range(4):
            u_all[qrow(q, 0, QROWS), :] = dot(dab(q), gt[ds(0, W), :], 1, 1).astype(BF)
        store_dz.start()
        wait_all(mini_copies(0))
        for h, (b, p, pn, q, qn) in enumerate(mini):
            r = sl(b + p * MSH, MSH)
            m8[r, :] = m8[r, :] + sum(mr1[h, d] for d in THREE)
        start_all(mini_copies(1))

    def mini_second():
        store_dz.wait()
        wait_all(mini_copies(1))
        for h, (b, p, pn, q, qn) in enumerate(mini):
            r = b + p * MSH + q * MSUB
            out[sl(MG0 + r, MSUB), :] = m8[sl(r, MSUB), :] + sum(mr2[h, d] for d in THREE)
        start_all(mini_copies(2))

    def mini_third():
        wait_all(mini_copies(2))
        start_all(mini_copies(3))

    def weight_x():
        wait_all(mini_copies(3))
        out[dwrow(vp, 0, W), :] = out[ds(MG0, W), :]
        start_all(c_w1)

    def weight_on():
        wait_all(c_w1)
        start_all(c_w2)

    def weight_mate():
        wait_all(c_w2)
        start_all(c_w3)

    pieces = (du_theirs, du_mine, du_near, norm_back, pass_on, weight_grad, input_grad,
              mini_first, mini_second, mini_third, weight_x, weight_on, weight_mate)

    def step(stages, now, t, carry):
        for st in stages:
            k = t - st
            pl.when((k >= 0) & (k < NCH))(functools.partial(stage, st, k))
        for at, piece in now:
            pl.when(t == at)(piece)
        return carry

    timed = list(enumerate(pieces, 1))
    filling = functools.partial(step, range(NSTAGE - 1, -1, -1), [p for p in timed if p[0] < NCH])
    emptying = functools.partial(step, range(1, NSTAGE + 1), [p for p in timed if p[0] >= NCH])
    lax.fori_loop(0, NCH, filling, 0)
    lax.fori_loop(NCH, NCH + NSTAGE, emptying, 0)

    def drain(k, carry):
        mate_copy(k).wait()
        return carry

    lax.fori_loop(0, NCH, drain, 0)
    wait_all(c_w3)
    save = [pltpu.make_async_copy(out.at[ds(r, MINI - W)], aux.at[j], sem_w.at[j]) for j, r in enumerate((MG0 + W, TAIL0))]
    start_all(save)
    wait_all(save)


def head_call(scale, *args):
    vm, hbm = (pl.BlockSpec(memory_space=s) for s in (VMEM, pltpu.HBM))
    pair = (2, 2)
    sems = [(NSTAGE,) + pair + (NCH,)] * 2 + [(NCH,)] * 2 + [(SEQS + 1,), pair[:1]] + [(7,)] * 4 + [(6, 2)] * 2 + [(4, 2, 3)] * 2
    return pl.pallas_call(
        functools.partial(head_kernel, scale),
        out_shape=(jax.ShapeDtypeStruct((TOK, W), BF), jax.ShapeDtypeStruct((2, MINI - W, L), F32), VMEM((OUT_ROWS, L), F32)),
        in_specs=[vm] * 6 + [hbm] * 3,
        out_specs=(hbm, hbm, vm),
        scratch_shapes=[
            VMEM((ROWS, 2 * TOK), BF), VMEM((2 * TOK, W), BF),
            VMEM((2,) + pair + (CUT, L), F32), VMEM((2,) + pair + (SH, L), F32), VMEM((3,) + pair + (SCUT, L), F32),
            VMEM((3,) + pair + (SUB, L), F32), VMEM((4,) + pair + (SUB, L), F32), VMEM((3,) + pair + (SCUT, L), F32),
            VMEM((TOK, W), F32), VMEM((TOK, W), F32), VMEM((2, QROWS // 2, W), F32),
            VMEM((4 * XROWS, W), F32), VMEM((XROWS, W), F32), VMEM((MINI, L), F32), VMEM((2, 3, MSH, L), F32),
            VMEM((2, 3, MSUB, L), F32), VMEM((2 * BLK, W), BF), VMEM((TOK, 2 * L), BF), VMEM((QROWS, W), F32),
            VMEM((TILE, L), jnp.int32), VMEM((TILE, TOK), F32), VMEM((N_SMALL, L), F32), VMEM((TILE, TOK), F32), VMEM((TILE, 2 * TOK), F32), VMEM((7, TILE, 2 * TOK), F32),
            VMEM((N_SMALL, L), F32),
        ] + [DMA(s) for s in sems],
        compiler_params=pltpu.CompilerParams(collective_id=0, has_side_effects=True, vmem_limit_bytes=30560000),
        name="mlm_head",
    )(*args)


def write_kernel(res, pos_in, dz_in, d_emb, d_w, d_hid, hid, pos, dz, sem, sem_w, sem_h, sem_i):
    c = lax.axis_index("dp") % 2
    cps = []
    for j, core in enumerate((c, 1 - c)):
        for k in range(NCH):
            cps.append(pltpu.make_async_copy(
                res.at[ds(j * OTH0 + k * ROWS, VROWS)], d_emb.at[sl(core * VROWS, VROWS), lanes(k)], sem.at[k, j]))
            for x in range(4):
                cps.append(pltpu.make_async_copy(
                    res.at[ds(DW0 + (j * 4 + x) * W + k * L, L)],
                    d_w.at[sl(x * 2 * L + core * L, L), lanes(k)], sem_w.at[k, j, x]))
    loads = [pltpu.make_async_copy(src, dst, sem_i.at[j]) for j, (src, dst) in enumerate(((pos_in, pos), (dz_in, dz)))]
    start_all(loads)
    start_all(cps)
    wait_all(loads)
    for b in range(SEQS):
        where = jnp.broadcast_to(jnp.concatenate([pos[b:b + 1, :], jnp.full((1, L - MASKS), -1, jnp.int32)], axis=1), (SEQ, L))
        hot = jnp.where(where == lax.broadcasted_iota(jnp.int32, (SEQ, L), 0), 1.0, 0.0).astype(BF)
        rows = jnp.concatenate([dz[b * SLOT:(b + 1) * SLOT, :], jnp.zeros((L - SLOT, W), BF)], axis=0)
        r = ds(b * SEQ, SEQ)
        hid[r, :] = dot(hot, rows, 1, 0).astype(BF)
        cp = pltpu.make_async_copy(hid.at[r], d_hid.at[r], sem_h.at[b])
        cp.start()
        cps.append(cp)
    wait_all(cps)


def write_call(res, pos, dz):
    vm, hbm = (pl.BlockSpec(memory_space=s) for s in (VMEM, pltpu.HBM))
    return pl.pallas_call(
        write_kernel,
        out_shape=tuple(jax.ShapeDtypeStruct(s, t) for s, t in (
            ((2 * VROWS, W), F32), ((W, W), F32), ((SEQS * SEQ, W), BF))),
        in_specs=[vm, hbm, hbm],
        out_specs=(hbm,) * 3,
        scratch_shapes=[VMEM((SEQS * SEQ, W), BF), VMEM((SEQS, MASKS), jnp.int32), VMEM((TOK, W), BF), DMA((NCH, 2)), DMA((NCH, 2, 4)),
                        DMA((SEQS,)), DMA((2,))],
        compiler_params=pltpu.CompilerParams(vmem_limit_bytes=16 << 20),
        name="write_rows",
    )(res, *(pltpu.with_memory_space_constraint(t, pltpu.HBM) for t in (pos, dz)))


def small_kernel(aux, b_trans, ln_gain, ln_bias, db, loss):
    c = lax.axis_index("dp") % 2
    for i, ref in enumerate((b_trans, ln_gain, ln_bias)):
        ref[...] = aux[0, ds(i * TILE, TILE), :]
    first, second = aux[ds(c, 1), ds(SMALL0 - VEC0, N_SMALL), :][0], aux[ds(1 - c, 1), ds(SMALL0 - VEC0, N_SMALL), :][0]
    rest = VROWS % L
    lane = lax.broadcasted_iota(jnp.int32, (LOSS_ROW, L), 1)
    second = pltpu.roll(second, rest, 1)
    db[ds(0, LOSS_ROW), :] = jnp.where((lane < rest) | (lax.broadcasted_iota(jnp.int32, (LOSS_ROW, L), 0) < LOSS_ROW - 1),
                                       first[:LOSS_ROW], second[:1])
    db[ds(LOSS_ROW, LOSS_ROW), :] = jnp.where(lane < rest, second[:LOSS_ROW], second[1:LOSS_ROW + 1])
    at = SMALL0 - VEC0 + LOSS_ROW
    total = aux[0, ds(at, 1), :] + aux[1, ds(at, 1), :] - aux[0, ds(at + 1, 1), :]
    loss[...] = jnp.sum(total, axis=1, keepdims=True)


def small_call(aux):
    vm = pl.BlockSpec(memory_space=VMEM)
    return pl.pallas_call(
        small_kernel,
        out_shape=tuple(jax.ShapeDtypeStruct(t, F32) for t in [(TILE, L)] * 3 + [(2 * LOSS_ROW, L), (1, 1)]),
        in_specs=[vm],
        out_specs=(vm,) * 5,
        name="small_results",
    )(aux)


def solution(mesh):
    n_groups = mesh.shape["dp"]

    def local_step(hidden, mask_pos, labels, w_trans, b_trans, ln_gain, ln_bias, emb_table, b_vocab):
        n_rows, seq_len, width = hidden.shape
        n_masks = mask_pos.shape[1]
        n_tokens = n_rows * n_masks * n_groups
        line = lambda v: v.reshape(1, v.shape[0])
        dz, aux, res = head_call(1.0 / n_tokens, mask_pos, labels, line(b_vocab), line(b_trans), line(ln_gain), line(ln_bias),
                                 hidden.reshape(n_rows * seq_len, width), emb_table, w_trans)
        d_emb, d_w_trans, d_hidden = write_call(res, mask_pos, dz)
        aux, d_w_trans = lax.optimization_barrier((aux, d_w_trans))
        *vecs, db, loss = small_call(aux)
        d_b_trans, d_gain, d_bias = (v.reshape(width) for v in vecs)
        d_b_vocab = db.reshape(2 * ROWS)[:2 * VROWS]
        return loss.reshape(()) / n_tokens, d_hidden.reshape(hidden.shape), d_w_trans, d_b_trans, d_gain, d_bias, d_emb, d_b_vocab

    in_specs = (P("dp", None, None), P("dp", None), P("dp", None), P(None, None), P(None), P(None), P(None), P("vp", None), P("vp"))
    out_specs = (P(), P("dp", None, None), P(None, None), P(None), P(None), P(None), P("vp", None), P("vp"))
    return jax.shard_map(local_step, mesh=mesh, in_specs=in_specs, out_specs=out_specs, check_vma=False)
```

```python
import functools

import jax
import jax.numpy as jnp
from jax import lax
from jax.experimental import pallas as pl
from jax.experimental.pallas import tpu as pltpu
from jax.sharding import PartitionSpec as P

MESH = pl.DeviceIdType.MESH
F32, BF = jnp.float32, jnp.bfloat16
VMEM, DMA, ds = pltpu.VMEM, pltpu.SemaphoreType.DMA, pl.ds
LN_EPS = 1e-5
HALF_SQRT, INV_SQRT_2PI = 0.7071067811865476, 0.3989422804014327
LOW, HIGH, NO_LABEL = -3e38, 3e38, -1e6
W, L, TILE, BTILE = 1024, 128, 8, 16
SEQS, SEQ, MASKS, SLOT = 6, 512, 77, 80
USED, TOK = SEQS * SLOT, 512
VROWS, ROWS, BLK = 3824, 3840, 384
N_BLK = ROWS // BLK
LAST = VROWS - (N_BLK - 1) * BLK
NCH = W // L
HALF, SH, SUB = ROWS // 2, ROWS // 8, ROWS // 32
CUT, SCUT = SH // 2, 64
SCUTS = (SCUT, SUB - SCUT)
QROWS, XROWS, XCUT = 128, 136, 72
VEC0, SMALL0, MINI = W, W + 24, 1280
MSH, MSUB = MINI // 8, MINI // 32
LOSS_ROW, N_SMALL = ROWS // L, 32
OTH0 = NCH * ROWS
DW0 = 2 * OTH0
MG0 = DW0 + 8 * W
TAIL0 = MG0 + MINI
OUT_ROWS = TAIL0 + MINI - W
NSTAGE = 8
NEAR, FAR = (1, 3), 2
AROUND = NEAR + (FAR,)
TWO, THREE = (0, 1), (0, 1, 2)


def sl(start, n):
    return ds(pl.multiple_of(start, TILE), n)


def wait_all(cps):
    for cp in cps:
        cp.wait()


def start_all(cps):
    for cp in cps:
        cp.start()


def gelu_norm(a):
    cdf = 0.5 * (1.0 + lax.erf(a * HALF_SQRT))
    g = a * cdf
    cen = g - row_mean(g)
    rstd = lax.rsqrt(row_mean(cen * cen) + LN_EPS)
    return cdf, rstd, cen * rstd


def row_mean(t):
    return jnp.mean(t, axis=-1, keepdims=True)


def over_rows(fn, t):
    return fn(t, axis=0, keepdims=True)


def dot(a, b, ca=1, cb=0):
    return lax.dot_general(a, b, (((ca,), (cb,)), ((), ())), preferred_element_type=F32)


def lanes(j):
    return ds(j * L, L)


def add_rows(dst, srcs, n, blk):
    def body(i, carry):
        r = sl(i * blk, blk)
        v = dst[r, :]
        for s in srcs:
            v = v + s[r, :]
        dst[r, :] = v
        return carry
    lax.fori_loop(0, n // blk, body, 0)


def head_kernel(scale, pos_in, lab_in, b_in, b_trans, ln_gain, ln_bias, hidden, emb, w_in, dz, aux, out,
                gt, u_all, r1, r2, r3, r4, a1, a2, part, drx, xr1, dabx, dwrx, m8, mr1, mr2,
                wbuf, zbuf, abuf, pos, lab_own, bias, lab_rx, stat, stats, small,
                ssem, rsem, psend, precv, sem_h, sem_w, es, er, st_s, st_r, xs, xr, ms, mr):
    dp, vp = lax.axis_index("dp"), lax.axis_index("vp")
    z, y, c = dp // 8, (dp // 2) % 4, dp % 2
    ynb = [z * 8 + ((y + d) % 4) * 2 + c for d in AROUND]
    znb = [((z + d) % 4) * 8 + y * 2 + c for d in AROUND]
    xnb = [(vp + d) % 4 for d in AROUND]
    mate = dp + 1 - 2 * c
    peers = [{"vp": v, "dp": d} for v in xnb for d in (dp, mate)] + [{"vp": vp, "dp": mate}]

    def load_hidden(b):
        r = sl(b * SEQ, SEQ)
        return pltpu.make_async_copy(hidden.at[r], gt.at[r], sem_h.at[b])

    def load_emb(i, slot, n):
        return pltpu.make_async_copy(emb.at[ds(pl.multiple_of(c * VROWS, BTILE) + i * BLK, n)],
                                     wbuf.at[ds(pl.multiple_of(slot * BLK, BTILE), n)], sem_w.at[slot])

    load_w = pltpu.make_async_copy(w_in, u_all, sem_h.at[SEQS])
    store_dz = pltpu.make_async_copy(u_all.at[ds(0, TOK)], dz, sem_h.at[0])
    load_w_again = pltpu.make_async_copy(w_in, gt.at[ds(0, W)], sem_h.at[SEQS])
    for b in range(SEQS):
        load_hidden(b).start()
    load_w.start()
    load_emb(0, 0, BLK).start()

    barrier = pltpu.get_barrier_semaphore()
    greet = peers + [{"dp": d} for d in ynb + znb]
    for d in greet:
        pl.semaphore_signal(barrier, inc=1, device_id=d, device_id_type=MESH)

    def remote(src, dst, send, recv, dev):
        return pltpu.make_async_remote_copy(src_ref=src, dst_ref=dst, send_sem=send, recv_sem=recv,
                                            device_id=dev, device_id_type=MESH)

    def to_mate(src, dst, i):
        return remote(src, dst, es.at[i], er.at[i], {"dp": mate})

    def to_x(src, dst, i, d):
        return remote(src, dst, xs.at[i, d], xr.at[i, d], {"vp": xnb[d]})

    c_u = [to_mate(part, drx, 0), to_mate(lab_own, lab_rx, 1)]
    own0 = pl.multiple_of(c * TOK, TOK)
    oth0 = pl.multiple_of((1 - c) * TOK, TOK)

    pos[...] = jnp.full((TILE, L), -1, jnp.int32)
    pos[ds(0, SEQS), ds(0, MASKS)] = pos_in[...]
    lane = lax.broadcasted_iota(jnp.int32, (L, TOK), 1)
    seq = sum((lane >= b * SLOT).astype(jnp.int32) for b in range(1, SEQS))
    slot = lane - seq * SLOT
    place = jnp.where(slot == lax.broadcasted_iota(jnp.int32, (L, TOK), 0), 1.0, 0.0).astype(BF)[:MASKS]
    high, low = lab_in[...] >> 8, lab_in[...] & 255
    spread = dot(high.astype(F32).astype(BF), place) * 256.0 + dot(low.astype(F32).astype(BF), place)
    row = lax.broadcasted_iota(jnp.int32, (SEQS, TOK), 0)
    lab = over_rows(jnp.sum, jnp.where(row == seq[:SEQS], spread, 0.0))
    lab = jnp.where(slot[:1] < MASKS, lab, NO_LABEL)
    lab_own[...] = jnp.broadcast_to(lab, (TILE, TOK))
    rest = VROWS % L
    for core in TWO:
        @pl.when(c == core)
        def _():
            for i in range(VROWS // L):
                bias[ds(i, 1), :] = b_in[:, core * VROWS + i * L:core * VROWS + (i + 1) * L]
            bias[ds(LOSS_ROW - 1, 1), :] = jnp.full((1, L), LOW, F32)
            bias[ds(LOSS_ROW - 1, 1), ds(0, rest)] = b_in[:, (core + 1) * VROWS - rest:(core + 1) * VROWS]

    z0 = SEQS * SEQ

    def gather(b, carry):
        load_hidden(b).wait()
        where = jnp.broadcast_to(pos[ds(b, 1), :], (SEQ, L))
        hot = jnp.where(where == lax.broadcasted_iota(jnp.int32, (SEQ, L), 0), 1.0, 0.0).astype(BF)
        gt[ds(pl.multiple_of(z0 + b * SLOT, BTILE), SLOT), :] = dot(hot, gt[sl(b * SEQ, SEQ), :], 0, 0)[:SLOT].astype(BF)
        return carry

    gt[ds(z0 + USED, TOK - USED), :] = jnp.zeros((TOK - USED, W), BF)
    lax.fori_loop(0, SEQS, gather, 0)
    load_w.wait()
    zbuf[...] = gt[ds(z0, TOK), ds(pl.multiple_of(vp * 2 * L, L), 2 * L)]

    def transform(i, carry):
        r = sl(i * 2 * L, 2 * L)
        dabx[r, :] = dot(gt[ds(pl.multiple_of(z0 + i * 2 * L, L), 2 * L), :], u_all[...]) + b_trans[...]
        return carry

    lax.fori_loop(0, TOK // (2 * L), transform, 0)

    def norm(i, carry):
        r = sl(i * 4 * TILE, 4 * TILE)
        _, _, xhat = gelu_norm(dabx[r, :])
        part[r, :] = (xhat * ln_gain[...] + ln_bias[...]).astype(BF).astype(F32)
        return carry

    lax.fori_loop(0, TOK // (4 * TILE), norm, 0)
    abuf[...] = dabx[sl(vp * QROWS, QROWS), :]
    u_all[ds(own0, TOK), :] = part[...].astype(BF)
    pl.semaphore_wait(barrier, len(greet))
    start_all(c_u)

    def stream(body, init, again):
        def pair(m, carry):
            last = m + 1 == N_BLK // 2
            i = 2 * m
            for at, n in ((~last, BLK), (last, LAST)):
                pl.when(at)(load_emb(i + 1, 1, n).start)
            load_emb(i, 0, BLK).wait()
            carry = body(i, 0, wbuf[ds(0, BLK), :], carry)
            pl.when(~last)(load_emb(i + 2, 0, BLK).start)
            if again:
                pl.when(last)(load_emb(0, 0, BLK).start)
            for at, n in ((~last, BLK), (last, LAST)):
                pl.when(at)(load_emb(i + 1, 1, n).wait)
            return body(i + 1, 1, wbuf[ds(BLK, BLK), :], carry)
        return lax.fori_loop(0, N_BLK // 2, pair, init)

    row0 = (vp * 2 * VROWS + c * VROWS).astype(F32)

    def local_labels(ref):
        v = ref[0:1, :] - row0
        return jnp.where((v >= 0) & (v < VROWS), v, -1.0)

    def logits(tok0, again):
        u = u_all[ds(tok0, TOK), :]

        def sums(slot, top):
            return jnp.concatenate(
                [jnp.sum(jnp.exp(r2[slot, j // 2, j % 2, ds(0, BLK), :].reshape(BLK // TILE, TILE, L)
                                 - top[:, j * L:(j + 1) * L][None]), axis=0) for j in range(TOK // L)], axis=1)

        def block(i, slot, e, carry):
            old, mx, sm = carry
            sm = sm * jnp.exp(old - mx) + sums(1 - slot, mx)
            x = dot(e, u, 1, 1)
            col = [jnp.transpose(jnp.broadcast_to(bias[ds(i * (BLK // L) + j, 1), :], (L, L))) for j in range(BLK // L)]
            col = jnp.concatenate(col, axis=0)
            top = []
            for j in range(TOK // L):
                v = x[:, j * L:(j + 1) * L] + col
                out[sl((tok0 // L + j) * ROWS + i * BLK, BLK), :] = v
                r2[slot, j // 2, j % 2, ds(0, BLK), :] = v
                top.append(jnp.max(v.reshape(BLK // TILE, TILE, L), axis=0))
            return mx, jnp.maximum(mx, jnp.concatenate(top, axis=1)), sm

        low = jnp.full((TILE, TOK), LOW, F32)
        for j in range(TOK // L):
            r2[1, j // 2, j % 2, ds(0, BLK), :] = jnp.full((BLK, L), LOW, F32)
        old, mx, sm = stream(block, (low, low, jnp.zeros((TILE, TOK), F32)), again)
        sm = sm * jnp.exp(old - mx) + sums(1, mx)
        top = over_rows(jnp.max, mx)
        sm = over_rows(jnp.sum, sm * jnp.exp(mx - top))
        stat[:, ds(tok0, TOK)] = jnp.concatenate([top, sm, jnp.zeros((TILE - 2, TOK), F32)], axis=0)

    lab1 = local_labels(lab_own)
    logits(own0, True)
    wait_all(c_u)
    u_all[ds(oth0, TOK), :] = drx[...].astype(BF)
    lab2 = local_labels(lab_rx)
    logits(oth0, True)
    c_st = [remote(stat, stats.at[j], st_s.at[j], st_r.at[j], d) for j, d in enumerate(peers)]
    start_all(c_st)
    wait_all(c_st)
    mx, sm = (jnp.concatenate([stat[i:i + 1, :]] + [stats[j, i:i + 1, :] for j in range(len(peers))], axis=0)
              for i in TWO)
    top = over_rows(jnp.max, mx)
    norm = top + jnp.log(over_rows(jnp.sum, sm * jnp.exp(mx - top)))
    stat[0:1, :] = norm
    own_norm = jnp.where(lab_own[0:1, :] >= 0, stat[0:1, ds(own0, TOK)], 0.0)
    small[ds(LOSS_ROW, 1), :] = sum(own_norm[:, j * L:(j + 1) * L] for j in range(TOK // L))
    for t0, ref, lab in ((own0, lab_own, lab1), (oth0, lab_rx, lab2)):
        stat[0:1, ds(t0, TOK)] = jnp.where(ref[0:1, :] >= 0, stat[0:1, ds(t0, TOK)], HIGH)
        stat[1:2, ds(t0, TOK)] = lab

    def grad(i, target):
        ids = (lax.broadcasted_iota(jnp.int32, (L, L), 0) + i * L).astype(F32)
        s = jnp.zeros((L, L), F32)
        for j in range(2 * TOK // L):
            x = out[sl(j * ROWS + i * L, L), :]
            hit = ids == stat[1:2, lanes(j)]
            g = (jnp.exp(x - stat[0:1, lanes(j)]) - jnp.where(hit, 1.0, 0.0)) * scale
            gt[ds(pl.multiple_of(i * L, L), L), lanes(j)] = g.astype(BF)
            s = s + g
            target = target + jnp.where(hit, x, 0.0)
        small[ds(i, 1), :] = over_rows(jnp.sum, jnp.transpose(s))
        return target

    target = lax.fori_loop(0, ROWS // L, grad, jnp.zeros((L, L), F32))
    small[ds(LOSS_ROW + 1, 1), :] = over_rows(jnp.sum, target)

    def rows(k, start, n):
        return out.at[sl(k * ROWS + start, n)]

    halves = []
    for b, p, pn, q, qn in ((0, y, ynb, z, znb), (HALF, z, znb, y, ynb)):
        pc, qc = ([(t + d) % 4 * n for d in NEAR] for t, n in ((p, SH), (q, SUB)))
        halves.append((b, pn, qn, pc, qc, b + (p + FAR) % 4 * SH, b + p * SH, (q + FAR) % 4 * SUB, q * SUB))

    def stage_copies(st, k):
        cps = []
        for h, (b, pn, qn, pc, qc, po, b2, qo, q0) in enumerate(halves):
            for d in TWO:
                n = SCUTS[d]
                if st == 0:
                    a = rows(k, po + d * CUT, CUT), r1.at[k % 2, h, d], pn
                elif st == 1:
                    a = rows(k, b + pc[d], SH), r2.at[k % 2, h, d], pn
                elif st == 2:
                    a = rows(k, b2 + qo + d * SCUT, n), r3.at[k % 3, h, d, ds(0, n)], qn
                elif st == 3:
                    a = rows(k, b2 + qc[d], SUB), r4.at[k % 3, h, d], qn
                elif st == 4:
                    a = rows(k, b2 + q0, SUB), a1.at[k % 4, h, d], qn
                elif st == 5:
                    a = a1.at[k % 4, h, d, ds(d * SCUT, n)], a2.at[k % 3, h, d, ds(0, n)], qn
                elif st == 6:
                    a = rows(k, b2, SH), rows(k, b2, SH), pn
                else:
                    s = rows(k, b + pc[1 - d] + d * CUT, CUT)
                    a = s, s, pn
                src, dst, nb = a
                cps.append(remote(src, dst, ssem.at[st, h, d, k], rsem.at[st, h, d, k], {"dp": nb[d]}))
        return cps

    def mate_copy(k):
        return remote(rows(k, 0, ROWS), rows(k, OTH0, ROWS), psend.at[k], precv.at[k], {"dp": mate})

    def stage(st, k):
        if st == 0:
            def mm(r):
                r = pl.multiple_of(r, BTILE)
                rows(k, r, SH)[...] = dot(gt[ds(r, SH), :], u_all[:, ds(pl.multiple_of(k * L, L), L)])

            for h in halves:
                mm(h[5])
            start_all(stage_copies(st, k))

            def others(i, carry):
                mm(i // 3 * HALF + (jnp.where(i < 3, y, z) + (i % 3 + 3)) % 4 * SH)
                return carry
            lax.fori_loop(0, 6, others, 0)
        else:
            wait_all(stage_copies(st - 1, k))
            for h, (b, pn, qn, pc, qc, po, b2, qo, q0) in enumerate(halves):
                both = lambda r, m: [r.at[k % m, h, d] for d in TWO]
                if st == 2:
                    add_rows(rows(k, b2, SH), both(r2, 2), SH, SLOT)
                elif st == 4:
                    add_rows(rows(k, b2 + q0, SUB), both(r4, 3), SUB, SUB)
                for d in TWO:
                    n = SCUTS[d]
                    if st == 1:
                        add_rows(rows(k, b + pc[d] + d * CUT, CUT), [r1.at[k % 2, h, d]], CUT, SLOT)
                    elif st == 3:
                        add_rows(rows(k, b2 + qc[d] + d * SCUT, n), [r3.at[k % 3, h, d]], n, n)
                    elif st == 5:
                        rows(k, b2 + qc[1 - d], SUB)[...] = a1[k % 4, h, d]
                    elif st == 6:
                        rows(k, b2 + qo + d * SCUT, n)[...] = a2[k % 3, h, d, ds(0, n)]
        if st == NSTAGE:
            mate_copy(k).start()
        elif st:
            start_all(stage_copies(st, k))

    xp, xm, xo = xnb

    def qrow(q, o, n):
        return sl(q * QROWS + o, n)

    def arow(q, o, n):
        return sl(q * XROWS + o, n)

    def same(ref, r):
        return ref.at[r], ref.at[r]

    def dwrow(j, o, n):
        return sl(DW0 + j * W + o, n)

    XTWO = ((xo, 0), (xo, QROWS // 2))
    c_du = [to_mate(part, drx, 2)]
    c_x1 = [to_x(drx.at[qrow(q, o, QROWS // 2)], xr1.at[d], 0, d) for d, (q, o) in enumerate(XTWO)]
    c_x2 = [to_x(drx.at[qrow(xnb[d], 0, QROWS)], part.at[ds(d * QROWS, QROWS)], 1, d) for d in TWO]
    c_x3 = [to_x(*same(dabx, arow(vp, 0, XROWS)), 2, d) for d in TWO]
    c_x4 = [to_x(*same(dabx, arow(q, o, n)), 3, d)
            for d, (q, o, n) in enumerate(((xm, 0, XCUT), (xp, XCUT, XROWS - XCUT)))]
    c_dw = [to_mate(part.at[qrow(1 - c, 0, QROWS)], dwrx.at[ds(0, QROWS)], 3),
            to_mate(part.at[ds(2 * QROWS, TILE)], dwrx.at[ds(QROWS, TILE)], 4)]
    c_w1 = [to_x(*same(out, dwrow(vp, 0, W)), 4, d) for d in TWO]
    c_w2 = [to_x(*same(out, dwrow(q, d * (W // 2), W // 2)), 5, d) for d, q in enumerate((xm, xp))]
    c_w3 = [to_mate(out.at[ds(DW0, 4 * W)], out.at[ds(DW0 + 4 * W, 4 * W)], 5),
            to_mate(out.at[ds(MG0 + W, MINI - W)], out.at[ds(TAIL0, MINI - W)], 6)]

    def du_part(col0, dst, again):
        def block(i, slot, e, carry):
            dst[...] += dot(gt[ds(pl.multiple_of(i * BLK, L), BLK), ds(col0, TOK)], e, 0, 0)
            return carry
        stream(block, 0, again)

    def du_theirs():
        part[...] = jnp.zeros((TOK, W), F32)
        du_part(oth0, part, True)
        start_all(c_du)

    def du_mine():
        wait_all(c_du)
        du_part(own0, drx, False)

        def rnd(i, carry):
            r = sl(i * SCUT, SCUT)
            drx[r, :] = drx[r, :].astype(BF).astype(F32)
            return carry

        lax.fori_loop(0, TOK // SCUT, rnd, 0)
        start_all(c_x1)

    def du_near():
        wait_all(c_x1)
        for d, o in ((0, 0), (1, QROWS // 2)):
            drx[qrow(xnb[d], o, QROWS // 2), :] += xr1[d]
        start_all(c_x2)

    def norm_back():
        wait_all(c_x2)

        def block(i, sums):
            r = sl(i * 2 * TILE, 2 * TILE)
            a = abuf[r, :]
            dun = drx[qrow(vp, i * 2 * TILE, 2 * TILE), :] + part[r, :] + part[sl(QROWS + i * 2 * TILE, 2 * TILE), :]
            cdf, rstd, xhat = gelu_norm(a)
            dx = dun * ln_gain[...]
            dg = rstd * (dx - row_mean(dx) - xhat * row_mean(dx * xhat))
            da = dg * (cdf + a * jnp.exp(-0.5 * a * a) * INV_SQRT_2PI)
            dabx[arow(vp, i * 2 * TILE, 2 * TILE), :] = da.astype(BF).astype(F32)
            return tuple(s + t[:TILE] + t[TILE:] for s, t in zip(sums, (da, dun * xhat, dun)))

        sums = lax.fori_loop(0, QROWS // (2 * TILE), block, (jnp.zeros((TILE, W), F32),) * 3)
        sums = [over_rows(jnp.sum, t) for t in sums]
        sums.append(jnp.concatenate([small[ds(LOSS_ROW + 1, 1), :], jnp.zeros((1, W - L), F32)], axis=1))
        dabx[arow(vp, QROWS, TILE), :] = jnp.concatenate(sums + [jnp.zeros((TILE - len(sums), W), F32)], axis=0)
        start_all(c_x3)

    def pass_on():
        wait_all(c_x3)
        start_all(c_x4)

    def dab(q):
        return dabx[arow(q, 0, QROWS), :].astype(BF)

    def weight_grad():
        wait_all(c_x4)
        part[ds(0, 2 * QROWS), :] = sum(dot(zbuf[qrow(q, 0, QROWS), :], dab(q), 0, 0) for q in range(4))
        part[ds(2 * QROWS, TILE), :] = sum(dabx[arow(q, QROWS, TILE), :] for q in range(4))
        start_all(c_dw)

    def input_grad():
        load_w_again.start()
        wait_all(c_dw)
        for j in range(W // L):
            m8[lanes(j), :] = part[qrow(c, 0, QROWS), lanes(j)] + dwrx[ds(0, QROWS), lanes(j)]
            v = part[ds(2 * QROWS, TILE), lanes(j)] + dwrx[ds(QROWS, TILE), lanes(j)]
            for i in THREE:
                m8[ds(VEC0 + i * TILE + j, 1), :] = v[i:i + 1]
            if j == 0:
                small[ds(LOSS_ROW + 1, 1), :] = v[3:4]
        m8[ds(SMALL0, N_SMALL), :] = small[...]
        m8[ds(SMALL0 + N_SMALL, MINI - SMALL0 - N_SMALL), :] = jnp.zeros((MINI - SMALL0 - N_SMALL, L), F32)
        start_all(mini_copies(0))

    mini = ((0, y, ynb, z, znb), (MINI // 2, z, znb, y, ynb))

    def mini_copies(st):
        cps = []
        for h, (b, p, pn, q, qn) in enumerate(mini):
            b2 = b + p * MSH
            for d, off in enumerate(AROUND):
                if st == 0:
                    a = m8.at[sl(b + (p + off) % 4 * MSH, MSH)], mr1.at[h, d], pn
                elif st == 1:
                    a = m8.at[sl(b2 + (q + off) % 4 * MSUB, MSUB)], mr2.at[h, d], qn
                elif st == 2:
                    a = *same(out, sl(MG0 + b2 + q * MSUB, MSUB)), qn
                else:
                    a = *same(out, sl(MG0 + b2, MSH)), pn
                src, dst, nb = a
                cps.append(remote(src, dst, ms.at[st, h, d], mr.at[st, h, d], {"dp": nb[d]}))
        return cps

    def mini_first():
        load_w_again.wait()
        for q in range(4):
            u_all[qrow(q, 0, QROWS), :] = dot(dab(q), gt[ds(0, W), :], 1, 1).astype(BF)
        store_dz.start()
        wait_all(mini_copies(0))
        for h, (b, p, pn, q, qn) in enumerate(mini):
            r = sl(b + p * MSH, MSH)
            m8[r, :] = m8[r, :] + sum(mr1[h, d] for d in THREE)
        start_all(mini_copies(1))

    def mini_second():
        store_dz.wait()
        wait_all(mini_copies(1))
        for h, (b, p, pn, q, qn) in enumerate(mini):
            r = b + p * MSH + q * MSUB
            out[sl(MG0 + r, MSUB), :] = m8[sl(r, MSUB), :] + sum(mr2[h, d] for d in THREE)
        start_all(mini_copies(2))

    def mini_third():
        wait_all(mini_copies(2))
        start_all(mini_copies(3))

    def weight_x():
        wait_all(mini_copies(3))
        out[dwrow(vp, 0, W), :] = out[ds(MG0, W), :]
        start_all(c_w1)

    def weight_on():
        wait_all(c_w1)
        start_all(c_w2)

    def weight_mate():
        wait_all(c_w2)
        start_all(c_w3)

    pieces = (du_theirs, du_mine, du_near, norm_back, pass_on, weight_grad, input_grad,
              mini_first, mini_second, mini_third, weight_x, weight_on, weight_mate)

    def step(stages, now, t, carry):
        for st in stages:
            k = t - st
            pl.when((k >= 0) & (k < NCH))(functools.partial(stage, st, k))
            if st == NSTAGE // 2:
                for at, piece in now:
                    if piece is weight_grad:
                        pl.when(t == at)(piece)
        for at, piece in now:
            if piece is not weight_grad:
                pl.when(t == at)(piece)
        return carry

    timed = [(at, piece) for at, piece in zip((2, 3, 4, 5, 6, 7, 7, *range(NCH, NCH + 6)), pieces)]
    filling = functools.partial(step, range(NSTAGE - 1, -1, -1), [p for p in timed if p[0] < NCH])
    emptying = functools.partial(step, range(1, NSTAGE + 1), [p for p in timed if p[0] >= NCH])
    lax.fori_loop(0, NCH, filling, 0)
    lax.fori_loop(NCH, NCH + NSTAGE, emptying, 0)

    def drain(k, carry):
        mate_copy(k).wait()
        return carry

    lax.fori_loop(0, NCH, drain, 0)
    wait_all(c_w3)
    save = [pltpu.make_async_copy(out.at[ds(r, MINI - W)], aux.at[j], sem_w.at[j]) for j, r in enumerate((MG0 + W, TAIL0))]
    start_all(save)
    wait_all(save)


def head_call(scale, *args):
    vm, hbm = (pl.BlockSpec(memory_space=s) for s in (VMEM, pltpu.HBM))
    pair = (2, 2)
    sems = [(NSTAGE,) + pair + (NCH,)] * 2 + [(NCH,)] * 2 + [(SEQS + 1,), pair[:1]] + [(7,)] * 4 + [(6, 2)] * 2 + [(4, 2, 3)] * 2
    return pl.pallas_call(
        functools.partial(head_kernel, scale),
        out_shape=(jax.ShapeDtypeStruct((TOK, W), BF), jax.ShapeDtypeStruct((2, MINI - W, L), F32), VMEM((OUT_ROWS, L), F32)),
        in_specs=[vm] * 6 + [hbm] * 3,
        out_specs=(hbm, hbm, vm),
        scratch_shapes=[
            VMEM((ROWS, 2 * TOK), BF), VMEM((2 * TOK, W), BF),
            VMEM((2,) + pair + (CUT, L), F32), VMEM((2,) + pair + (SH, L), F32), VMEM((3,) + pair + (SCUT, L), F32),
            VMEM((3,) + pair + (SUB, L), F32), VMEM((4,) + pair + (SUB, L), F32), VMEM((3,) + pair + (SCUT, L), F32),
            VMEM((TOK, W), F32), VMEM((TOK, W), F32), VMEM((2, QROWS // 2, W), F32),
            VMEM((4 * XROWS, W), F32), VMEM((XROWS, W), F32), VMEM((MINI, L), F32), VMEM((2, 3, MSH, L), F32),
            VMEM((2, 3, MSUB, L), F32), VMEM((2 * BLK, W), BF), VMEM((TOK, 2 * L), BF), VMEM((QROWS, W), F32),
            VMEM((TILE, L), jnp.int32), VMEM((TILE, TOK), F32), VMEM((N_SMALL, L), F32), VMEM((TILE, TOK), F32), VMEM((TILE, 2 * TOK), F32), VMEM((7, TILE, 2 * TOK), F32),
            VMEM((N_SMALL, L), F32),
        ] + [DMA(s) for s in sems],
        compiler_params=pltpu.CompilerParams(collective_id=0, has_side_effects=True, vmem_limit_bytes=30560000),
        name="mlm_head",
    )(*args)


def write_kernel(res, pos_in, dz_in, d_emb, d_w, d_hid, hid, pos, dz, sem, sem_w, sem_h, sem_i):
    c = lax.axis_index("dp") % 2
    cps = []
    for j, core in enumerate((c, 1 - c)):
        for k in range(NCH):
            cps.append(pltpu.make_async_copy(
                res.at[ds(j * OTH0 + k * ROWS, VROWS)], d_emb.at[sl(core * VROWS, VROWS), lanes(k)], sem.at[k, j]))
            for x in range(4):
                cps.append(pltpu.make_async_copy(
                    res.at[ds(DW0 + (j * 4 + x) * W + k * L, L)],
                    d_w.at[sl(x * 2 * L + core * L, L), lanes(k)], sem_w.at[k, j, x]))
    loads = [pltpu.make_async_copy(src, dst, sem_i.at[j]) for j, (src, dst) in enumerate(((pos_in, pos), (dz_in, dz)))]
    start_all(loads)
    start_all(cps)
    wait_all(loads)
    for b in range(SEQS):
        where = jnp.broadcast_to(jnp.concatenate([pos[b:b + 1, :], jnp.full((1, L - MASKS), -1, jnp.int32)], axis=1), (SEQ, L))
        hot = jnp.where(where == lax.broadcasted_iota(jnp.int32, (SEQ, L), 0), 1.0, 0.0).astype(BF)
        rows = jnp.concatenate([dz[b * SLOT:(b + 1) * SLOT, :], jnp.zeros((L - SLOT, W), BF)], axis=0)
        r = ds(b * SEQ, SEQ)
        hid[r, :] = dot(hot, rows).astype(BF)
        cp = pltpu.make_async_copy(hid.at[r], d_hid.at[r], sem_h.at[b])
        cp.start()
        cps.append(cp)
    wait_all(cps)


def write_call(res, pos, dz):
    vm, hbm = (pl.BlockSpec(memory_space=s) for s in (VMEM, pltpu.HBM))
    return pl.pallas_call(
        write_kernel,
        out_shape=tuple(jax.ShapeDtypeStruct(s, t) for s, t in (
            ((2 * VROWS, W), F32), ((W, W), F32), ((SEQS * SEQ, W), BF))),
        in_specs=[vm, hbm, hbm],
        out_specs=(hbm,) * 3,
        scratch_shapes=[VMEM((SEQS * SEQ, W), BF), VMEM((SEQS, MASKS), jnp.int32), VMEM((TOK, W), BF), DMA((NCH, 2)), DMA((NCH, 2, 4)),
                        DMA((SEQS,)), DMA((2,))],
        compiler_params=pltpu.CompilerParams(vmem_limit_bytes=16 << 20),
        name="write_rows",
    )(res, *(pltpu.with_memory_space_constraint(t, pltpu.HBM) for t in (pos, dz)))


def small_kernel(aux, b_trans, ln_gain, ln_bias, db, loss):
    c = lax.axis_index("dp") % 2
    for i, ref in enumerate((b_trans, ln_gain, ln_bias)):
        ref[...] = aux[0, ds(i * TILE, TILE), :]
    first, second = aux[ds(c, 1), ds(SMALL0 - VEC0, N_SMALL), :][0], aux[ds(1 - c, 1), ds(SMALL0 - VEC0, N_SMALL), :][0]
    rest = VROWS % L
    lane = lax.broadcasted_iota(jnp.int32, (LOSS_ROW, L), 1)
    second = pltpu.roll(second, rest, 1)
    db[ds(0, LOSS_ROW), :] = jnp.where((lane < rest) | (lax.broadcasted_iota(jnp.int32, (LOSS_ROW, L), 0) < LOSS_ROW - 1),
                                       first[:LOSS_ROW], second[:1])
    db[ds(LOSS_ROW, LOSS_ROW), :] = jnp.where(lane < rest, second[:LOSS_ROW], second[1:LOSS_ROW + 1])
    at = SMALL0 - VEC0 + LOSS_ROW
    total = aux[0, ds(at, 1), :] + aux[1, ds(at, 1), :] - aux[0, ds(at + 1, 1), :]
    loss[...] = jnp.sum(total, axis=1, keepdims=True)


def small_call(aux):
    vm = pl.BlockSpec(memory_space=VMEM)
    return pl.pallas_call(
        small_kernel,
        out_shape=tuple(jax.ShapeDtypeStruct(t, F32) for t in [(TILE, L)] * 3 + [(2 * LOSS_ROW, L), (1, 1)]),
        in_specs=[vm],
        out_specs=(vm,) * 5,
        name="small_results",
    )(aux)


def solution(mesh):
    n_groups = mesh.shape["dp"]

    def local_step(hidden, mask_pos, labels, w_trans, b_trans, ln_gain, ln_bias, emb_table, b_vocab):
        n_rows, seq_len, width = hidden.shape
        n_masks = mask_pos.shape[1]
        n_tokens = n_rows * n_masks * n_groups
        line = lambda v: v.reshape(1, v.shape[0])
        dz, aux, res = head_call(1.0 / n_tokens, mask_pos, labels, line(b_vocab), line(b_trans), line(ln_gain), line(ln_bias),
                                 hidden.reshape(n_rows * seq_len, width), emb_table, w_trans)
        d_emb, d_w_trans, d_hidden = write_call(res, mask_pos, dz)
        aux, d_w_trans = lax.optimization_barrier((aux, d_w_trans))
        *vecs, db, loss = small_call(aux)
        d_b_trans, d_gain, d_bias = (v.reshape(width) for v in vecs)
        d_b_vocab = db.reshape(2 * ROWS)[:2 * VROWS]
        return loss.reshape(()) / n_tokens, d_hidden.reshape(hidden.shape), d_w_trans, d_b_trans, d_gain, d_bias, d_emb, d_b_vocab

    in_specs = (P("dp", None, None), P("dp", None), P("dp", None), P(None, None), P(None), P(None), P(None), P("vp", None), P("vp"))
    out_specs = (P(), P("dp", None, None), P(None, None), P(None), P(None), P(None), P("vp", None), P("vp"))
    return jax.shard_map(local_step, mesh=mesh, in_specs=in_specs, out_specs=out_specs, check_vma=False)
```

```python
import functools

import jax
import jax.numpy as jnp
from jax import lax
from jax.experimental import pallas as pl
from jax.experimental.pallas import tpu as pltpu
from jax.sharding import PartitionSpec as P

MESH = pl.DeviceIdType.MESH
F32, BF = jnp.float32, jnp.bfloat16
VMEM, DMA, ds = pltpu.VMEM, pltpu.SemaphoreType.DMA, pl.ds
LN_EPS = 1e-5
HALF_SQRT, INV_SQRT_2PI = 0.7071067811865476, 0.3989422804014327
LOW, HIGH, NO_LABEL = -3e38, 3e38, -1e6
W, L, TILE, BTILE = 1024, 128, 8, 16
SEQS, SEQ, MASKS, SLOT = 6, 512, 77, 80
USED, TOK = SEQS * SLOT, 512
VROWS, ROWS, BLK = 3824, 3840, 384
N_BLK = ROWS // BLK
LAST = VROWS - (N_BLK - 1) * BLK
NCH = W // L
HALF, SH, SUB = ROWS // 2, ROWS // 8, ROWS // 32
CUT, SCUT = SH // 2, 64
SCUTS = (SCUT, SUB - SCUT)
QROWS, XROWS, XCUT = 128, 136, 72
VEC0, SMALL0, MINI = W, W + 24, 1280
MSH, MSUB = MINI // 8, MINI // 32
LOSS_ROW, N_SMALL = ROWS // L, 32
OTH0 = NCH * ROWS
DW0 = 2 * OTH0
MG0 = DW0 + 8 * W
TAIL0 = MG0 + MINI
TAIL = 64
OUT_ROWS = TAIL0 + TAIL
NSTAGE, EARLY = 8, 3
NEAR, FAR = (1, 3), 2
AROUND = NEAR + (FAR,)
TWO, THREE = (0, 1), (0, 1, 2)


def sl(start, n):
    return ds(pl.multiple_of(start, TILE), n)


def wait_all(cps):
    for cp in cps:
        cp.wait()


def start_all(cps):
    for cp in cps:
        cp.start()


def gelu_norm(a):
    cdf = 0.5 * (1.0 + lax.erf(a * HALF_SQRT))
    g = a * cdf
    cen = g - row_mean(g)
    rstd = lax.rsqrt(row_mean(cen * cen) + LN_EPS)
    return cdf, rstd, cen * rstd


def row_mean(t):
    return jnp.mean(t, axis=-1, keepdims=True)


def over_rows(fn, t):
    return fn(t, axis=0, keepdims=True)


def dot(a, b, ca=1, cb=0):
    return lax.dot_general(a, b, (((ca,), (cb,)), ((), ())), preferred_element_type=F32)


def lanes(j):
    return ds(j * L, L)


def add_rows(dst, srcs, n, blk):
    def body(i, carry):
        r = sl(i * blk, blk)
        v = dst[r, :]
        for s in srcs:
            v = v + s[r, :]
        dst[r, :] = v
        return carry
    lax.fori_loop(0, n // blk, body, 0)


def head_kernel(scale, pos_in, lab_in, b_in, b_trans, ln_gain, ln_bias, hidden, emb, w_in, dz, aux, out,
                gt, u_all, r1, r2, r3, r4, a1, a2, part, drx, xr1, dabx, dwrx, m8, mr1, mr2,
                wbuf, zbuf, abuf, pos, lab_own, bias, lab_rx, stat, stats, small,
                ssem, rsem, psend, precv, sem_h, sem_w, es, er, st_s, st_r, xs, xr, ms, mr):
    dp, vp = lax.axis_index("dp"), lax.axis_index("vp")
    z, y, c = dp // 8, (dp // 2) % 4, dp % 2
    ynb = [z * 8 + ((y + d) % 4) * 2 + c for d in AROUND]
    znb = [((z + d) % 4) * 8 + y * 2 + c for d in AROUND]
    xnb = [(vp + d) % 4 for d in AROUND]
    mate = dp + 1 - 2 * c
    peers = [{"vp": v, "dp": d} for v in xnb for d in (dp, mate)] + [{"vp": vp, "dp": mate}]

    def load_hidden(b):
        r = sl(b * SEQ, SEQ)
        return pltpu.make_async_copy(hidden.at[r], gt.at[r], sem_h.at[b])

    def load_emb(i, slot, n):
        return pltpu.make_async_copy(emb.at[ds(pl.multiple_of(c * VROWS, BTILE) + i * BLK, n)],
                                     wbuf.at[ds(pl.multiple_of(slot * BLK, BTILE), n)], sem_w.at[slot])

    load_w = pltpu.make_async_copy(w_in, u_all, sem_h.at[SEQS])
    store_dz = pltpu.make_async_copy(u_all.at[ds(0, TOK)], dz, sem_h.at[0])
    load_w_again = pltpu.make_async_copy(w_in, gt.at[ds(0, W)], sem_h.at[SEQS])
    for b in range(SEQS):
        load_hidden(b).start()
    load_w.start()
    load_emb(0, 0, BLK).start()

    barrier = pltpu.get_barrier_semaphore()
    greet = peers + [{"dp": d} for d in ynb + znb]
    for d in greet:
        pl.semaphore_signal(barrier, inc=1, device_id=d, device_id_type=MESH)

    def remote(src, dst, send, recv, dev):
        return pltpu.make_async_remote_copy(src_ref=src, dst_ref=dst, send_sem=send, recv_sem=recv,
                                            device_id=dev, device_id_type=MESH)

    def to_mate(src, dst, i):
        return remote(src, dst, es.at[i], er.at[i], {"dp": mate})

    def to_x(src, dst, i, d):
        return remote(src, dst, xs.at[i, d], xr.at[i, d], {"vp": xnb[d]})

    c_u = [to_mate(part, drx, 0), to_mate(lab_own, lab_rx, 1)]
    own0 = pl.multiple_of(c * TOK, TOK)
    oth0 = pl.multiple_of((1 - c) * TOK, TOK)

    pos[...] = jnp.full((TILE, L), -1, jnp.int32)
    pos[ds(0, SEQS), ds(0, MASKS)] = pos_in[...]
    lane = lax.broadcasted_iota(jnp.int32, (L, TOK), 1)
    seq = sum((lane >= b * SLOT).astype(jnp.int32) for b in range(1, SEQS))
    slot = lane - seq * SLOT
    place = jnp.where(slot == lax.broadcasted_iota(jnp.int32, (L, TOK), 0), 1.0, 0.0).astype(BF)[:MASKS]
    high, low = lab_in[...] >> 8, lab_in[...] & 255
    spread = dot(high.astype(F32).astype(BF), place) * 256.0 + dot(low.astype(F32).astype(BF), place)
    row = lax.broadcasted_iota(jnp.int32, (SEQS, TOK), 0)
    lab = over_rows(jnp.sum, jnp.where(row == seq[:SEQS], spread, 0.0))
    lab = jnp.where(slot[:1] < MASKS, lab, NO_LABEL)
    lab_own[...] = jnp.broadcast_to(lab, (TILE, TOK))
    rest = VROWS % L
    for core in TWO:
        @pl.when(c == core)
        def _():
            for i in range(VROWS // L):
                bias[ds(i, 1), :] = b_in[:, core * VROWS + i * L:core * VROWS + (i + 1) * L]
            bias[ds(LOSS_ROW - 1, 1), :] = jnp.full((1, L), LOW, F32)
            bias[ds(LOSS_ROW - 1, 1), ds(0, rest)] = b_in[:, (core + 1) * VROWS - rest:(core + 1) * VROWS]

    z0 = SEQS * SEQ

    def gather(b, carry):
        load_hidden(b).wait()
        where = jnp.broadcast_to(pos[ds(b, 1), :], (SEQ, L))
        hot = jnp.where(where == lax.broadcasted_iota(jnp.int32, (SEQ, L), 0), 1.0, 0.0).astype(BF)
        gt[ds(pl.multiple_of(z0 + b * SLOT, BTILE), SLOT), :] = dot(hot, gt[sl(b * SEQ, SEQ), :], 0, 0)[:SLOT].astype(BF)
        return carry

    gt[ds(z0 + USED, TOK - USED), :] = jnp.zeros((TOK - USED, W), BF)
    lax.fori_loop(0, SEQS, gather, 0)
    load_w.wait()
    zbuf[...] = gt[ds(z0, TOK), ds(pl.multiple_of(vp * 2 * L, L), 2 * L)]

    def transform(i, carry):
        r = sl(i * 2 * L, 2 * L)
        dabx[r, :] = dot(gt[ds(pl.multiple_of(z0 + i * 2 * L, L), 2 * L), :], u_all[...]) + b_trans[...]
        return carry

    lax.fori_loop(0, TOK // (2 * L), transform, 0)

    def norm(i, carry):
        r = sl(i * 4 * TILE, 4 * TILE)
        _, _, xhat = gelu_norm(dabx[r, :])
        part[r, :] = (xhat * ln_gain[...] + ln_bias[...]).astype(BF).astype(F32)
        return carry

    lax.fori_loop(0, TOK // (4 * TILE), norm, 0)
    abuf[...] = dabx[sl(vp * QROWS, QROWS), :]
    u_all[ds(own0, TOK), :] = part[...].astype(BF)
    pl.semaphore_wait(barrier, len(greet))
    start_all(c_u)

    def stream(body, init, again):
        def pair(m, carry):
            last = m + 1 == N_BLK // 2
            i = 2 * m
            for at, n in ((~last, BLK), (last, LAST)):
                pl.when(at)(load_emb(i + 1, 1, n).start)
            load_emb(i, 0, BLK).wait()
            carry = body(i, 0, wbuf[ds(0, BLK), :], carry)
            pl.when(~last)(load_emb(i + 2, 0, BLK).start)
            if again:
                pl.when(last)(load_emb(0, 0, BLK).start)
            for at, n in ((~last, BLK), (last, LAST)):
                pl.when(at)(load_emb(i + 1, 1, n).wait)
            return body(i + 1, 1, wbuf[ds(BLK, BLK), :], carry)
        return lax.fori_loop(0, N_BLK // 2, pair, init)

    row0 = (vp * 2 * VROWS + c * VROWS).astype(F32)

    def local_labels(ref):
        v = ref[0:1, :] - row0
        return jnp.where((v >= 0) & (v < VROWS), v, -1.0)

    def logits(tok0, again):
        u = u_all[ds(tok0, TOK), :]

        def sums(slot, top):
            return jnp.concatenate(
                [jnp.sum(jnp.exp(r2[slot, j // 2, j % 2, ds(0, BLK), :].reshape(BLK // TILE, TILE, L)
                                 - top[:, j * L:(j + 1) * L][None]), axis=0) for j in range(TOK // L)], axis=1)

        def block(i, slot, e, carry):
            old, mx, sm = carry
            sm = sm * jnp.exp(old - mx) + sums(1 - slot, mx)
            x = dot(e, u, 1, 1)
            col = [jnp.transpose(jnp.broadcast_to(bias[ds(i * (BLK // L) + j, 1), :], (L, L))) for j in range(BLK // L)]
            col = jnp.concatenate(col, axis=0)
            top = []
            for j in range(TOK // L):
                v = x[:, j * L:(j + 1) * L] + col
                out[sl((tok0 // L + j) * ROWS + i * BLK, BLK), :] = v
                r2[slot, j // 2, j % 2, ds(0, BLK), :] = v
                top.append(jnp.max(v.reshape(BLK // TILE, TILE, L), axis=0))
            return mx, jnp.maximum(mx, jnp.concatenate(top, axis=1)), sm

        low = jnp.full((TILE, TOK), LOW, F32)
        for j in range(TOK // L):
            r2[1, j // 2, j % 2, ds(0, BLK), :] = jnp.full((BLK, L), LOW, F32)
        old, mx, sm = stream(block, (low, low, jnp.zeros((TILE, TOK), F32)), again)
        sm = sm * jnp.exp(old - mx) + sums(1, mx)
        top = over_rows(jnp.max, mx)
        sm = over_rows(jnp.sum, sm * jnp.exp(mx - top))
        stat[:, ds(tok0, TOK)] = jnp.concatenate([top, sm, jnp.zeros((TILE - 2, TOK), F32)], axis=0)

    lab1 = local_labels(lab_own)
    logits(own0, True)
    wait_all(c_u)
    u_all[ds(oth0, TOK), :] = drx[...].astype(BF)
    lab2 = local_labels(lab_rx)
    logits(oth0, True)
    c_st = [remote(stat, stats.at[j], st_s.at[j], st_r.at[j], d) for j, d in enumerate(peers)]
    start_all(c_st)
    wait_all(c_st)
    mx, sm = (jnp.concatenate([stat[i:i + 1, :]] + [stats[j, i:i + 1, :] for j in range(len(peers))], axis=0)
              for i in TWO)
    top = over_rows(jnp.max, mx)
    norm = top + jnp.log(over_rows(jnp.sum, sm * jnp.exp(mx - top)))
    stat[0:1, :] = norm
    own_norm = jnp.where(lab_own[0:1, :] >= 0, stat[0:1, ds(own0, TOK)], 0.0)
    small[ds(LOSS_ROW, 1), :] = sum(own_norm[:, j * L:(j + 1) * L] for j in range(TOK // L))
    for t0, ref, lab in ((own0, lab_own, lab1), (oth0, lab_rx, lab2)):
        stat[0:1, ds(t0, TOK)] = jnp.where(ref[0:1, :] >= 0, stat[0:1, ds(t0, TOK)], HIGH)
        stat[1:2, ds(t0, TOK)] = lab

    def grad(i, target):
        ids = (lax.broadcasted_iota(jnp.int32, (L, L), 0) + i * L).astype(F32)
        s = jnp.zeros((L, L), F32)
        for j in range(2 * TOK // L):
            x = out[sl(j * ROWS + i * L, L), :]
            hit = ids == stat[1:2, lanes(j)]
            g = (jnp.exp(x - stat[0:1, lanes(j)]) - jnp.where(hit, 1.0, 0.0)) * scale
            gt[ds(pl.multiple_of(i * L, L), L), lanes(j)] = g.astype(BF)
            s = s + g
            target = target + jnp.where(hit, x, 0.0)
        small[ds(i, 1), :] = over_rows(jnp.sum, jnp.transpose(s))
        return target

    target = lax.fori_loop(0, ROWS // L, grad, jnp.zeros((L, L), F32))
    small[ds(LOSS_ROW + 1, 1), :] = over_rows(jnp.sum, target)

    def rows(k, start, n):
        return out.at[sl(k * ROWS + start, n)]

    halves = []
    for b, p, pn, q, qn in ((0, y, ynb, z, znb), (HALF, z, znb, y, ynb)):
        pc, qc = ([(t + d) % 4 * n for d in NEAR] for t, n in ((p, SH), (q, SUB)))
        halves.append((b, pn, qn, pc, qc, b + (p + FAR) % 4 * SH, b + p * SH, (q + FAR) % 4 * SUB, q * SUB))

    def stage_copies(st, k):
        cps = []
        for h, (b, pn, qn, pc, qc, po, b2, qo, q0) in enumerate(halves):
            for d in TWO:
                n = SCUTS[d]
                if st == 0:
                    a = rows(k, po + d * CUT, CUT), r1.at[k % EARLY, h, d], pn
                elif st == 1:
                    a = rows(k, b + pc[d], SH), r2.at[k % 2, h, d], pn
                elif st == 2:
                    a = rows(k, b2 + qo + d * SCUT, n), r3.at[k % 3, h, d, ds(0, n)], qn
                elif st == 3:
                    a = rows(k, b2 + qc[d], SUB), r4.at[k % 3, h, d], qn
                elif st == 4:
                    a = rows(k, b2 + q0, SUB), a1.at[k % 4, h, d], qn
                elif st == 5:
                    a = a1.at[k % 4, h, d, ds(d * SCUT, n)], a2.at[k % 3, h, d, ds(0, n)], qn
                elif st == 6:
                    a = rows(k, b2, SH), rows(k, b2, SH), pn
                else:
                    s = rows(k, b + pc[1 - d] + d * CUT, CUT)
                    a = s, s, pn
                src, dst, nb = a
                cps.append(remote(src, dst, ssem.at[st, h, d, k], rsem.at[st, h, d, k], {"dp": nb[d]}))
        return cps

    def mate_copies(k, far):
        cps = []
        for h, (b, pn, qn, pc, qc, po, b2, qo, q0) in enumerate(halves):
            for i, r in enumerate([b2] + [b + t for t in pc] + [po]):
                if far == (i == 3):
                    cps.append(remote(rows(k, r, SH), rows(k, OTH0 + r, SH), psend.at[k, h, i], precv.at[k, h, i], {"dp": mate}))
        return cps

    def mm(k, r):
        r = pl.multiple_of(r, BTILE)
        rows(k, r, SH)[...] = dot(gt[ds(r, SH), :], u_all[:, ds(pl.multiple_of(k * L, L), L)])

    def first_rows(k):
        for h in halves:
            mm(k, h[5])
        start_all(stage_copies(0, k))

    def other_rows(k):
        def shard(i, carry):
            mm(k, i // 3 * HALF + (jnp.where(i < 3, y, z) + (i % 3 + 3)) % 4 * SH)
            return carry
        lax.fori_loop(0, 6, shard, 0)

    def stage(st, k):
        if st == 0:
            first_rows(k)
            other_rows(k)
            return
        wait_all(stage_copies(st - 1, k))
        for h, (b, pn, qn, pc, qc, po, b2, qo, q0) in enumerate(halves):
            both = lambda r, m: [r.at[k % m, h, d] for d in TWO]
            if st == 2:
                add_rows(rows(k, b2, SH), both(r2, 2), SH, SLOT)
            elif st == 4:
                add_rows(rows(k, b2 + q0, SUB), both(r4, 3), SUB, SUB)
            for d in TWO:
                n = SCUTS[d]
                if st == 1:
                    add_rows(rows(k, b + pc[d] + d * CUT, CUT), [r1.at[k % EARLY, h, d]], CUT, SLOT)
                elif st == 3:
                    add_rows(rows(k, b2 + qc[d] + d * SCUT, n), [r3.at[k % 3, h, d]], n, n)
                elif st == 5:
                    rows(k, b2 + qc[1 - d], SUB)[...] = a1[k % 4, h, d]
                elif st == 6:
                    rows(k, b2 + qo + d * SCUT, n)[...] = a2[k % 3, h, d, ds(0, n)]
        if st < NSTAGE:
            start_all(stage_copies(st, k))
        if st + 1 >= NSTAGE:
            start_all(mate_copies(k, st == NSTAGE))

    xp, xm, xo = xnb

    def qrow(q, o, n):
        return sl(q * QROWS + o, n)

    def arow(q, o, n):
        return sl(q * XROWS + o, n)

    def same(ref, r):
        return ref.at[r], ref.at[r]

    def dwrow(j, o, n):
        return sl(DW0 + j * W + o, n)

    XTWO = ((xo, 0), (xo, QROWS // 2))
    c_du = [to_mate(part, drx, 2)]
    c_x1 = [to_x(drx.at[qrow(q, o, QROWS // 2)], xr1.at[d], 0, d) for d, (q, o) in enumerate(XTWO)]
    c_x2 = [to_x(drx.at[qrow(xnb[d], 0, QROWS)], part.at[ds(d * QROWS, QROWS)], 1, d) for d in TWO]
    c_x3 = [to_x(*same(dabx, arow(vp, 0, XROWS)), 2, d) for d in TWO]
    c_x4 = [to_x(*same(dabx, arow(q, o, n)), 3, d)
            for d, (q, o, n) in enumerate(((xm, 0, XCUT), (xp, XCUT, XROWS - XCUT)))]
    c_dw = [to_mate(part.at[qrow(1 - c, 0, QROWS)], dwrx.at[ds(0, QROWS)], 3),
            to_mate(part.at[ds(2 * QROWS, TILE)], dwrx.at[ds(QROWS, TILE)], 4)]
    c_w1 = [to_x(*same(out, dwrow(vp, 0, W)), 4, d) for d in TWO]
    c_w2 = [to_x(*same(out, dwrow(q, d * (W // 2), W // 2)), 5, d) for d, q in enumerate((xm, xp))]
    c_w3 = [to_mate(out.at[ds(DW0, 4 * W)], out.at[ds(DW0 + 4 * W, 4 * W)], 5),
            to_mate(out.at[ds(MG0 + W, TAIL)], out.at[ds(TAIL0, TAIL)], 6)]

    def du_part(col0, dst, again):
        def block(i, slot, e, carry):
            dst[...] += dot(gt[ds(pl.multiple_of(i * BLK, L), BLK), ds(col0, TOK)], e, 0, 0)
            return carry
        stream(block, 0, again)

    def du_theirs():
        part[...] = jnp.zeros((TOK, W), F32)
        du_part(oth0, part, True)
        start_all(c_du)

    def du_mine():
        wait_all(c_du)
        du_part(own0, drx, False)

        def rnd(i, carry):
            r = sl(i * SCUT, SCUT)
            drx[r, :] = drx[r, :].astype(BF).astype(F32)
            return carry

        lax.fori_loop(0, TOK // SCUT, rnd, 0)
        start_all(c_x1)

    def du_near():
        wait_all(c_x1)
        for d, o in ((0, 0), (1, QROWS // 2)):
            drx[qrow(xnb[d], o, QROWS // 2), :] += xr1[d]
        start_all(c_x2)

    def norm_back():
        wait_all(c_x2)

        def block(i, sums):
            r = sl(i * 2 * TILE, 2 * TILE)
            a = abuf[r, :]
            dun = drx[qrow(vp, i * 2 * TILE, 2 * TILE), :] + part[r, :] + part[sl(QROWS + i * 2 * TILE, 2 * TILE), :]
            cdf, rstd, xhat = gelu_norm(a)
            dx = dun * ln_gain[...]
            dg = rstd * (dx - row_mean(dx) - xhat * row_mean(dx * xhat))
            da = dg * (cdf + a * jnp.exp(-0.5 * a * a) * INV_SQRT_2PI)
            dabx[arow(vp, i * 2 * TILE, 2 * TILE), :] = da.astype(BF).astype(F32)
            return tuple(s + t[:TILE] + t[TILE:] for s, t in zip(sums, (da, dun * xhat, dun)))

        sums = lax.fori_loop(0, QROWS // (2 * TILE), block, (jnp.zeros((TILE, W), F32),) * 3)
        sums = [over_rows(jnp.sum, t) for t in sums]
        sums.append(jnp.concatenate([small[ds(LOSS_ROW + 1, 1), :], jnp.zeros((1, W - L), F32)], axis=1))
        dabx[arow(vp, QROWS, TILE), :] = jnp.concatenate(sums + [jnp.zeros((TILE - len(sums), W), F32)], axis=0)
        start_all(c_x3)

    def pass_on():
        wait_all(c_x3)
        start_all(c_x4)

    def dab(q):
        return dabx[arow(q, 0, QROWS), :].astype(BF)

    def weight_grad():
        wait_all(c_x4)
        part[ds(0, 2 * QROWS), :] = sum(dot(zbuf[qrow(q, 0, QROWS), :], dab(q), 0, 0) for q in range(4))
        part[ds(2 * QROWS, TILE), :] = sum(dabx[arow(q, QROWS, TILE), :] for q in range(4))
        start_all(c_dw)

    def input_grad():
        load_w_again.start()
        wait_all(c_dw)
        for j in range(W // L):
            m8[lanes(j), :] = part[qrow(c, 0, QROWS), lanes(j)] + dwrx[ds(0, QROWS), lanes(j)]
            v = part[ds(2 * QROWS, TILE), lanes(j)] + dwrx[ds(QROWS, TILE), lanes(j)]
            for i in THREE:
                m8[ds(VEC0 + i * TILE + j, 1), :] = v[i:i + 1]
            if j == 0:
                small[ds(LOSS_ROW + 1, 1), :] = v[3:4]
        m8[ds(SMALL0, N_SMALL), :] = small[...]
        m8[ds(SMALL0 + N_SMALL, MINI - SMALL0 - N_SMALL), :] = jnp.zeros((MINI - SMALL0 - N_SMALL, L), F32)
        start_all(mini_copies(0))

    mini = ((0, y, ynb, z, znb), (MINI // 2, z, znb, y, ynb))

    def mini_copies(st):
        cps = []
        for h, (b, p, pn, q, qn) in enumerate(mini):
            b2 = b + p * MSH
            for d, off in enumerate(AROUND):
                if st == 0:
                    a = m8.at[sl(b + (p + off) % 4 * MSH, MSH)], mr1.at[h, d], pn
                elif st == 1:
                    a = m8.at[sl(b2 + (q + off) % 4 * MSUB, MSUB)], mr2.at[h, d], qn
                elif st == 2:
                    a = *same(out, sl(MG0 + b2 + q * MSUB, MSUB)), qn
                else:
                    a = *same(out, sl(MG0 + b2, MSH)), pn
                src, dst, nb = a
                cps.append(remote(src, dst, ms.at[st, h, d], mr.at[st, h, d], {"dp": nb[d]}))
        return cps

    def mini_first():
        load_w_again.wait()
        for q in range(4):
            u_all[qrow(q, 0, QROWS), :] = dot(dab(q), gt[ds(0, W), :], 1, 1).astype(BF)
        store_dz.start()
        wait_all(mini_copies(0))
        for h, (b, p, pn, q, qn) in enumerate(mini):
            r = sl(b + p * MSH, MSH)
            m8[r, :] = m8[r, :] + sum(mr1[h, d] for d in THREE)
        start_all(mini_copies(1))

    def mini_second():
        store_dz.wait()
        wait_all(mini_copies(1))
        for h, (b, p, pn, q, qn) in enumerate(mini):
            r = b + p * MSH + q * MSUB
            out[sl(MG0 + r, MSUB), :] = m8[sl(r, MSUB), :] + sum(mr2[h, d] for d in THREE)
        start_all(mini_copies(2))

    def mini_third():
        wait_all(mini_copies(2))
        start_all(mini_copies(3))

    def weight_x():
        wait_all(mini_copies(3))
        out[dwrow(vp, 0, W), :] = out[ds(MG0, W), :]
        start_all(c_w1)

    def weight_on():
        wait_all(c_w1)
        start_all(c_w2)

    def weight_mate():
        wait_all(c_w2)
        start_all(c_w3)

    pieces = (du_theirs, du_mine, du_near, norm_back, pass_on, weight_grad, input_grad,
              mini_first, mini_second, mini_third, weight_x, weight_on, weight_mate)

    def step(stages, now, t, carry):
        for st in stages:
            k = t - st
            pl.when((k >= (0 if st else EARLY)) & (k < NCH))(functools.partial(stage, st, k))
        for at, piece in now:
            pl.when(t == at)(piece)
        return carry

    timed = [(at, piece) for at, piece in enumerate(pieces, 1)]
    filling = functools.partial(step, range(NSTAGE - 1, -1, -1), [p for p in timed if p[0] < NCH])
    emptying = functools.partial(step, range(1, NSTAGE + 1), [p for p in timed if p[0] >= NCH])
    for k in range(EARLY):
        first_rows(k)
    for k in range(EARLY):
        other_rows(k)
    lax.fori_loop(1, NCH, filling, 0)
    lax.fori_loop(NCH, NCH + NSTAGE, emptying, 0)

    def drain(k, carry):
        for far in (False, True):
            wait_all(mate_copies(k, far))
        return carry

    lax.fori_loop(0, NCH, drain, 0)
    wait_all(c_w3)
    save = [pltpu.make_async_copy(out.at[ds(r, TAIL)], aux.at[j], sem_w.at[j]) for j, r in enumerate((MG0 + W, TAIL0))]
    start_all(save)
    wait_all(save)


def head_call(scale, *args):
    vm, hbm = (pl.BlockSpec(memory_space=s) for s in (VMEM, pltpu.HBM))
    pair = (2, 2)
    sems = [(NSTAGE,) + pair + (NCH,)] * 2 + [(NCH, 2, 4)] * 2 + [(SEQS + 1,), pair[:1]] + [(7,)] * 4 + [(6, 2)] * 2 + [(4, 2, 3)] * 2
    return pl.pallas_call(
        functools.partial(head_kernel, scale),
        out_shape=(jax.ShapeDtypeStruct((TOK, W), BF), jax.ShapeDtypeStruct((2, TAIL, L), F32), VMEM((OUT_ROWS, L), F32)),
        in_specs=[vm] * 6 + [hbm] * 3,
        out_specs=(hbm, hbm, vm),
        scratch_shapes=[
            VMEM((ROWS, 2 * TOK), BF), VMEM((2 * TOK, W), BF),
            VMEM((EARLY,) + pair + (CUT, L), F32), VMEM((2,) + pair + (SH, L), F32), VMEM((3,) + pair + (SCUT, L), F32),
            VMEM((3,) + pair + (SUB, L), F32), VMEM((4,) + pair + (SUB, L), F32), VMEM((3,) + pair + (SCUT, L), F32),
            VMEM((TOK, W), F32), VMEM((TOK, W), F32), VMEM((2, QROWS // 2, W), F32),
            VMEM((4 * XROWS, W), F32), VMEM((XROWS, W), F32), VMEM((MINI, L), F32), VMEM((2, 3, MSH, L), F32),
            VMEM((2, 3, MSUB, L), F32), VMEM((2 * BLK, W), BF), VMEM((TOK, 2 * L), BF), VMEM((QROWS, W), F32),
            VMEM((TILE, L), jnp.int32), VMEM((TILE, TOK), F32), VMEM((N_SMALL, L), F32), VMEM((TILE, TOK), F32), VMEM((TILE, 2 * TOK), F32), VMEM((7, TILE, 2 * TOK), F32),
            VMEM((N_SMALL, L), F32),
        ] + [DMA(s) for s in sems],
        compiler_params=pltpu.CompilerParams(collective_id=0, has_side_effects=True, vmem_limit_bytes=30655000),
        name="mlm_head",
    )(*args)


def write_kernel(res, pos_in, dz_in, d_emb, d_w, d_hid, hid, pos, dz, sem, sem_w, sem_h, sem_i):
    c = lax.axis_index("dp") % 2
    cps = []
    for j, core in enumerate((c, 1 - c)):
        for k in range(NCH):
            cps.append(pltpu.make_async_copy(
                res.at[ds(j * OTH0 + k * ROWS, VROWS)], d_emb.at[sl(core * VROWS, VROWS), lanes(k)], sem.at[k, j]))
            for x in range(4):
                cps.append(pltpu.make_async_copy(
                    res.at[ds(DW0 + (j * 4 + x) * W + k * L, L)],
                    d_w.at[sl(x * 2 * L + core * L, L), lanes(k)], sem_w.at[k, j, x]))
    loads = [pltpu.make_async_copy(src, dst, sem_i.at[j]) for j, (src, dst) in enumerate(((pos_in, pos), (dz_in, dz)))]
    start_all(loads)
    start_all(cps)
    wait_all(loads)
    for b in range(SEQS):
        where = jnp.broadcast_to(jnp.concatenate([pos[b:b + 1, :], jnp.full((1, L - MASKS), -1, jnp.int32)], axis=1), (SEQ, L))
        hot = jnp.where(where == lax.broadcasted_iota(jnp.int32, (SEQ, L), 0), 1.0, 0.0).astype(BF)
        rows = jnp.concatenate([dz[b * SLOT:(b + 1) * SLOT, :], jnp.zeros((L - SLOT, W), BF)], axis=0)
        r = ds(b * SEQ, SEQ)
        hid[r, :] = dot(hot, rows).astype(BF)
        cp = pltpu.make_async_copy(hid.at[r], d_hid.at[r], sem_h.at[b])
        cp.start()
        cps.append(cp)
    wait_all(cps)


def write_call(res, pos, dz):
    vm, hbm = (pl.BlockSpec(memory_space=s) for s in (VMEM, pltpu.HBM))
    return pl.pallas_call(
        write_kernel,
        out_shape=tuple(jax.ShapeDtypeStruct(s, t) for s, t in (
            ((2 * VROWS, W), F32), ((W, W), F32), ((SEQS * SEQ, W), BF))),
        in_specs=[vm, hbm, hbm],
        out_specs=(hbm,) * 3,
        scratch_shapes=[VMEM((SEQS * SEQ, W), BF), VMEM((SEQS, MASKS), jnp.int32), VMEM((TOK, W), BF), DMA((NCH, 2)), DMA((NCH, 2, 4)),
                        DMA((SEQS,)), DMA((2,))],
        compiler_params=pltpu.CompilerParams(vmem_limit_bytes=16 << 20),
        name="write_rows",
    )(res, *(pltpu.with_memory_space_constraint(t, pltpu.HBM) for t in (pos, dz)))


def small_kernel(aux, b_trans, ln_gain, ln_bias, db, loss):
    c = lax.axis_index("dp") % 2
    for i, ref in enumerate((b_trans, ln_gain, ln_bias)):
        ref[...] = aux[0, ds(i * TILE, TILE), :]
    first, second = aux[ds(c, 1), ds(SMALL0 - VEC0, N_SMALL), :][0], aux[ds(1 - c, 1), ds(SMALL0 - VEC0, N_SMALL), :][0]
    rest = VROWS % L
    lane = lax.broadcasted_iota(jnp.int32, (LOSS_ROW, L), 1)
    second = pltpu.roll(second, rest, 1)
    db[ds(0, LOSS_ROW), :] = jnp.where((lane < rest) | (lax.broadcasted_iota(jnp.int32, (LOSS_ROW, L), 0) < LOSS_ROW - 1),
                                       first[:LOSS_ROW], second[:1])
    db[ds(LOSS_ROW, LOSS_ROW), :] = jnp.where(lane < rest, second[:LOSS_ROW], second[1:LOSS_ROW + 1])
    at = SMALL0 - VEC0 + LOSS_ROW
    total = aux[0, ds(at, 1), :] + aux[1, ds(at, 1), :] - aux[0, ds(at + 1, 1), :]
    loss[...] = jnp.sum(total, axis=1, keepdims=True)


def small_call(aux):
    vm = pl.BlockSpec(memory_space=VMEM)
    return pl.pallas_call(
        small_kernel,
        out_shape=tuple(jax.ShapeDtypeStruct(t, F32) for t in [(TILE, L)] * 3 + [(2 * LOSS_ROW, L), (1, 1)]),
        in_specs=[vm],
        out_specs=(vm,) * 5,
        name="small_results",
    )(aux)


def solution(mesh):
    n_groups = mesh.shape["dp"]

    def local_step(hidden, mask_pos, labels, w_trans, b_trans, ln_gain, ln_bias, emb_table, b_vocab):
        n_rows, seq_len, width = hidden.shape
        n_masks = mask_pos.shape[1]
        n_tokens = n_rows * n_masks * n_groups
        line = lambda v: v.reshape(1, v.shape[0])
        dz, aux, res = head_call(1.0 / n_tokens, mask_pos, labels, line(b_vocab), line(b_trans), line(ln_gain), line(ln_bias),
                                 hidden.reshape(n_rows * seq_len, width), emb_table, w_trans)
        d_emb, d_w_trans, d_hidden = write_call(res, mask_pos, dz)
        aux, d_w_trans = lax.optimization_barrier((aux, d_w_trans))
        *vecs, db, loss = small_call(aux)
        d_b_trans, d_gain, d_bias = (v.reshape(width) for v in vecs)
        d_b_vocab = db.reshape(2 * ROWS)[:2 * VROWS]
        return loss.reshape(()) / n_tokens, d_hidden.reshape(hidden.shape), d_w_trans, d_b_trans, d_gain, d_bias, d_emb, d_b_vocab

    in_specs = (P("dp", None, None), P("dp", None), P("dp", None), P(None, None), P(None), P(None), P(None), P("vp", None), P("vp"))
    out_specs = (P(), P("dp", None, None), P(None, None), P(None), P(None), P(None), P("vp", None), P("vp"))
    return jax.shard_map(local_step, mesh=mesh, in_specs=in_specs, out_specs=out_specs, check_vma=False)
```

```python
import functools
import math

import jax
import jax.numpy as jnp
from jax import lax
from jax.experimental import pallas as pl
from jax.experimental.pallas import tpu as pltpu
from jax.sharding import PartitionSpec as P

MESH = pl.DeviceIdType.MESH
F32, BF = jnp.float32, jnp.bfloat16
VMEM, DMA, ds = pltpu.VMEM, pltpu.SemaphoreType.DMA, pl.ds
LN_EPS = 1e-5
HALF_SQRT, INV_SQRT_2PI = 0.7071067811865476, 0.3989422804014327
LOW, HIGH, NO_LABEL = -3e38, 3e38, -1e6
W, L, TILE, BTILE = 1024, 128, 8, 16
SEQS, SEQ, MASKS, SLOT = 6, 512, 77, 80
USED, TOK = SEQS * SLOT, 512
VROWS, ROWS, BLK = 3824, 3840, 384
N_BLK = ROWS // BLK
LAST = VROWS - (N_BLK - 1) * BLK
NCH = W // L
HALF, SH, SUB = ROWS // 2, ROWS // 8, ROWS // 32
CUT, SCUT = SH // 2, 64
SCUTS = (SCUT, SUB - SCUT)
QROWS, XROWS, XCUT = 128, 136, 72
VEC0, SMALL0, MINI = W, W + 24, 1280
MSH, MSUB = MINI // 8, MINI // 32
MCUT = MSH // 2
LOSS_ROW, N_SMALL = ROWS // L, 32
OTH0 = NCH * ROWS
DW0 = 2 * OTH0
MG0 = DW0 + 8 * W
TAIL0 = MG0 + MINI
TAIL = 64
OUT_ROWS = TAIL0 + TAIL
NSTAGE, EARLY = 8, 3
NEAR, FAR = (1, 3), 2
AROUND = NEAR + (FAR,)
TWO, THREE = (0, 1), (0, 1, 2)
FIRST, SECOND = slice(0, 1), slice(1, 2)


def sl(start, n):
    return ds(pl.multiple_of(start, TILE), n)


def wait_all(cps):
    for cp in cps:
        cp.wait()


def start_all(cps):
    for cp in cps:
        cp.start()


def gelu_norm(a):
    cdf = 0.5 * (1.0 + lax.erf(a * HALF_SQRT))
    g = a * cdf
    cen = g - row_mean(g)
    rstd = lax.rsqrt(row_mean(cen * cen) + LN_EPS)
    return cdf, rstd, cen * rstd


def row_mean(t):
    return jnp.mean(t, axis=-1, keepdims=True)


def over_rows(fn, t):
    return fn(t, axis=0, keepdims=True)


def dot(a, b, ca=1, cb=0):
    return lax.dot_general(a, b, (((ca,), (cb,)), ((), ())), preferred_element_type=F32)


def lanes(j):
    return ds(j * L, L)


def add_rows(dst, srcs, n, blk):
    def body(i, carry):
        r = sl(i * blk, blk)
        v = dst[r, :]
        for s in srcs:
            v = v + s[r, :]
        dst[r, :] = v
        return carry
    lax.fori_loop(0, n // blk, body, 0)


def head_kernel(scale, pos_in, lab_in, b_in, b_trans, ln_gain, ln_bias, hidden, emb, w_in, dz, aux, out,
                gt, u_all, r1, r2, r3, r4, a1, a2, part, drx, xr1, dabx, dwrx, m8, mr1, mr2,
                wbuf, zbuf, abuf, pos, lab_own, bias, lab_rx, stat, stats, small,
                ssem, rsem, psend, precv, sem_h, sem_w, es, er, st_s, st_r, xs, xr, ms, mr):
    dp, vp = lax.axis_index("dp"), lax.axis_index("vp")
    z, y, c = dp // 8, (dp // 2) % 4, dp % 2
    ynb = [z * 8 + ((y + d) % 4) * 2 + c for d in AROUND]
    znb = [((z + d) % 4) * 8 + y * 2 + c for d in AROUND]
    xnb = [(vp + d) % 4 for d in AROUND]
    mate = dp + 1 - 2 * c
    peers = [{"vp": v, "dp": d} for v in xnb for d in (dp, mate)] + [{"vp": vp, "dp": mate}]

    def load_hidden(b):
        r = sl(b * SEQ, SEQ)
        return pltpu.make_async_copy(hidden.at[r], gt.at[r], sem_h.at[b])

    def load_emb(i, slot, n):
        return pltpu.make_async_copy(emb.at[ds(pl.multiple_of(c * VROWS, BTILE) + i * BLK, n)],
                                     wbuf.at[ds(pl.multiple_of(slot * BLK, BTILE), n)], sem_w.at[slot])

    load_w = pltpu.make_async_copy(w_in, u_all, sem_h.at[SEQS])
    store_dz = pltpu.make_async_copy(u_all.at[ds(0, TOK)], dz, sem_h.at[0])
    load_w_again = pltpu.make_async_copy(w_in, gt.at[ds(0, W)], sem_h.at[SEQS])
    for b in range(SEQS):
        load_hidden(b).start()
    load_w.start()
    load_emb(0, 0, BLK).start()

    barrier = pltpu.get_barrier_semaphore()
    greet = peers + [{"dp": d} for d in ynb + znb]
    for d in greet:
        pl.semaphore_signal(barrier, inc=1, device_id=d, device_id_type=MESH)

    def remote(src, dst, send, recv, dev):
        return pltpu.make_async_remote_copy(src_ref=src, dst_ref=dst, send_sem=send, recv_sem=recv,
                                            device_id=dev, device_id_type=MESH)

    def to_mate(src, dst, i):
        return remote(src, dst, es.at[i], er.at[i], {"dp": mate})

    def to_x(src, dst, i, d):
        return remote(src, dst, xs.at[i, d], xr.at[i, d], {"vp": xnb[d]})

    c_u = [to_mate(part, drx, 0), to_mate(lab_own, lab_rx, 1)]
    own0 = pl.multiple_of(c * TOK, TOK)
    oth0 = pl.multiple_of((1 - c) * TOK, TOK)

    pos[...] = jnp.full((TILE, L), -1, jnp.int32)
    pos[ds(0, SEQS), ds(0, MASKS)] = pos_in[...]
    lane = lax.broadcasted_iota(jnp.int32, (L, TOK), 1)
    seq = sum((lane >= b * SLOT).astype(jnp.int32) for b in range(1, SEQS))
    slot = lane - seq * SLOT
    place = jnp.where(slot == lax.broadcasted_iota(jnp.int32, (L, TOK), 0), 1.0, 0.0).astype(BF)[:MASKS]
    high, low = lab_in[...] >> 8, lab_in[...] & 255
    spread = dot(high.astype(F32).astype(BF), place) * 256.0 + dot(low.astype(F32).astype(BF), place)
    row = lax.broadcasted_iota(jnp.int32, (SEQS, TOK), 0)
    lab = over_rows(jnp.sum, jnp.where(row == seq[:SEQS], spread, 0.0))
    lab = jnp.where(slot[:1] < MASKS, lab, NO_LABEL)
    lab_own[...] = jnp.broadcast_to(lab, (TILE, TOK))
    rest = VROWS % L
    for core in TWO:
        @pl.when(c == core)
        def _():
            for i in range(VROWS // L):
                bias[ds(i, 1), :] = b_in[:, core * VROWS + i * L:core * VROWS + (i + 1) * L]
            bias[ds(LOSS_ROW - 1, 1), :] = jnp.full((1, L), LOW, F32)
            bias[ds(LOSS_ROW - 1, 1), ds(0, rest)] = b_in[:, (core + 1) * VROWS - rest:(core + 1) * VROWS]

    z0 = SEQS * SEQ

    def gather(b, carry):
        load_hidden(b).wait()
        where = jnp.broadcast_to(pos[ds(b, 1), :], (SEQ, L))
        hot = jnp.where(where == lax.broadcasted_iota(jnp.int32, (SEQ, L), 0), 1.0, 0.0).astype(BF)
        gt[ds(pl.multiple_of(z0 + b * SLOT, BTILE), SLOT), :] = dot(hot, gt[sl(b * SEQ, SEQ), :], 0, 0)[:SLOT].astype(BF)
        return carry

    gt[ds(z0 + USED, TOK - USED), :] = jnp.zeros((TOK - USED, W), BF)
    lax.fori_loop(0, SEQS, gather, 0)
    load_w.wait()
    zbuf[...] = gt[ds(z0, TOK), ds(pl.multiple_of(vp * 2 * L, L), 2 * L)]

    def transform(i, carry):
        r = sl(i * 2 * L, 2 * L)
        dabx[r, :] = dot(gt[ds(pl.multiple_of(z0 + i * 2 * L, L), 2 * L), :], u_all[...]) + b_trans[...]
        return carry

    lax.fori_loop(0, TOK // (2 * L), transform, 0)

    def norm(i, carry):
        r = sl(i * 4 * TILE, 4 * TILE)
        _, _, xhat = gelu_norm(dabx[r, :])
        part[r, :] = (xhat * ln_gain[...] + ln_bias[...]).astype(BF).astype(F32)
        return carry

    lax.fori_loop(0, TOK // (4 * TILE), norm, 0)
    abuf[...] = dabx[sl(vp * QROWS, QROWS), :]
    u_all[ds(own0, TOK), :] = part[...].astype(BF)
    pl.semaphore_wait(barrier, len(greet))
    start_all(c_u)

    def stream(body, init, again):
        def pair(m, carry):
            last = m + 1 == N_BLK // 2
            i = 2 * m
            for at, n in ((~last, BLK), (last, LAST)):
                pl.when(at)(load_emb(i + 1, 1, n).start)
            load_emb(i, 0, BLK).wait()
            carry = body(i, 0, wbuf[ds(0, BLK), :], carry)
            pl.when(~last)(load_emb(i + 2, 0, BLK).start)
            if again:
                pl.when(last)(load_emb(0, 0, BLK).start)
            for at, n in ((~last, BLK), (last, LAST)):
                pl.when(at)(load_emb(i + 1, 1, n).wait)
            return body(i + 1, 1, wbuf[ds(BLK, BLK), :], carry)
        return lax.fori_loop(0, N_BLK // 2, pair, init)

    row0 = (vp * 2 * VROWS + c * VROWS).astype(F32)

    def local_labels(ref):
        v = ref[FIRST, :] - row0
        return jnp.where((v >= 0) & (v < VROWS), v, -1.0)

    def logits(tok0, again):
        u = u_all[ds(tok0, TOK), :]

        def sums(slot, top):
            return jnp.concatenate(
                [jnp.sum(jnp.exp(r2[slot, j // 2, j % 2, ds(0, BLK), :].reshape(BLK // TILE, TILE, L)
                                 - top[:, j * L:(j + 1) * L][None]), axis=0) for j in range(TOK // L)], axis=1)

        def block(i, slot, e, carry):
            old, mx, sm = carry
            sm = sm * jnp.exp(old - mx) + sums(1 - slot, mx)
            x = dot(e, u, 1, 1)
            col = [jnp.transpose(jnp.broadcast_to(bias[ds(i * (BLK // L) + j, 1), :], (L, L))) for j in range(BLK // L)]
            col = jnp.concatenate(col, axis=0)
            top = []
            for j in range(TOK // L):
                v = x[:, j * L:(j + 1) * L] + col
                out[sl((tok0 // L + j) * ROWS + i * BLK, BLK), :] = v
                r2[slot, j // 2, j % 2, ds(0, BLK), :] = v
                top.append(jnp.max(v.reshape(BLK // TILE, TILE, L), axis=0))
            return mx, jnp.maximum(mx, jnp.concatenate(top, axis=1)), sm

        low = jnp.full((TILE, TOK), LOW, F32)
        for j in range(TOK // L):
            r2[1, j // 2, j % 2, ds(0, BLK), :] = jnp.full((BLK, L), LOW, F32)
        old, mx, sm = stream(block, (low, low, jnp.zeros((TILE, TOK), F32)), again)
        sm = sm * jnp.exp(old - mx) + sums(1, mx)
        top = over_rows(jnp.max, mx)
        sm = over_rows(jnp.sum, sm * jnp.exp(mx - top))
        stat[:, ds(tok0, TOK)] = jnp.concatenate([top, sm, jnp.zeros((TILE - 2, TOK), F32)], axis=0)

    lab1 = local_labels(lab_own)
    logits(own0, True)
    wait_all(c_u)
    u_all[ds(oth0, TOK), :] = drx[...].astype(BF)
    lab2 = local_labels(lab_rx)
    logits(oth0, True)
    c_st = [remote(stat, stats.at[j], st_s.at[j], st_r.at[j], d) for j, d in enumerate(peers)]
    start_all(c_st)
    wait_all(c_st)
    mx, sm = (jnp.concatenate([stat[i:i + 1, :]] + [stats[j, i:i + 1, :] for j in range(len(peers))], axis=0)
              for i in TWO)
    top = over_rows(jnp.max, mx)
    norm = top + jnp.log(over_rows(jnp.sum, sm * jnp.exp(mx - top)))
    stat[FIRST, :] = norm
    own_norm = jnp.where(lab_own[FIRST, :] >= 0, stat[FIRST, ds(own0, TOK)], 0.0)
    small[ds(LOSS_ROW, 1), :] = sum(own_norm[:, j * L:(j + 1) * L] for j in range(TOK // L))
    for t0, ref, lab in ((own0, lab_own, lab1), (oth0, lab_rx, lab2)):
        stat[FIRST, ds(t0, TOK)] = jnp.where(ref[FIRST, :] >= 0, stat[FIRST, ds(t0, TOK)] - math.log(scale), HIGH)
        stat[SECOND, ds(t0, TOK)] = lab

    def grad(i, target):
        ids = (lax.broadcasted_iota(jnp.int32, (L, L), 0) + i * L).astype(F32)
        s = jnp.zeros((L, L), F32)
        for j in range(2 * TOK // L):
            x = out[sl(j * ROWS + i * L, L), :]
            hit = ids == stat[SECOND, lanes(j)]
            g = jnp.exp(x - stat[FIRST, lanes(j)]) - jnp.where(hit, scale, 0.0)
            gt[ds(pl.multiple_of(i * L, L), L), lanes(j)] = g.astype(BF)
            s = s + g
            target = target + jnp.where(hit, x, 0.0)
        small[ds(i, 1), :] = over_rows(jnp.sum, jnp.transpose(s))
        return target

    target = lax.fori_loop(0, ROWS // L, grad, jnp.zeros((L, L), F32))
    small[ds(LOSS_ROW + 1, 1), :] = over_rows(jnp.sum, target)

    def rows(k, start, n):
        return out.at[sl(k * ROWS + start, n)]

    halves = []
    for b, p, pn, q, qn in ((0, y, ynb, z, znb), (HALF, z, znb, y, ynb)):
        pc, qc = ([(t + d) % 4 * n for d in NEAR] for t, n in ((p, SH), (q, SUB)))
        halves.append((b, pn, qn, pc, qc, b + (p + FAR) % 4 * SH, b + p * SH, (q + FAR) % 4 * SUB, q * SUB))

    def stage_copies(st, k):
        cps = []
        for h, (b, pn, qn, pc, qc, po, b2, qo, q0) in enumerate(halves):
            for d in TWO:
                n = SCUTS[d]
                if st == 0:
                    a = rows(k, po + d * CUT, CUT), r1.at[k % EARLY, h, d], pn
                elif st == 1:
                    a = rows(k, b + pc[d], SH), r2.at[k % 2, h, d], pn
                elif st == 2:
                    a = rows(k, b2 + qo + d * SCUT, n), r3.at[k % 3, h, d, ds(0, n)], qn
                elif st == 3:
                    a = rows(k, b2 + qc[d], SUB), r4.at[k % 3, h, d], qn
                elif st == 4:
                    a = rows(k, b2 + q0, SUB), a1.at[k % 4, h, d], qn
                elif st == 5:
                    a = a1.at[k % 4, h, d, ds(d * SCUT, n)], a2.at[k % 3, h, d, ds(0, n)], qn
                elif st == 6:
                    a = rows(k, b2, SH), rows(k, b2, SH), pn
                else:
                    s = rows(k, b + pc[1 - d] + d * CUT, CUT)
                    a = s, s, pn
                src, dst, nb = a
                cps.append(remote(src, dst, ssem.at[st, h, d, k], rsem.at[st, h, d, k], {"dp": nb[d]}))
        return cps

    def mate_copies(k, far):
        cps = []
        for h, (b, pn, qn, pc, qc, po, b2, qo, q0) in enumerate(halves):
            for i, r in enumerate([b2] + [b + t for t in pc] + [po]):
                if far == (i == 3):
                    cps.append(remote(rows(k, r, SH), rows(k, OTH0 + r, SH), psend.at[k, h, i], precv.at[k, h, i], {"dp": mate}))
        return cps

    def mm(k, r):
        r = pl.multiple_of(r, BTILE)
        rows(k, r, SH)[...] = dot(gt[ds(r, SH), :], u_all[:, ds(pl.multiple_of(k * L, L), L)])

    def first_rows(k):
        for h in halves:
            mm(k, h[5])
        start_all(stage_copies(0, k))

    def other_rows(k):
        def shard(i, carry):
            mm(k, i // 3 * HALF + (jnp.where(i < 3, y, z) + (i % 3 + 3)) % 4 * SH)
            return carry
        lax.fori_loop(0, 6, shard, 0)

    def stage(st, k):
        if st == 0:
            first_rows(k)
            other_rows(k)
            return
        wait_all(stage_copies(st - 1, k))
        for h, (b, pn, qn, pc, qc, po, b2, qo, q0) in enumerate(halves):
            both = lambda r, m: [r.at[k % m, h, d] for d in TWO]
            if st == 2:
                add_rows(rows(k, b2, SH), both(r2, 2), SH, SLOT)
            elif st == 4:
                add_rows(rows(k, b2 + q0, SUB), both(r4, 3), SUB, SUB)
            for d in TWO:
                n = SCUTS[d]
                if st == 1:
                    add_rows(rows(k, b + pc[d] + d * CUT, CUT), [r1.at[k % EARLY, h, d]], CUT, SLOT)
                elif st == 3:
                    add_rows(rows(k, b2 + qc[d] + d * SCUT, n), [r3.at[k % 3, h, d]], n, n)
                elif st == 5:
                    rows(k, b2 + qc[1 - d], SUB)[...] = a1[k % 4, h, d]
                elif st == 6:
                    rows(k, b2 + qo + d * SCUT, n)[...] = a2[k % 3, h, d, ds(0, n)]
        if st < NSTAGE:
            start_all(stage_copies(st, k))
        if st + 1 >= NSTAGE:
            start_all(mate_copies(k, st == NSTAGE))

    xp, xm, xo = xnb

    def qrow(q, o, n):
        return sl(q * QROWS + o, n)

    def arow(q, o, n):
        return sl(q * XROWS + o, n)

    def same(ref, r):
        return ref.at[r], ref.at[r]

    def dwrow(j, o, n):
        return sl(DW0 + j * W + o, n)

    XTWO = ((xo, 0), (xo, QROWS // 2))
    c_du = [to_mate(part, drx, 2)]
    c_x1 = [to_x(drx.at[qrow(q, o, QROWS // 2)], xr1.at[d], 0, d) for d, (q, o) in enumerate(XTWO)]
    c_x2 = [to_x(drx.at[qrow(xnb[d], 0, QROWS)], part.at[ds(d * QROWS, QROWS)], 1, d) for d in TWO]
    c_x3 = [to_x(*same(dabx, arow(vp, 0, XROWS)), 2, d) for d in TWO]
    c_x4 = [to_x(*same(dabx, arow(q, o, n)), 3, d)
            for d, (q, o, n) in enumerate(((xm, 0, XCUT), (xp, XCUT, XROWS - XCUT)))]
    c_dw = [to_mate(part.at[qrow(1 - c, 0, QROWS)], dwrx.at[ds(0, QROWS)], 3),
            to_mate(part.at[ds(2 * QROWS, TILE)], dwrx.at[ds(QROWS, TILE)], 4)]
    c_w1 = [to_x(*same(out, dwrow(vp, 0, W)), 4, d) for d in TWO]
    c_w2 = [to_x(*same(out, dwrow(q, d * (W // 2), W // 2)), 5, d) for d, q in enumerate((xm, xp))]
    c_w3 = [to_mate(out.at[ds(DW0, 4 * W)], out.at[ds(DW0 + 4 * W, 4 * W)], 5),
            to_mate(out.at[ds(MG0 + W, TAIL)], out.at[ds(TAIL0, TAIL)], 6)]

    def du_part(col0, dst, again):
        def block(i, slot, e, carry):
            dst[...] += dot(gt[ds(pl.multiple_of(i * BLK, L), BLK), ds(col0, TOK)], e, 0, 0)
            return carry
        stream(block, 0, again)

    def du_theirs():
        part[...] = jnp.zeros((TOK, W), F32)
        du_part(oth0, part, True)
        start_all(c_du)

    def du_mine():
        wait_all(c_du)
        du_part(own0, drx, False)

        def rnd(i, carry):
            r = sl(i * SCUT, SCUT)
            drx[r, :] = drx[r, :].astype(BF).astype(F32)
            return carry

        lax.fori_loop(0, TOK // SCUT, rnd, 0)
        start_all(c_x1)

    def du_near():
        wait_all(c_x1)
        for d, o in ((0, 0), (1, QROWS // 2)):
            drx[qrow(xnb[d], o, QROWS // 2), :] += xr1[d]
        start_all(c_x2)

    def norm_back():
        wait_all(c_x2)

        def block(i, sums):
            r = sl(i * 2 * TILE, 2 * TILE)
            a = abuf[r, :]
            dun = drx[qrow(vp, i * 2 * TILE, 2 * TILE), :] + part[r, :] + part[sl(QROWS + i * 2 * TILE, 2 * TILE), :]
            cdf, rstd, xhat = gelu_norm(a)
            dx = dun * ln_gain[...]
            dg = rstd * (dx - row_mean(dx) - xhat * row_mean(dx * xhat))
            da = dg * (cdf + a * jnp.exp(-0.5 * a * a) * INV_SQRT_2PI)
            dabx[arow(vp, i * 2 * TILE, 2 * TILE), :] = da.astype(BF).astype(F32)
            return tuple(s + t[:TILE] + t[TILE:] for s, t in zip(sums, (da, dun * xhat, dun)))

        sums = lax.fori_loop(0, QROWS // (2 * TILE), block, (jnp.zeros((TILE, W), F32),) * 3)
        sums = [over_rows(jnp.sum, t) for t in sums]
        sums.append(jnp.concatenate([small[ds(LOSS_ROW + 1, 1), :], jnp.zeros((1, W - L), F32)], axis=1))
        dabx[arow(vp, QROWS, TILE), :] = jnp.concatenate(sums + [jnp.zeros((TILE - len(sums), W), F32)], axis=0)
        start_all(c_x3)

    def pass_on():
        wait_all(c_x3)
        start_all(c_x4)

    def dab(q):
        return dabx[arow(q, 0, QROWS), :].astype(BF)

    def weight_grad():
        wait_all(c_x4)
        part[ds(0, 2 * QROWS), :] = sum(dot(zbuf[qrow(q, 0, QROWS), :], dab(q), 0, 0) for q in range(4))
        part[ds(2 * QROWS, TILE), :] = sum(dabx[arow(q, QROWS, TILE), :] for q in range(4))
        start_all(c_dw)

    def input_grad():
        load_w_again.start()
        wait_all(c_dw)
        for j in range(W // L):
            m8[lanes(j), :] = part[qrow(c, 0, QROWS), lanes(j)] + dwrx[ds(0, QROWS), lanes(j)]
            v = part[ds(2 * QROWS, TILE), lanes(j)] + dwrx[ds(QROWS, TILE), lanes(j)]
            for i in THREE:
                m8[ds(VEC0 + i * TILE + j, 1), :] = v[i:i + 1]
            if j == 0:
                small[ds(LOSS_ROW + 1, 1), :] = v[3:4]
        m8[ds(SMALL0, N_SMALL), :] = small[...]
        m8[ds(SMALL0 + N_SMALL, MINI - SMALL0 - N_SMALL), :] = jnp.zeros((MINI - SMALL0 - N_SMALL, L), F32)
        start_all(mini_copies(0))

    mini = ((0, y, ynb, z, znb), (MINI // 2, z, znb, y, ynb))

    def mini_copies(st):
        cps = []
        for h, (b, p, pn, q, qn) in enumerate(mini):
            b2 = b + p * MSH
            direct = st in (2, 3)
            for d, off in enumerate(AROUND if direct else NEAR):
                half, near = d * MCUT, b + (p + off) % 4 * MSH
                if st == 0:
                    a = m8.at[sl(b + (p + FAR) % 4 * MSH + half, MCUT)], mr1.at[h, FAR, ds(half, MCUT)]
                elif st == 1:
                    a = m8.at[sl(near, MSH)], mr1.at[h, d]
                elif st == 2:
                    a = m8.at[sl(b2 + (q + off) % 4 * MSUB, MSUB)], mr2.at[h, d]
                elif st == 3:
                    a = same(out, sl(MG0 + b2 + q * MSUB, MSUB))
                elif st == 4:
                    a = same(out, sl(MG0 + b2, MSH))
                else:
                    a = same(out, sl(MG0 + b + (p + NEAR[1 - d]) % 4 * MSH + half, MCUT))
                cps.append(remote(*a, ms.at[st, h, d], mr.at[st, h, d], {"dp": (qn if direct else pn)[d]}))
        return cps

    def mini_step(st):
        wait_all(mini_copies(st - 1))
        for h, (b, p, pn, q, qn) in enumerate(mini):
            if st == 1:
                for d, off in enumerate(NEAR):
                    m8[sl(b + (p + off) % 4 * MSH + d * MCUT, MCUT), :] += mr1[h, FAR, ds(d * MCUT, MCUT), :]
            elif st == 2:
                m8[sl(b + p * MSH, MSH), :] += mr1[h, 0] + mr1[h, 1]
            elif st == 3:
                r = b + p * MSH + q * MSUB
                out[sl(MG0 + r, MSUB), :] = m8[sl(r, MSUB), :] + sum(mr2[h, d] for d in THREE)
        start_all(mini_copies(st))

    def hidden_grad():
        load_w_again.wait()
        for q in range(4):
            u_all[qrow(q, 0, QROWS), :] = dot(dab(q), gt[ds(0, W), :], 1, 1).astype(BF)
        store_dz.start()

    def weight_x():
        store_dz.wait()
        wait_all(mini_copies(5))
        out[dwrow(vp, 0, W), :] = out[ds(MG0, W), :]
        start_all(c_w1)

    def weight_on():
        wait_all(c_w1)
        start_all(c_w2)

    def weight_mate():
        wait_all(c_w2)
        start_all(c_w3)

    m = functools.partial
    at_end = (du_theirs, du_mine, du_near, norm_back, pass_on, input_grad, hidden_grad, m(mini_step, 3), m(mini_step, 5),
              weight_x, weight_on, weight_mate)
    ends = list(enumerate(at_end, FAR))
    middles = list(enumerate((weight_grad, m(mini_step, 1), m(mini_step, 2), m(mini_step, 4)), NCH - 1))

    def step(stages, wanted, t, carry):
        def run(pieces):
            for at, piece in pieces:
                if wanted(at):
                    pl.when(t == at)(piece)
        for st in stages:
            k = t - st
            pl.when((k >= (0 if st else EARLY)) & (k < NCH))(m(stage, st, k))
            if st == NSTAGE // 2:
                run(middles)
        run(ends)
        return carry

    filling = m(step, range(NSTAGE - 1, -1, -1), lambda at: at < NCH)
    emptying = m(step, range(1, NSTAGE + 1), lambda at: at >= NCH)
    for k in range(EARLY):
        first_rows(k)
    for k in range(EARLY):
        other_rows(k)
    lax.fori_loop(1, NCH, filling, 0)
    lax.fori_loop(NCH, NCH + NSTAGE, emptying, 0)

    def drain(k, carry):
        for far in (False, True):
            wait_all(mate_copies(k, far))
        return carry

    lax.fori_loop(0, NCH, drain, 0)
    wait_all(c_w3)
    save = [pltpu.make_async_copy(out.at[ds(r, TAIL)], aux.at[j], sem_w.at[j]) for j, r in enumerate((MG0 + W, TAIL0))]
    start_all(save)
    wait_all(save)


def head_call(scale, *args):
    vm, hbm = (pl.BlockSpec(memory_space=s) for s in (VMEM, pltpu.HBM))
    pair = (2, 2)
    sems = [(NSTAGE,) + pair + (NCH,)] * 2 + [(NCH, 2, 4)] * 2 + [(SEQS + 1,), pair[:1]] + [(7,)] * 4 + [(6, 2)] * 2 + [(6, 2, 3)] * 2
    return pl.pallas_call(
        functools.partial(head_kernel, scale),
        out_shape=(jax.ShapeDtypeStruct((TOK, W), BF), jax.ShapeDtypeStruct((2, TAIL, L), F32), VMEM((OUT_ROWS, L), F32)),
        in_specs=[vm] * 6 + [hbm] * 3,
        out_specs=(hbm, hbm, vm),
        scratch_shapes=[
            VMEM((ROWS, 2 * TOK), BF), VMEM((2 * TOK, W), BF),
            VMEM((EARLY,) + pair + (CUT, L), F32), VMEM((2,) + pair + (SH, L), F32), VMEM((3,) + pair + (SCUT, L), F32),
            VMEM((3,) + pair + (SUB, L), F32), VMEM((4,) + pair + (SUB, L), F32), VMEM((3,) + pair + (SCUT, L), F32),
            VMEM((TOK, W), F32), VMEM((TOK, W), F32), VMEM((2, QROWS // 2, W), F32),
            VMEM((4 * XROWS, W), F32), VMEM((XROWS, W), F32), VMEM((MINI, L), F32), VMEM((2, 3, MSH, L), F32),
            VMEM((2, 3, MSUB, L), F32), VMEM((2 * BLK, W), BF), VMEM((TOK, 2 * L), BF), VMEM((QROWS, W), F32),
            VMEM((TILE, L), jnp.int32), VMEM((TILE, TOK), F32), VMEM((N_SMALL, L), F32), VMEM((TILE, TOK), F32), VMEM((TILE, 2 * TOK), F32), VMEM((7, TILE, 2 * TOK), F32),
            VMEM((N_SMALL, L), F32),
        ] + [DMA(s) for s in sems],
        compiler_params=pltpu.CompilerParams(collective_id=0, has_side_effects=True, vmem_limit_bytes=30655000),
        name="mlm_head",
    )(*args)


def write_kernel(res, pos_in, dz_in, d_emb, d_w, d_hid, hid, pos, dz, sem, sem_w, sem_h, sem_i):
    c = lax.axis_index("dp") % 2
    cps = []
    for j, core in enumerate((c, 1 - c)):
        for k in range(NCH):
            cps.append(pltpu.make_async_copy(
                res.at[ds(j * OTH0 + k * ROWS, VROWS)], d_emb.at[sl(core * VROWS, VROWS), lanes(k)], sem.at[k, j]))
            for x in range(4):
                cps.append(pltpu.make_async_copy(
                    res.at[ds(DW0 + (j * 4 + x) * W + k * L, L)],
                    d_w.at[sl(x * 2 * L + core * L, L), lanes(k)], sem_w.at[k, j, x]))
    loads = [pltpu.make_async_copy(src, dst, sem_i.at[j]) for j, (src, dst) in enumerate(((pos_in, pos), (dz_in, dz)))]
    start_all(loads)
    start_all(cps)
    wait_all(loads)
    for b in range(SEQS):
        where = jnp.broadcast_to(jnp.concatenate([pos[b:b + 1, :], jnp.full((1, L - MASKS), -1, jnp.int32)], axis=1), (SEQ, L))
        hot = jnp.where(where == lax.broadcasted_iota(jnp.int32, (SEQ, L), 0), 1.0, 0.0).astype(BF)
        rows = jnp.concatenate([dz[b * SLOT:(b + 1) * SLOT, :], jnp.zeros((L - SLOT, W), BF)], axis=0)
        r = ds(b * SEQ, SEQ)
        hid[r, :] = dot(hot, rows).astype(BF)
        cp = pltpu.make_async_copy(hid.at[r], d_hid.at[r], sem_h.at[b])
        cp.start()
        cps.append(cp)
    wait_all(cps)


def write_call(res, pos, dz):
    vm, hbm = (pl.BlockSpec(memory_space=s) for s in (VMEM, pltpu.HBM))
    return pl.pallas_call(
        write_kernel,
        out_shape=tuple(jax.ShapeDtypeStruct(s, t) for s, t in (
            ((2 * VROWS, W), F32), ((W, W), F32), ((SEQS * SEQ, W), BF))),
        in_specs=[vm, hbm, hbm],
        out_specs=(hbm,) * 3,
        scratch_shapes=[VMEM((SEQS * SEQ, W), BF), VMEM((SEQS, MASKS), jnp.int32), VMEM((TOK, W), BF), DMA((NCH, 2)), DMA((NCH, 2, 4)),
                        DMA((SEQS,)), DMA((2,))],
        compiler_params=pltpu.CompilerParams(vmem_limit_bytes=16 << 20),
        name="write_rows",
    )(res, *(pltpu.with_memory_space_constraint(t, pltpu.HBM) for t in (pos, dz)))


def small_kernel(aux, b_trans, ln_gain, ln_bias, db, loss):
    c = lax.axis_index("dp") % 2
    for i, ref in enumerate((b_trans, ln_gain, ln_bias)):
        ref[...] = aux[0, ds(i * TILE, TILE), :]
    first, second = aux[ds(c, 1), ds(SMALL0 - VEC0, N_SMALL), :][0], aux[ds(1 - c, 1), ds(SMALL0 - VEC0, N_SMALL), :][0]
    rest = VROWS % L
    lane = lax.broadcasted_iota(jnp.int32, (LOSS_ROW, L), 1)
    second = pltpu.roll(second, rest, 1)
    db[ds(0, LOSS_ROW), :] = jnp.where((lane < rest) | (lax.broadcasted_iota(jnp.int32, (LOSS_ROW, L), 0) < LOSS_ROW - 1),
                                       first[:LOSS_ROW], second[:1])
    db[ds(LOSS_ROW, LOSS_ROW), :] = jnp.where(lane < rest, second[:LOSS_ROW], second[1:LOSS_ROW + 1])
    at = SMALL0 - VEC0 + LOSS_ROW
    total = aux[0, ds(at, 1), :] + aux[1, ds(at, 1), :] - aux[0, ds(at + 1, 1), :]
    loss[...] = jnp.sum(total, axis=1, keepdims=True)


def small_call(aux):
    vm = pl.BlockSpec(memory_space=VMEM)
    return pl.pallas_call(
        small_kernel,
        out_shape=tuple(jax.ShapeDtypeStruct(t, F32) for t in [(TILE, L)] * 3 + [(2 * LOSS_ROW, L), (1, 1)]),
        in_specs=[vm],
        out_specs=(vm,) * 5,
        name="small_results",
    )(aux)


def solution(mesh):
    n_groups = mesh.shape["dp"]

    def local_step(hidden, mask_pos, labels, w_trans, b_trans, ln_gain, ln_bias, emb_table, b_vocab):
        n_rows, seq_len, width = hidden.shape
        n_masks = mask_pos.shape[1]
        n_tokens = n_rows * n_masks * n_groups
        line = lambda v: v.reshape(1, v.shape[0])
        dz, aux, res = head_call(1.0 / n_tokens, mask_pos, labels, line(b_vocab), line(b_trans), line(ln_gain), line(ln_bias),
                                 hidden.reshape(n_rows * seq_len, width), emb_table, w_trans)
        d_emb, d_w_trans, d_hidden = write_call(res, mask_pos, dz)
        aux, d_w_trans = lax.optimization_barrier((aux, d_w_trans))
        *vecs, db, loss = small_call(aux)
        d_b_trans, d_gain, d_bias = (v.reshape(width) for v in vecs)
        d_b_vocab = db.reshape(2 * ROWS)[:2 * VROWS]
        return loss.reshape(()) / n_tokens, d_hidden.reshape(hidden.shape), d_w_trans, d_b_trans, d_gain, d_bias, d_emb, d_b_vocab

    in_specs = (P("dp", None, None), P("dp", None), P("dp", None), P(None, None), P(None), P(None), P(None), P("vp", None), P("vp"))
    out_specs = (P(), P("dp", None, None), P(None, None), P(None), P(None), P(None), P("vp", None), P("vp"))
    return jax.shard_map(local_step, mesh=mesh, in_specs=in_specs, out_specs=out_specs, check_vma=False)
```

```python
import functools
import math

import jax
import jax.numpy as jnp
from jax import lax
from jax.experimental import pallas as pl
from jax.experimental.pallas import tpu as pltpu
from jax.sharding import PartitionSpec as P

MESH = pl.DeviceIdType.MESH
F32, BF = jnp.float32, jnp.bfloat16
VMEM, DMA, ds = pltpu.VMEM, pltpu.SemaphoreType.DMA, pl.ds
LN_EPS = 1e-5
HALF_SQRT, INV_SQRT_2PI = 0.7071067811865476, 0.3989422804014327
LOW, HIGH, NO_LABEL = -3e38, 3e38, -1e6
W, L, TILE, BTILE = 1024, 128, 8, 16
SEQS, SEQ, MASKS, SLOT = 6, 512, 77, 80
USED, TOK = SEQS * SLOT, 512
VROWS, ROWS, BLK = 3824, 3840, 384
N_BLK = ROWS // BLK
LAST = VROWS - (N_BLK - 1) * BLK
NCH = W // L
HALF, SH, SUB = ROWS // 2, ROWS // 8, ROWS // 32
CUT, SCUT = SH // 2, 64
SCUTS = (SCUT, SUB - SCUT)
QROWS, XROWS, XCUT = 128, 136, 72
VEC0, SMALL0, MINI = W, W + 24, 1280
MSH, MSUB = MINI // 8, MINI // 32
MCUT = MSH // 2
LOSS_ROW, N_SMALL = ROWS // L, 32
OTH0 = NCH * ROWS
DW0 = 2 * OTH0
MG0 = DW0 + 8 * W
TAIL0 = MG0 + MINI
TAIL = 64
OUT_ROWS = TAIL0 + TAIL
NSTAGE, EARLY = 8, 3
NEAR, FAR = (1, 3), 2
AROUND = NEAR + (FAR,)
TWO, THREE, FOUR = (0, 1), (0, 1, 2), range(4)
QW = TOK // 2
FIRST, SECOND = slice(0, 1), slice(1, 2)


def sl(start, n):
    return ds(pl.multiple_of(start, TILE), n)


def wait_all(cps):
    for cp in cps:
        cp.wait()


def start_all(cps):
    for cp in cps:
        cp.start()


def gelu_norm(a):
    cdf = 0.5 * (1.0 + lax.erf(a * HALF_SQRT))
    g = a * cdf
    cen = g - row_mean(g)
    rstd = lax.rsqrt(row_mean(cen * cen) + LN_EPS)
    return cdf, rstd, cen * rstd


def row_mean(t):
    return jnp.mean(t, axis=-1, keepdims=True)


def over_rows(fn, t):
    return fn(t, axis=0, keepdims=True)


def dot(a, b, ca=1, cb=0):
    return lax.dot_general(a, b, (((ca,), (cb,)), ((), ())), preferred_element_type=F32)


def lanes(j):
    return ds(j * L, L)


def add_rows(dst, srcs, n, blk):
    def body(i, carry):
        r = sl(i * blk, blk)
        v = dst[r, :]
        for s in srcs:
            v = v + s[r, :]
        dst[r, :] = v
        return carry
    lax.fori_loop(0, n // blk, body, 0)


def head_kernel(scale, pos_in, lab_in, b_in, b_trans, ln_gain, ln_bias, hidden, emb, w_in, dz, aux, out,
                gt, u_all, r1, r2, r3, r4, a1, a2, part, drx, xr1, dabx, dwrx, m8, mr1, mr2,
                wbuf, zbuf, abuf, pos, lab_own, bias, lab_rx, stat, msg, stats, small,
                ssem, rsem, psend, precv, sem_h, sem_w, es, er, st_s, st_r, xs, xr, ms, mr):
    dp, vp = lax.axis_index("dp"), lax.axis_index("vp")
    z, y, c = dp // 8, (dp // 2) % 4, dp % 2
    ynb = [z * 8 + ((y + d) % 4) * 2 + c for d in AROUND]
    znb = [((z + d) % 4) * 8 + y * 2 + c for d in AROUND]
    xnb = [(vp + d) % 4 for d in AROUND]
    mate = dp + 1 - 2 * c
    peers = [{"vp": v, "dp": d} for v in xnb for d in (dp, mate)] + [{"vp": vp, "dp": mate}]

    def load_hidden(b):
        r = sl(b * SEQ, SEQ)
        return pltpu.make_async_copy(hidden.at[r], gt.at[r], sem_h.at[b])

    def load_emb(i, slot, n):
        return pltpu.make_async_copy(emb.at[ds(pl.multiple_of(c * VROWS, BTILE) + i * BLK, n)],
                                     wbuf.at[ds(pl.multiple_of(slot * BLK, BTILE), n)], sem_w.at[slot])

    load_w = pltpu.make_async_copy(w_in, u_all, sem_h.at[SEQS])
    store_dz = pltpu.make_async_copy(u_all.at[ds(0, TOK)], dz, sem_h.at[0])
    load_w_again = pltpu.make_async_copy(w_in, gt.at[ds(0, W)], sem_h.at[SEQS])
    for b in range(SEQS):
        load_hidden(b).start()
    load_w.start()
    load_emb(0, 0, BLK).start()

    barrier = pltpu.get_barrier_semaphore()
    greet = peers + [{"dp": d} for d in ynb + znb]
    for d in greet:
        pl.semaphore_signal(barrier, inc=1, device_id=d, device_id_type=MESH)

    def remote(src, dst, send, recv, dev):
        return pltpu.make_async_remote_copy(src_ref=src, dst_ref=dst, send_sem=send, recv_sem=recv,
                                            device_id=dev, device_id_type=MESH)

    def to_mate(src, dst, i):
        return remote(src, dst, es.at[i], er.at[i], {"dp": mate})

    def to_x(src, dst, i, d):
        return remote(src, dst, xs.at[i, d], xr.at[i, d], {"vp": xnb[d]})

    c_u = [to_mate(part, drx, 0), to_mate(lab_own, lab_rx, 1)]
    own0 = pl.multiple_of(c * TOK, TOK)
    oth0 = pl.multiple_of((1 - c) * TOK, TOK)

    pos[...] = jnp.full((TILE, L), -1, jnp.int32)
    pos[ds(0, SEQS), ds(0, MASKS)] = pos_in[...]
    lane = lax.broadcasted_iota(jnp.int32, (L, TOK), 1)
    seq = sum((lane >= b * SLOT).astype(jnp.int32) for b in range(1, SEQS))
    slot = lane - seq * SLOT
    place = jnp.where(slot == lax.broadcasted_iota(jnp.int32, (L, TOK), 0), 1.0, 0.0).astype(BF)[:MASKS]
    high, low = lab_in[...] >> 8, lab_in[...] & 255
    spread = dot(high.astype(F32).astype(BF), place) * 256.0 + dot(low.astype(F32).astype(BF), place)
    row = lax.broadcasted_iota(jnp.int32, (SEQS, TOK), 0)
    lab = over_rows(jnp.sum, jnp.where(row == seq[:SEQS], spread, 0.0))
    lab = jnp.where(slot[:1] < MASKS, lab, NO_LABEL)
    lab_own[...] = jnp.broadcast_to(lab, (TILE, TOK))
    rest = VROWS % L
    for core in TWO:
        @pl.when(c == core)
        def _():
            for i in range(VROWS // L):
                bias[ds(i, 1), :] = b_in[:, core * VROWS + i * L:core * VROWS + (i + 1) * L]
            bias[ds(LOSS_ROW - 1, 1), :] = jnp.full((1, L), LOW, F32)
            bias[ds(LOSS_ROW - 1, 1), ds(0, rest)] = b_in[:, (core + 1) * VROWS - rest:(core + 1) * VROWS]

    z0 = SEQS * SEQ

    def gather(b, carry):
        load_hidden(b).wait()
        where = jnp.broadcast_to(pos[ds(b, 1), :], (SEQ, L))
        hot = jnp.where(where == lax.broadcasted_iota(jnp.int32, (SEQ, L), 0), 1.0, 0.0).astype(BF)
        gt[ds(pl.multiple_of(z0 + b * SLOT, BTILE), SLOT), :] = dot(hot, gt[sl(b * SEQ, SEQ), :], 0, 0)[:SLOT].astype(BF)
        return carry

    gt[ds(z0 + USED, TOK - USED), :] = jnp.zeros((TOK - USED, W), BF)
    lax.fori_loop(0, SEQS, gather, 0)
    load_w.wait()
    zbuf[...] = gt[ds(z0, TOK), ds(pl.multiple_of(vp * 2 * L, L), 2 * L)]

    def transform(i, carry):
        r = sl(i * 2 * L, 2 * L)
        dabx[r, :] = dot(gt[ds(pl.multiple_of(z0 + i * 2 * L, L), 2 * L), :], u_all[...]) + b_trans[...]
        return carry

    lax.fori_loop(0, TOK // (2 * L), transform, 0)

    def norm(i, carry):
        r = sl(i * 4 * TILE, 4 * TILE)
        _, _, xhat = gelu_norm(dabx[r, :])
        part[r, :] = (xhat * ln_gain[...] + ln_bias[...]).astype(BF).astype(F32)
        return carry

    lax.fori_loop(0, USED // (4 * TILE), norm, 0)
    part[ds(USED, TOK - USED), :] = jnp.zeros((TOK - USED, W), F32)
    abuf[...] = dabx[sl(vp * QROWS, QROWS), :]
    u_all[ds(own0, TOK), :] = part[...].astype(BF)
    pl.semaphore_wait(barrier, len(greet))
    start_all(c_u)

    def stream(body, init, again):
        def pair(m, carry):
            last = m + 1 == N_BLK // 2
            i = 2 * m
            for at, n in ((~last, BLK), (last, LAST)):
                pl.when(at)(load_emb(i + 1, 1, n).start)
            load_emb(i, 0, BLK).wait()
            carry = body(i, 0, wbuf[ds(0, BLK), :], carry)
            pl.when(~last)(load_emb(i + 2, 0, BLK).start)
            if again:
                pl.when(last)(load_emb(0, 0, BLK).start)
            for at, n in ((~last, BLK), (last, LAST)):
                pl.when(at)(load_emb(i + 1, 1, n).wait)
            return body(i + 1, 1, wbuf[ds(BLK, BLK), :], carry)
        return lax.fori_loop(0, N_BLK // 2, pair, init)

    row0 = (vp * 2 * VROWS + c * VROWS).astype(F32)

    def local_labels(ref):
        v = ref[FIRST, :] - row0
        return jnp.where((v >= 0) & (v < VROWS), v, -1.0)

    def logits(tok0, again):
        u = u_all[ds(tok0, TOK), :]

        def sums(slot, top):
            return jnp.concatenate(
                [jnp.sum(jnp.exp(r2[slot, j // 2, j % 2, ds(0, BLK), :].reshape(BLK // TILE, TILE, L)
                                 - top[:, j * L:(j + 1) * L][None]), axis=0) for j in range(TOK // L)], axis=1)

        def block(i, slot, e, carry):
            old, mx, sm = carry
            sm = sm * jnp.exp(old - mx) + sums(1 - slot, mx)
            x = dot(e, u, 1, 1)
            col = [jnp.transpose(jnp.broadcast_to(bias[ds(i * (BLK // L) + j, 1), :], (L, L))) for j in range(BLK // L)]
            col = jnp.concatenate(col, axis=0)
            top = []
            for j in range(TOK // L):
                v = x[:, j * L:(j + 1) * L] + col
                out[sl((tok0 // L + j) * ROWS + i * BLK, BLK), :] = v
                r2[slot, j // 2, j % 2, ds(0, BLK), :] = v
                top.append(jnp.max(v.reshape(BLK // TILE, TILE, L), axis=0))
            return mx, jnp.maximum(mx, jnp.concatenate(top, axis=1)), sm

        low = jnp.full((TILE, TOK), LOW, F32)
        for j in range(TOK // L):
            r2[1, j // 2, j % 2, ds(0, BLK), :] = jnp.full((BLK, L), LOW, F32)
        old, mx, sm = stream(block, (low, low, jnp.zeros((TILE, TOK), F32)), again)
        sm = sm * jnp.exp(old - mx) + sums(1, mx)
        top = over_rows(jnp.max, mx)
        sm = over_rows(jnp.sum, sm * jnp.exp(mx - top))
        stat[:, ds(tok0, TOK)] = jnp.concatenate([top, sm, jnp.zeros((TILE - 2, TOK), F32)], axis=0)

    lab1 = local_labels(lab_own)
    logits(own0, True)
    wait_all(c_u)
    u_all[ds(oth0, TOK), :] = drx[...].astype(BF)
    lab2 = local_labels(lab_rx)
    logits(oth0, True)
    msg[...] = jnp.concatenate([stat[ds(i, 1), ds(j * QW, QW)] for i in TWO for j in FOUR], axis=0)
    c_st = [remote(msg, stats.at[j], st_s.at[j], st_r.at[j], d) for j, d in enumerate(peers)]
    start_all(c_st)
    wait_all(c_st)
    for j in FOUR:
        mx, sm = (jnp.concatenate([ref[ds(r, 1), :] for ref in (msg, *(stats.at[p] for p in range(len(peers))))], axis=0)
                  for r in (j, j + len(FOUR)))
        top = over_rows(jnp.max, mx)
        stat[FIRST, ds(j * QW, QW)] = top + jnp.log(over_rows(jnp.sum, sm * jnp.exp(mx - top)))
    own_norm = jnp.where(lab_own[FIRST, :] >= 0, stat[FIRST, ds(own0, TOK)], 0.0)
    small[ds(LOSS_ROW, 1), :] = sum(own_norm[:, j * L:(j + 1) * L] for j in range(TOK // L))
    for t0, ref, lab in ((own0, lab_own, lab1), (oth0, lab_rx, lab2)):
        stat[FIRST, ds(t0, TOK)] = jnp.where(ref[FIRST, :] >= 0, stat[FIRST, ds(t0, TOK)] - math.log(scale), HIGH)
        stat[SECOND, ds(t0, TOK)] = lab

    def grad(i, target):
        ids = (lax.broadcasted_iota(jnp.int32, (L, L), 0) + i * L).astype(F32)
        s = jnp.zeros((L, L), F32)
        for j in range(2 * TOK // L):
            x = out[sl(j * ROWS + i * L, L), :]
            hit = ids == stat[SECOND, lanes(j)]
            g = jnp.exp(x - stat[FIRST, lanes(j)]) - jnp.where(hit, scale, 0.0)
            gt[ds(pl.multiple_of(i * L, L), L), lanes(j)] = g.astype(BF)
            s = s + g
            target = target + jnp.where(hit, x, 0.0)
        small[ds(i, 1), :] = over_rows(jnp.sum, jnp.transpose(s))
        return target

    target = lax.fori_loop(0, ROWS // L, grad, jnp.zeros((L, L), F32))
    small[ds(LOSS_ROW + 1, 1), :] = over_rows(jnp.sum, target)

    def rows(k, start, n):
        return out.at[sl(k * ROWS + start, n)]

    halves = []
    for b, p, pn, q, qn in ((0, y, ynb, z, znb), (HALF, z, znb, y, ynb)):
        pc, qc = ([(t + d) % 4 * n for d in NEAR] for t, n in ((p, SH), (q, SUB)))
        halves.append((b, pn, qn, pc, qc, b + (p + FAR) % 4 * SH, b + p * SH, (q + FAR) % 4 * SUB, q * SUB))

    def stage_copies(st, k):
        cps = []
        for h, (b, pn, qn, pc, qc, po, b2, qo, q0) in enumerate(halves):
            for d in TWO:
                n = SCUTS[d]
                if st == 0:
                    a = rows(k, po + d * CUT, CUT), r1.at[k % EARLY, h, d], pn
                elif st == 1:
                    a = rows(k, b + pc[d], SH), r2.at[k % 2, h, d], pn
                elif st == 2:
                    a = rows(k, b2 + qo + d * SCUT, n), r3.at[k % 3, h, d, ds(0, n)], qn
                elif st == 3:
                    a = rows(k, b2 + qc[d], SUB), r4.at[k % 3, h, d], qn
                elif st == 4:
                    a = rows(k, b2 + q0, SUB), a1.at[k % 4, h, d], qn
                elif st == 5:
                    a = a1.at[k % 4, h, d, ds(d * SCUT, n)], a2.at[k % 3, h, d, ds(0, n)], qn
                elif st == 6:
                    a = rows(k, b2, SH), rows(k, b2, SH), pn
                else:
                    s = rows(k, b + pc[1 - d] + d * CUT, CUT)
                    a = s, s, pn
                src, dst, nb = a
                cps.append(remote(src, dst, ssem.at[st, h, d, k], rsem.at[st, h, d, k], {"dp": nb[d]}))
        return cps

    def mate_copies(k, far):
        cps = []
        for h, (b, pn, qn, pc, qc, po, b2, qo, q0) in enumerate(halves):
            for i, r in enumerate([b2] + [b + t for t in pc] + [po]):
                if far == (i == 3):
                    cps.append(remote(rows(k, r, SH), rows(k, OTH0 + r, SH), psend.at[k, h, i], precv.at[k, h, i], {"dp": mate}))
        return cps

    def mm(k, r):
        r = pl.multiple_of(r, BTILE)
        rows(k, r, SH)[...] = dot(gt[ds(r, SH), :], u_all[:, ds(pl.multiple_of(k * L, L), L)])

    def first_rows(k):
        for h in halves:
            mm(k, h[5])
        start_all(stage_copies(0, k))

    def other_rows(k):
        def shard(i, carry):
            mm(k, i // 3 * HALF + (jnp.where(i < 3, y, z) + (i % 3 + 3)) % 4 * SH)
            return carry
        lax.fori_loop(0, 6, shard, 0)

    def stage(st, k):
        if st == 0:
            first_rows(k)
            other_rows(k)
            return
        wait_all(stage_copies(st - 1, k))
        for h, (b, pn, qn, pc, qc, po, b2, qo, q0) in enumerate(halves):
            both = lambda r, m: [r.at[k % m, h, d] for d in TWO]
            if st == 2:
                add_rows(rows(k, b2, SH), both(r2, 2), SH, SLOT)
            elif st == 4:
                add_rows(rows(k, b2 + q0, SUB), both(r4, 3), SUB, SUB)
            for d in TWO:
                n = SCUTS[d]
                if st == 1:
                    add_rows(rows(k, b + pc[d] + d * CUT, CUT), [r1.at[k % EARLY, h, d]], CUT, SLOT)
                elif st == 3:
                    add_rows(rows(k, b2 + qc[d] + d * SCUT, n), [r3.at[k % 3, h, d]], n, n)
                elif st == 5:
                    rows(k, b2 + qc[1 - d], SUB)[...] = a1[k % 4, h, d]
                elif st == 6:
                    rows(k, b2 + qo + d * SCUT, n)[...] = a2[k % 3, h, d, ds(0, n)]
        if st < NSTAGE:
            start_all(stage_copies(st, k))
        if st + 1 >= NSTAGE:
            start_all(mate_copies(k, st == NSTAGE))

    xp, xm, xo = xnb

    def qrow(q, o, n):
        return sl(q * QROWS + o, n)

    def arow(q, o, n):
        return sl(q * XROWS + o, n)

    def same(ref, r):
        return ref.at[r], ref.at[r]

    def dwrow(j, o, n):
        return sl(DW0 + j * W + o, n)

    XTWO = ((xo, 0), (xo, QROWS // 2))
    c_du = [to_mate(part, drx, 2)]
    c_x1 = [to_x(drx.at[qrow(q, o, QROWS // 2)], xr1.at[d], 0, d) for d, (q, o) in enumerate(XTWO)]
    c_x2 = [to_x(drx.at[qrow(xnb[d], 0, QROWS)], part.at[ds(d * QROWS, QROWS)], 1, d) for d in TWO]
    c_x3 = [to_x(*same(dabx, arow(vp, 0, XROWS)), 2, d) for d in TWO]
    c_x4 = [to_x(*same(dabx, arow(q, o, n)), 3, d)
            for d, (q, o, n) in enumerate(((xm, 0, XCUT), (xp, XCUT, XROWS - XCUT)))]
    c_dw = [to_mate(part.at[qrow(1 - c, 0, QROWS)], dwrx.at[ds(0, QROWS)], 3),
            to_mate(part.at[ds(2 * QROWS, TILE)], dwrx.at[ds(QROWS, TILE)], 4)]
    c_w1 = [to_x(*same(out, dwrow(vp, 0, W)), 4, d) for d in TWO]
    c_w2 = [to_x(*same(out, dwrow(q, d * (W // 2), W // 2)), 5, d) for d, q in enumerate((xm, xp))]
    c_w3 = [to_mate(out.at[ds(DW0, 4 * W)], out.at[ds(DW0 + 4 * W, 4 * W)], 5),
            to_mate(out.at[ds(MG0 + W, TAIL)], out.at[ds(TAIL0, TAIL)], 6)]

    def du_part(col0, dst, again):
        def block(i, slot, e, carry):
            dst[...] += dot(gt[ds(pl.multiple_of(i * BLK, L), BLK), ds(col0, TOK)], e, 0, 0)
            return carry
        stream(block, 0, again)

    def du_theirs():
        part[...] = jnp.zeros((TOK, W), F32)
        du_part(oth0, part, True)
        start_all(c_du)

    def du_mine():
        wait_all(c_du)
        du_part(own0, drx, False)

        def rnd(i, carry):
            r = sl(i * SCUT, SCUT)
            drx[r, :] = drx[r, :].astype(BF).astype(F32)
            return carry

        lax.fori_loop(0, TOK // SCUT, rnd, 0)
        start_all(c_x1)

    def du_near():
        wait_all(c_x1)
        for d, o in ((0, 0), (1, QROWS // 2)):
            drx[qrow(xnb[d], o, QROWS // 2), :] += xr1[d]
        start_all(c_x2)

    def norm_back():
        wait_all(c_x2)

        def block(i, sums):
            r = sl(i * 2 * TILE, 2 * TILE)
            a = abuf[r, :]
            dun = drx[qrow(vp, i * 2 * TILE, 2 * TILE), :] + part[r, :] + part[sl(QROWS + i * 2 * TILE, 2 * TILE), :]
            cdf, rstd, xhat = gelu_norm(a)
            dx = dun * ln_gain[...]
            dg = rstd * (dx - row_mean(dx) - xhat * row_mean(dx * xhat))
            da = dg * (cdf + a * jnp.exp(-0.5 * a * a) * INV_SQRT_2PI)
            dabx[arow(vp, i * 2 * TILE, 2 * TILE), :] = da.astype(BF).astype(F32)
            return tuple(s + t[:TILE] + t[TILE:] for s, t in zip(sums, (da, dun * xhat, dun)))

        sums = lax.fori_loop(0, QROWS // (2 * TILE), block, (jnp.zeros((TILE, W), F32),) * 3)
        sums = [over_rows(jnp.sum, t) for t in sums]
        sums.append(jnp.concatenate([small[ds(LOSS_ROW + 1, 1), :], jnp.zeros((1, W - L), F32)], axis=1))
        dabx[arow(vp, QROWS, TILE), :] = jnp.concatenate(sums + [jnp.zeros((TILE - len(sums), W), F32)], axis=0)
        start_all(c_x3)

    def pass_on():
        wait_all(c_x3)
        start_all(c_x4)

    def dab(q):
        return dabx[arow(q, 0, QROWS), :].astype(BF)

    def weight_grad():
        wait_all(c_x4)
        part[ds(0, 2 * QROWS), :] = sum(dot(zbuf[qrow(q, 0, QROWS), :], dab(q), 0, 0) for q in FOUR)
        part[ds(2 * QROWS, TILE), :] = sum(dabx[arow(q, QROWS, TILE), :] for q in FOUR)
        start_all(c_dw)

    def input_grad():
        load_w_again.start()
        wait_all(c_dw)
        for j in range(W // L):
            m8[lanes(j), :] = part[qrow(c, 0, QROWS), lanes(j)] + dwrx[ds(0, QROWS), lanes(j)]
            v = part[ds(2 * QROWS, TILE), lanes(j)] + dwrx[ds(QROWS, TILE), lanes(j)]
            for i in THREE:
                m8[ds(VEC0 + i * TILE + j, 1), :] = v[i:i + 1]
            if j == 0:
                small[ds(LOSS_ROW + 1, 1), :] = v[3:4]
        m8[ds(SMALL0, N_SMALL), :] = small[...]
        m8[ds(SMALL0 + N_SMALL, MINI - SMALL0 - N_SMALL), :] = jnp.zeros((MINI - SMALL0 - N_SMALL, L), F32)
        start_all(mini_copies(0))

    mini = ((0, y, ynb, z, znb), (MINI // 2, z, znb, y, ynb))

    def mini_copies(st):
        cps = []
        for h, (b, p, pn, q, qn) in enumerate(mini):
            b2 = b + p * MSH
            direct = st in (2, 3)
            for d, off in enumerate(AROUND if direct else NEAR):
                half, near = d * MCUT, b + (p + off) % 4 * MSH
                if st == 0:
                    a = m8.at[sl(b + (p + FAR) % 4 * MSH + half, MCUT)], mr1.at[h, FAR, ds(half, MCUT)]
                elif st == 1:
                    a = m8.at[sl(near, MSH)], mr1.at[h, d]
                elif st == 2:
                    a = m8.at[sl(b2 + (q + off) % 4 * MSUB, MSUB)], mr2.at[h, d]
                elif st == 3:
                    a = same(out, sl(MG0 + b2 + q * MSUB, MSUB))
                elif st == 4:
                    a = same(out, sl(MG0 + b2, MSH))
                else:
                    a = same(out, sl(MG0 + b + (p + NEAR[1 - d]) % 4 * MSH + half, MCUT))
                cps.append(remote(*a, ms.at[st, h, d], mr.at[st, h, d], {"dp": (qn if direct else pn)[d]}))
        return cps

    def mini_step(st):
        wait_all(mini_copies(st - 1))
        for h, (b, p, pn, q, qn) in enumerate(mini):
            if st == 1:
                for d, off in enumerate(NEAR):
                    m8[sl(b + (p + off) % 4 * MSH + d * MCUT, MCUT), :] += mr1[h, FAR, ds(d * MCUT, MCUT), :]
            elif st == 2:
                m8[sl(b + p * MSH, MSH), :] += mr1[h, 0] + mr1[h, 1]
            elif st == 3:
                r = b + p * MSH + q * MSUB
                out[sl(MG0 + r, MSUB), :] = m8[sl(r, MSUB), :] + sum(mr2[h, d] for d in THREE)
        start_all(mini_copies(st))

    def hidden_grad():
        load_w_again.wait()
        for q in FOUR:
            u_all[qrow(q, 0, QROWS), :] = dot(dab(q), gt[ds(0, W), :], 1, 1).astype(BF)
        store_dz.start()

    def weight_x():
        store_dz.wait()
        wait_all(mini_copies(5))
        out[dwrow(vp, 0, W), :] = out[ds(MG0, W), :]
        start_all(c_w1)

    def weight_on():
        wait_all(c_w1)
        start_all(c_w2)

    def weight_mate():
        wait_all(c_w2)
        start_all(c_w3)

    m = functools.partial
    at_end = (du_theirs, du_mine, du_near, norm_back, pass_on, input_grad, hidden_grad, m(mini_step, 3), m(mini_step, 5),
              weight_x, weight_on, weight_mate)
    ends = list(enumerate(at_end, FAR))
    middles = list(enumerate((weight_grad, m(mini_step, 1), m(mini_step, 2), m(mini_step, 4)), NCH - 1))

    def step(stages, wanted, t, carry):
        def run(pieces):
            for at, piece in pieces:
                if wanted(at):
                    pl.when(t == at)(piece)
        for st in stages:
            k = t - st
            pl.when((k >= (0 if st else EARLY)) & (k < NCH))(m(stage, st, k))
            if st == NSTAGE // 2:
                run(middles)
        run(ends)
        return carry

    filling = m(step, range(NSTAGE - 1, -1, -1), lambda at: at < NCH)
    emptying = m(step, range(1, NSTAGE + 1), lambda at: at >= NCH)
    for k in range(EARLY):
        first_rows(k)
    for k in range(EARLY):
        other_rows(k)
    lax.fori_loop(1, NCH, filling, 0)
    lax.fori_loop(NCH, NCH + NSTAGE, emptying, 0)

    def drain(k, carry):
        for far in (False, True):
            wait_all(mate_copies(k, far))
        return carry

    lax.fori_loop(0, NCH, drain, 0)
    wait_all(c_w3)
    save = [pltpu.make_async_copy(out.at[ds(r, TAIL)], aux.at[j], sem_w.at[j]) for j, r in enumerate((MG0 + W, TAIL0))]
    start_all(save)
    wait_all(save)


def head_call(scale, *args):
    vm, hbm = (pl.BlockSpec(memory_space=s) for s in (VMEM, pltpu.HBM))
    pair = (2, 2)
    sems = [(NSTAGE,) + pair + (NCH,)] * 2 + [(NCH, 2, 4)] * 2 + [(SEQS + 1,), pair[:1]] + [(7,)] * 4 + [(6, 2)] * 2 + [(6, 2, 3)] * 2
    return pl.pallas_call(
        functools.partial(head_kernel, scale),
        out_shape=(jax.ShapeDtypeStruct((TOK, W), BF), jax.ShapeDtypeStruct((2, TAIL, L), F32), VMEM((OUT_ROWS, L), F32)),
        in_specs=[vm] * 6 + [hbm] * 3,
        out_specs=(hbm, hbm, vm),
        scratch_shapes=[
            VMEM((ROWS, 2 * TOK), BF), VMEM((2 * TOK, W), BF),
            VMEM((EARLY,) + pair + (CUT, L), F32), VMEM((2,) + pair + (SH, L), F32), VMEM((3,) + pair + (SCUT, L), F32),
            VMEM((3,) + pair + (SUB, L), F32), VMEM((4,) + pair + (SUB, L), F32), VMEM((3,) + pair + (SCUT, L), F32),
            VMEM((TOK, W), F32), VMEM((TOK, W), F32), VMEM((2, QROWS // 2, W), F32),
            VMEM((4 * XROWS, W), F32), VMEM((XROWS, W), F32), VMEM((MINI, L), F32), VMEM((2, 3, MSH, L), F32),
            VMEM((2, 3, MSUB, L), F32), VMEM((2 * BLK, W), BF), VMEM((TOK, 2 * L), BF), VMEM((QROWS, W), F32),
            VMEM((TILE, L), jnp.int32), VMEM((TILE, TOK), F32), VMEM((N_SMALL, L), F32), VMEM((TILE, TOK), F32), VMEM((TILE, 2 * TOK), F32), VMEM((TILE, QW), F32), VMEM((7, TILE, QW), F32),
            VMEM((N_SMALL, L), F32),
        ] + [DMA(s) for s in sems],
        compiler_params=pltpu.CompilerParams(collective_id=0, has_side_effects=True, vmem_limit_bytes=30655000),
        name="mlm_head",
    )(*args)


def write_kernel(res, pos_in, dz_in, d_emb, d_w, d_hid, hid, pos, dz, sem, sem_w, sem_h, sem_i):
    c = lax.axis_index("dp") % 2
    cps = []
    for j, core in enumerate((c, 1 - c)):
        for k in range(NCH):
            cps.append(pltpu.make_async_copy(
                res.at[ds(j * OTH0 + k * ROWS, VROWS)], d_emb.at[sl(core * VROWS, VROWS), lanes(k)], sem.at[k, j]))
            for x in FOUR:
                cps.append(pltpu.make_async_copy(
                    res.at[ds(DW0 + (j * 4 + x) * W + k * L, L)],
                    d_w.at[sl(x * 2 * L + core * L, L), lanes(k)], sem_w.at[k, j, x]))
    loads = [pltpu.make_async_copy(src, dst, sem_i.at[j]) for j, (src, dst) in enumerate(((pos_in, pos), (dz_in, dz)))]
    start_all(loads)
    start_all(cps)
    wait_all(loads)
    for b in range(SEQS):
        where = jnp.broadcast_to(jnp.concatenate([pos[b:b + 1, :], jnp.full((1, L - MASKS), -1, jnp.int32)], axis=1), (SEQ, L))
        hot = jnp.where(where == lax.broadcasted_iota(jnp.int32, (SEQ, L), 0), 1.0, 0.0).astype(BF)
        rows = jnp.concatenate([dz[b * SLOT:(b + 1) * SLOT, :], jnp.zeros((L - SLOT, W), BF)], axis=0)
        r = ds(b * SEQ, SEQ)
        hid[r, :] = dot(hot, rows).astype(BF)
        cp = pltpu.make_async_copy(hid.at[r], d_hid.at[r], sem_h.at[b])
        cp.start()
        cps.append(cp)
    wait_all(cps)


def write_call(res, pos, dz):
    vm, hbm = (pl.BlockSpec(memory_space=s) for s in (VMEM, pltpu.HBM))
    return pl.pallas_call(
        write_kernel,
        out_shape=tuple(jax.ShapeDtypeStruct(s, t) for s, t in (
            ((2 * VROWS, W), F32), ((W, W), F32), ((SEQS * SEQ, W), BF))),
        in_specs=[vm, hbm, hbm],
        out_specs=(hbm,) * 3,
        scratch_shapes=[VMEM((SEQS * SEQ, W), BF), VMEM((SEQS, MASKS), jnp.int32), VMEM((TOK, W), BF), DMA((NCH, 2)), DMA((NCH, 2, 4)),
                        DMA((SEQS,)), DMA((2,))],
        compiler_params=pltpu.CompilerParams(vmem_limit_bytes=16 << 20),
        name="write_rows",
    )(res, *(pltpu.with_memory_space_constraint(t, pltpu.HBM) for t in (pos, dz)))


def small_kernel(aux, b_trans, ln_gain, ln_bias, db, loss):
    c = lax.axis_index("dp") % 2
    for i, ref in enumerate((b_trans, ln_gain, ln_bias)):
        ref[...] = aux[0, ds(i * TILE, TILE), :]
    first, second = aux[ds(c, 1), ds(SMALL0 - VEC0, N_SMALL), :][0], aux[ds(1 - c, 1), ds(SMALL0 - VEC0, N_SMALL), :][0]
    rest = VROWS % L
    lane = lax.broadcasted_iota(jnp.int32, (LOSS_ROW, L), 1)
    second = pltpu.roll(second, rest, 1)
    db[ds(0, LOSS_ROW), :] = jnp.where((lane < rest) | (lax.broadcasted_iota(jnp.int32, (LOSS_ROW, L), 0) < LOSS_ROW - 1),
                                       first[:LOSS_ROW], second[:1])
    db[ds(LOSS_ROW, LOSS_ROW), :] = jnp.where(lane < rest, second[:LOSS_ROW], second[1:LOSS_ROW + 1])
    at = SMALL0 - VEC0 + LOSS_ROW
    total = aux[0, ds(at, 1), :] + aux[1, ds(at, 1), :] - aux[0, ds(at + 1, 1), :]
    loss[...] = jnp.sum(total, axis=1, keepdims=True)


def small_call(aux):
    vm = pl.BlockSpec(memory_space=VMEM)
    return pl.pallas_call(
        small_kernel,
        out_shape=tuple(jax.ShapeDtypeStruct(t, F32) for t in [(TILE, L)] * 3 + [(2 * LOSS_ROW, L), (1, 1)]),
        in_specs=[vm],
        out_specs=(vm,) * 5,
        name="small_results",
    )(aux)


def solution(mesh):
    n_groups = mesh.shape["dp"]

    def local_step(hidden, mask_pos, labels, w_trans, b_trans, ln_gain, ln_bias, emb_table, b_vocab):
        n_rows, seq_len, width = hidden.shape
        n_masks = mask_pos.shape[1]
        n_tokens = n_rows * n_masks * n_groups
        line = lambda v: v.reshape(1, v.shape[0])
        dz, aux, res = head_call(1.0 / n_tokens, mask_pos, labels, line(b_vocab), line(b_trans), line(ln_gain), line(ln_bias),
                                 hidden.reshape(n_rows * seq_len, width), emb_table, w_trans)
        d_emb, d_w_trans, d_hidden = write_call(res, mask_pos, dz)
        aux, d_w_trans = lax.optimization_barrier((aux, d_w_trans))
        *vecs, db, loss = small_call(aux)
        d_b_trans, d_gain, d_bias = (v.reshape(width) for v in vecs)
        d_b_vocab = db.reshape(2 * ROWS)[:2 * VROWS]
        return loss.reshape(()) / n_tokens, d_hidden.reshape(hidden.shape), d_w_trans, d_b_trans, d_gain, d_bias, d_emb, d_b_vocab

    in_specs = (P("dp", None, None), P("dp", None), P("dp", None), P(None, None), P(None), P(None), P(None), P("vp", None), P("vp"))
    out_specs = (P(), P("dp", None, None), P(None, None), P(None), P(None), P(None), P("vp", None), P("vp"))
    return jax.shard_map(local_step, mesh=mesh, in_specs=in_specs, out_specs=out_specs, check_vma=False)
```
